8 devices in a mesh: dp: 1 (over z), ep: 8 (over y, x, core).
Axes of the slice: x: 2, y: 2, z: 1, core: 2. Of those that a mesh axis runs over, the one named last changes fastest.
Arguments:
- tokens: bfloat16 [512, 4096], P(('dp', 'ep'))
- slot_ids: int32 [512, 4, 32], P(('dp', 'ep'))
- request_rows: int32 [8, 8, 128], P(('dp', 'ep'))
- gate_vals: float32 [512, 4, 32], P(('dp', 'ep'))
- grad_out: bfloat16 [512, 4096], P(('dp', 'ep'))
- table_up: bfloat16 [16384, 4096], P('ep')
- table_down: bfloat16 [16384, 4096], P('ep')
Outputs:
- output 1: bfloat16 [512, 4096], P(('dp', 'ep'))
- output 2: bfloat16 [512, 4096], P(('dp', 'ep'))
- output 3: bfloat16 [16384, 4096], P(('dp', 'ep'))
- output 4: bfloat16 [16384, 4096], P(('dp', 'ep'))
All inputs are finite; a program needn't handle non-finite values.
Results may differ from the reference program's by a relative error of at most 0.0087426.
Values are sent between devices in bfloat16 or wider.
A program may use at most 1 GiB of HBM per device.

```python
import math
import jax
import jax.numpy as jnp
from jax import lax

TOKENS_DEV = 64
DISTINCT = 128
GROUP_SIZE = 8
EXPERTS = 16384
MODEL_DIM = 4096
NUM_HEADS = 4
TOP_K = 32


def draw_routing(route_key):
    rows_owner = EXPERTS // GROUP_SIZE
    sel_dev = TOKENS_DEV * NUM_HEADS * TOP_K
    slots_dev = GROUP_SIZE * DISTINCT
    hot_slots = max(1, DISTINCT // 8)
    sub_keys = jax.random.split(route_key, 9)
    owner_perm = jax.vmap(lambda one_key: jax.random.permutation(one_key, rows_owner))(jax.random.split(sub_keys[0], GROUP_SIZE))
    hot_first = jax.random.randint(sub_keys[1], (), 0, GROUP_SIZE)
    hot_second = (hot_first + 1 + jax.random.randint(sub_keys[2], (), 0, GROUP_SIZE - 1)) % GROUP_SIZE
    owner_iota = jnp.arange(GROUP_SIZE)
    hot_owner = (owner_iota == hot_first) | (owner_iota == hot_second)
    offsets = jax.random.randint(sub_keys[3], (GROUP_SIZE, GROUP_SIZE), 0, rows_owner)
    offsets = jnp.where(hot_owner[None, :], 0, offsets)
    window_cols = (offsets[:, :, None] + jnp.arange(DISTINCT)[None, None, :]) % rows_owner
    request_rows = owner_perm[owner_iota[None, :, None], window_cols]
    cover_rank = jax.vmap(lambda one_key: jax.random.permutation(one_key, sel_dev))(jax.random.split(sub_keys[4], GROUP_SIZE))
    hot_pick = jax.random.randint(sub_keys[5], (GROUP_SIZE, sel_dev), 0, 2) == 0
    hot_side = jnp.where(jax.random.randint(sub_keys[6], (GROUP_SIZE, sel_dev), 0, 2) == 0, hot_first, hot_second)
    hot_slot = hot_side * DISTINCT + jax.random.randint(sub_keys[7], (GROUP_SIZE, sel_dev), 0, hot_slots)
    cold_slot = jax.random.randint(sub_keys[8], (GROUP_SIZE, sel_dev), 0, slots_dev)
    slot_ids = jnp.where(cover_rank < slots_dev, cover_rank, jnp.where(hot_pick, hot_slot, cold_slot))
    slot_ids = slot_ids.reshape(GROUP_SIZE * TOKENS_DEV, NUM_HEADS, TOP_K).astype(jnp.int32)
    return slot_ids, request_rows.astype(jnp.int32)


def setup_inputs(seed: int = 0, part: int = 0) -> dict:
    part_key = jax.random.fold_in(jax.random.key(seed), part)
    key_tok, key_grad, key_gate, key_route = jax.random.split(part_key, 4)
    key_up, key_down = jax.random.split(jax.random.key(seed + 1), 2)
    n_tok = GROUP_SIZE * TOKENS_DEV
    sel_tok = NUM_HEADS * TOP_K
    tokens = jax.random.normal(key_tok, (n_tok, MODEL_DIM), jnp.float32)
    grad_out = jax.random.normal(key_grad, (n_tok, MODEL_DIM), jnp.float32)
    gate_vals = jax.random.uniform(key_gate, (n_tok, NUM_HEADS, TOP_K), jnp.float32, 0.25, 1.75)
    table_up = jax.random.normal(key_up, (EXPERTS, MODEL_DIM), jnp.float32) * MODEL_DIM ** -0.5
    table_down = jax.random.normal(key_down, (EXPERTS, MODEL_DIM), jnp.float32) * sel_tok ** -0.5
    slot_ids, request_rows = draw_routing(key_route)
    return dict(tokens=tokens.astype(jnp.bfloat16), slot_ids=slot_ids, request_rows=request_rows, gate_vals=gate_vals, grad_out=grad_out.astype(jnp.bfloat16), table_up=table_up.astype(jnp.bfloat16), table_down=table_down.astype(jnp.bfloat16))


def gelu_pair(pre_act):
    normal_cdf = 0.5 * (1.0 + lax.erf(pre_act * (2.0 ** -0.5)))
    normal_pdf = jnp.exp(-0.5 * pre_act * pre_act) * ((2.0 * math.pi) ** -0.5)
    return pre_act * normal_cdf, normal_cdf + pre_act * normal_pdf


def reference(tokens, slot_ids, request_rows, gate_vals, grad_out, table_up, table_down):
    n_tok = GROUP_SIZE * TOKENS_DEV
    sel_tok = NUM_HEADS * TOP_K
    rows_owner = EXPERTS // GROUP_SIZE
    slot_flat = slot_ids.reshape(n_tok, sel_tok)
    dev_idx = jnp.arange(n_tok)[:, None] // TOKENS_DEV
    owner_idx = slot_flat // DISTINCT
    expert_ids = owner_idx * rows_owner + request_rows[dev_idx, owner_idx, slot_flat % DISTINCT]
    cap_tokens = max(1, 2 ** 23 // (sel_tok * MODEL_DIM))
    block_tok = math.gcd(n_tok, 2 ** int(math.log2(cap_tokens)))
    n_blocks = n_tok // block_tok

    def scan_step(acc_pair, block_in):
        acc_up, acc_down = acc_pair
        x_blk, id_blk, gate_blk, dy_blk = block_in
        x_wide = x_blk.astype(jnp.float32)
        dy_wide = dy_blk.astype(jnp.float32)
        up_rows = table_up[id_blk].astype(jnp.float32)
        down_rows = table_down[id_blk].astype(jnp.float32)
        pre_act = jnp.einsum('bsd,bd->bs', up_rows, x_wide)
        act_val, slope_val = gelu_pair(pre_act)
        w_out = (gate_blk * act_val).astype(jnp.bfloat16).astype(jnp.float32)
        y_blk = jnp.einsum('bs,bsd->bd', w_out, down_rows)
        back_dot = jnp.einsum('bsd,bd->bs', down_rows, dy_wide)
        coef_val = (gate_blk * slope_val * back_dot).astype(jnp.bfloat16).astype(jnp.float32)
        dx_blk = jnp.einsum('bs,bsd->bd', coef_val, up_rows)
        flat_ids = id_blk.reshape(-1)
        acc_up = acc_up.at[flat_ids].add((coef_val[:, :, None] * x_wide[:, None, :]).reshape(-1, MODEL_DIM))
        acc_down = acc_down.at[flat_ids].add((w_out[:, :, None] * dy_wide[:, None, :]).reshape(-1, MODEL_DIM))
        return (acc_up, acc_down), (y_blk, dx_blk)

    zero_acc = jnp.zeros((EXPERTS, MODEL_DIM), jnp.float32)
    blocks_in = (tokens.reshape(n_blocks, block_tok, MODEL_DIM), expert_ids.reshape(n_blocks, block_tok, sel_tok), gate_vals.reshape(n_blocks, block_tok, sel_tok), grad_out.reshape(n_blocks, block_tok, MODEL_DIM))
    (acc_up, acc_down), (y_all, dx_all) = lax.scan(scan_step, (zero_acc, zero_acc), blocks_in)
    out_tokens = y_all.reshape(n_tok, MODEL_DIM).astype(jnp.bfloat16)
    grad_tokens = dx_all.reshape(n_tok, MODEL_DIM).astype(jnp.bfloat16)
    return (out_tokens, grad_tokens, acc_up.astype(jnp.bfloat16), acc_down.astype(jnp.bfloat16))
```

```python
import functools
import math
import jax
import jax.numpy as jnp
from jax import lax
from jax.experimental import pallas as pl
from jax.experimental.pallas import tpu as pltpu
from jax.sharding import PartitionSpec as P

F32, BF16 = jnp.float32, jnp.bfloat16
N_DEV, TOK, SLOTS, SEL = 8, 64, 128, 128
VMEM_BYTES = 60 * 1024 * 1024


def gelu_pair(pre_act):
    normal_cdf = 0.5 * (1.0 + lax.erf(pre_act * (2.0 ** -0.5)))
    normal_pdf = jnp.exp(-0.5 * pre_act * pre_act) * ((2.0 * math.pi) ** -0.5)
    return pre_act * normal_cdf, normal_cdf + pre_act * normal_pdf


def split3(wide):
    high = wide.astype(BF16)
    rest = wide - high.astype(F32)
    mid = rest.astype(BF16)
    low = (rest - mid.astype(F32)).astype(BF16)
    return high, mid, low


def select_kernel(act_ref, slope_ref, slot_ref, gate_ref, w_ref, c_ref, wt_ref, ct_ref, slot_t, w_t, c_t):
    owner = lax.axis_index("ep")
    local = slot_ref[...] - owner * SLOTS
    valid = (local >= 0) & (local < SLOTS)
    index = jnp.where(valid, local, 0)
    act = jnp.take_along_axis(act_ref[...], index, axis=1)
    slope = jnp.take_along_axis(slope_ref[...], index, axis=1)
    gate = gate_ref[...]
    w_sel = jnp.where(valid, (gate * act).astype(BF16).astype(F32), 0.0)
    c_sel = jnp.where(valid, (gate * slope).astype(BF16).astype(F32), 0.0)
    slot_t[...] = jnp.where(valid, local, -1).T
    w_t[...] = w_sel.T
    c_t[...] = c_sel.T
    rows = lax.broadcasted_iota(jnp.int32, (SLOTS, 2 * TOK), 0)

    def step(s, acc):
        acc_w, acc_c = acc
        hit = rows == slot_t[pl.ds(s, 1), :]
        acc_w += jnp.where(hit, w_t[pl.ds(s, 1), :], 0.0)
        acc_c += jnp.where(hit, c_t[pl.ds(s, 1), :], 0.0)
        return acc_w, acc_c

    zero = jnp.zeros((SLOTS, 2 * TOK), F32)
    acc_w, acc_c = lax.fori_loop(0, SEL, step, (zero, zero), unroll=4)
    for k, term in enumerate(split3(acc_w.T)):
        w_ref[k] = term
    for k, term in enumerate(split3(acc_c.T)):
        c_ref[k] = term
    for k, term in enumerate(split3(acc_w)):
        wt_ref[k] = term
    for k, term in enumerate(split3(acc_c)):
        ct_ref[k] = term


def token_kernel(w_ref, c_ref, v_ref, u_ref, out_ref):
    width = v_ref.shape[1]
    for col in range(0, width, 512):
        out_ref[:, col:col + 512] = sum(jnp.dot(w_ref[k], v_ref[:, col:col + 512], preferred_element_type=F32) for k in range(3))
        out_ref[:, width + col:width + col + 512] = sum(jnp.dot(c_ref[k], u_ref[:, col:col + 512], preferred_element_type=F32) for k in range(3))


def row_kernel(block, req_ref, wt_ref, ct_ref, x_ref, dy_ref, du_ref, dv_ref, lhs):
    first = pl.program_id(0) * block
    rows = lax.broadcasted_iota(jnp.int32, (block, SLOTS), 0) + first
    for q in range(N_DEV):
        pick = jnp.where(rows == req_ref[pl.ds(q, 1), :], 1.0, 0.0).astype(BF16)
        cols = slice(q * TOK, (q + 1) * TOK)
        half = slice((q % 2) * TOK, (q % 2 + 1) * TOK)
        for k in range(3):
            for m, ref in enumerate((ct_ref, wt_ref)):
                full = jnp.dot(pick, ref[k, (q // 2) * SLOTS:(q // 2 + 1) * SLOTS, :], preferred_element_type=F32)
                lhs[m, k, :, cols] = full[:, half].astype(BF16)
    width = x_ref.shape[1]
    for col in range(0, width, 512):
        du_ref[:, col:col + 512] = sum(jnp.dot(lhs[0, k], x_ref[:, col:col + 512], preferred_element_type=F32) for k in range(3)).astype(BF16)
        dv_ref[:, col:col + 512] = sum(jnp.dot(lhs[1, k], dy_ref[:, col:col + 512], preferred_element_type=F32) for k in range(3)).astype(BF16)


def solution(mesh):
    tok_spec = P(('dp', 'ep'))
    table_spec = P('ep')

    def per_device(tokens, slot_ids, request_rows, gate_vals, grad_out, up_local, down_local):
        width = tokens.shape[1]
        rows_owner = up_local.shape[0]
        owner = lax.axis_index('ep')
        n_tok = N_DEV * TOK
        small = jnp.concatenate([request_rows[0].astype(F32), slot_ids.reshape(TOK, SEL).astype(F32), gate_vals.reshape(TOK, SEL)], axis=0)
        small_all = lax.all_gather(small, 'ep', axis=0)
        x_all = lax.all_gather(tokens, 'ep', axis=0)
        dy_all = lax.all_gather(grad_out, 'ep', axis=0)
        asked = lax.dynamic_index_in_dim(small_all[:, :N_DEV], owner, 1, keepdims=False).astype(jnp.int32)
        slot_all = small_all[:, N_DEV:N_DEV + TOK].astype(jnp.int32).reshape(n_tok, SEL)
        gate_all = small_all[:, N_DEV + TOK:].reshape(n_tok, SEL)
        up_rows = up_local[asked]
        down_rows = down_local[asked]
        pre_act = jnp.einsum('qtd,qrd->qtr', x_all, up_rows, preferred_element_type=F32)
        back_dot = jnp.einsum('qtd,qrd->qtr', dy_all, down_rows, preferred_element_type=F32)
        act, slope = gelu_pair(pre_act)
        slope = slope * back_dot
        pair = 2 * TOK
        blk = pl.BlockSpec((pair, SLOTS), lambda i: (i, 0))
        tok_blk = pl.BlockSpec((3, pair, SLOTS), lambda i: (0, i, 0))
        tr_blk = pl.BlockSpec((3, SLOTS, pair), lambda i: (0, i, 0))
        w_tok, c_tok, w_tr, c_tr = pl.pallas_call(
            select_kernel,
            grid=(n_tok // pair,),
            in_specs=[blk] * 4,
            out_specs=[tok_blk, tok_blk, tr_blk, tr_blk],
            out_shape=[jax.ShapeDtypeStruct((3, n_tok, SLOTS), BF16)] * 2 + [jax.ShapeDtypeStruct((3, n_tok // pair * SLOTS, pair), BF16)] * 2,
            scratch_shapes=[pltpu.VMEM((SEL, pair), jnp.int32), pltpu.VMEM((SEL, pair), F32), pltpu.VMEM((SEL, pair), F32)],
        )(act.reshape(n_tok, SLOTS), slope.reshape(n_tok, SLOTS), slot_all, gate_all)
        coef = pl.BlockSpec((3, TOK, SLOTS), lambda q: (0, q, 0))
        table = pl.BlockSpec((None, SLOTS, width), lambda q: (q, 0, 0))
        partial = pl.pallas_call(
            token_kernel,
            grid=(N_DEV,),
            in_specs=[coef, coef, table, table],
            out_specs=pl.BlockSpec((TOK, 2 * width), lambda q: (q, 0)),
            out_shape=jax.ShapeDtypeStruct((n_tok, 2 * width), F32),
            compiler_params=pltpu.CompilerParams(vmem_limit_bytes=VMEM_BYTES),
        )(w_tok, c_tok, down_rows, up_rows)
        token_out = lax.psum_scatter(partial, 'ep', scatter_dimension=0, tiled=True)
        block = 256
        whole = lambda *shape: pl.BlockSpec(shape, lambda i: (0,) * len(shape))
        rows_blk = pl.BlockSpec((block, width), lambda i: (i, 0))
        grad_up, grad_down = pl.pallas_call(
            functools.partial(row_kernel, block),
            grid=(rows_owner // block,),
            in_specs=[whole(N_DEV, SLOTS), whole(*w_tr.shape), whole(*c_tr.shape), whole(n_tok, width), whole(n_tok, width)],
            out_specs=[rows_blk, rows_blk],
            out_shape=[jax.ShapeDtypeStruct((rows_owner, width), BF16)] * 2,
            scratch_shapes=[pltpu.VMEM((2, 3, block, n_tok), BF16)],
            compiler_params=pltpu.CompilerParams(vmem_limit_bytes=VMEM_BYTES),
            cost_estimate=pl.CostEstimate(flops=12 * rows_owner * width * n_tok, bytes_accessed=4 * rows_owner * width, transcendentals=0),
        )(asked, w_tr, c_tr, x_all.reshape(n_tok, width), dy_all.reshape(n_tok, width))
        return token_out[:, :width].astype(BF16), token_out[:, width:].astype(BF16), grad_up, grad_down

    return jax.shard_map(per_device, mesh=mesh, in_specs=(tok_spec, tok_spec, tok_spec, tok_spec, tok_spec, table_spec, table_spec), out_specs=(tok_spec, tok_spec, tok_spec, tok_spec), check_vma=False)
```

```python
import functools
import math
import jax
import jax.numpy as jnp
from jax import lax
from jax.experimental import pallas as pl
from jax.experimental.pallas import tpu as pltpu
from jax.sharding import PartitionSpec as P

F32, BF16 = jnp.float32, jnp.bfloat16
N_DEV, TOK, SLOTS, SEL = 8, 64, 128, 128
VMEM_BYTES = 60 * 1024 * 1024


def gelu_pair(pre_act):
    normal_cdf = 0.5 * (1.0 + lax.erf(pre_act * (2.0 ** -0.5)))
    normal_pdf = jnp.exp(-0.5 * pre_act * pre_act) * ((2.0 * math.pi) ** -0.5)
    return pre_act * normal_cdf, normal_cdf + pre_act * normal_pdf


def split3(wide):
    high = wide.astype(BF16)
    rest = wide - high.astype(F32)
    mid = rest.astype(BF16)
    low = (rest - mid.astype(F32)).astype(BF16)
    return high, mid, low


def select_kernel(act_ref, slope_ref, slot_ref, gate_ref, w_ref, c_ref, wt_ref, ct_ref, slot_t, w_t, c_t):
    owner = lax.axis_index("ep")
    local = slot_ref[...] - owner * SLOTS
    valid = (local >= 0) & (local < SLOTS)
    index = jnp.where(valid, local, 0)
    act = jnp.take_along_axis(act_ref[...], index, axis=1)
    slope = jnp.take_along_axis(slope_ref[...], index, axis=1)
    gate = gate_ref[...]
    w_sel = jnp.where(valid, (gate * act).astype(BF16).astype(F32), 0.0)
    c_sel = jnp.where(valid, (gate * slope).astype(BF16).astype(F32), 0.0)
    slot_t[...] = jnp.where(valid, local, -1).T
    w_t[...] = w_sel.T
    c_t[...] = c_sel.T
    rows = lax.broadcasted_iota(jnp.int32, (SLOTS, 2 * TOK), 0)

    def step(s, acc):
        acc_w, acc_c = acc
        hit = rows == slot_t[pl.ds(s, 1), :]
        acc_w += jnp.where(hit, w_t[pl.ds(s, 1), :], 0.0)
        acc_c += jnp.where(hit, c_t[pl.ds(s, 1), :], 0.0)
        return acc_w, acc_c

    zero = jnp.zeros((SLOTS, 2 * TOK), F32)
    acc_w, acc_c = lax.fori_loop(0, SEL, step, (zero, zero), unroll=4)
    for k, term in enumerate(split3(acc_w.T)):
        w_ref[k] = term
    for k, term in enumerate(split3(acc_c.T)):
        c_ref[k] = term
    for k, term in enumerate(split3(acc_w)):
        wt_ref[k] = term
    for k, term in enumerate(split3(acc_c)):
        ct_ref[k] = term


def token_kernel(order_ref, w_m, c_m, v_m, u_m, w_o, c_o, v_o, u_o, mine_ref, other_ref):
    half = v_m.shape[1]
    for out, w, c, v, u in ((mine_ref, w_m, c_m, v_m, u_m), (other_ref, w_o, c_o, v_o, u_o)):
        for col in range(0, half, 512):
            out[:, col:col + 512] = sum(jnp.dot(w[k], v[:, col:col + 512], preferred_element_type=F32) for k in range(3))
            out[:, half + col:half + col + 512] = sum(jnp.dot(c[k], u[:, col:col + 512], preferred_element_type=F32) for k in range(3))


def row_kernel(block, req_ref, coef_ref, x_ref, out_ref, lhs):
    first = pl.program_id(0) * block
    rows = lax.broadcasted_iota(jnp.int32, (block, SLOTS), 0) + first
    for q in range(N_DEV):
        pick = jnp.where(rows == req_ref[pl.ds(q, 1), :], 1.0, 0.0).astype(BF16)
        cols = slice(q * TOK, (q + 1) * TOK)
        half = slice((q % 2) * TOK, (q % 2 + 1) * TOK)
        for k in range(3):
            full = jnp.dot(pick, coef_ref[k, (q // 2) * SLOTS:(q // 2 + 1) * SLOTS, :], preferred_element_type=F32)
            lhs[k, :, cols] = full[:, half].astype(BF16)
    width = x_ref.shape[1]
    for col in range(0, width, 512):
        out_ref[:, col:col + 512] = sum(jnp.dot(lhs[k], x_ref[:, col:col + 512], preferred_element_type=F32) for k in range(3)).astype(BF16)


def solution(mesh):
    tok_spec = P(('dp', 'ep'))
    table_spec = P('ep')

    def per_device(tokens, slot_ids, request_rows, gate_vals, grad_out, up_local, down_local):
        width = tokens.shape[1]
        rows_owner = up_local.shape[0]
        owner = lax.axis_index('ep')
        n_tok = N_DEV * TOK
        small = jnp.concatenate([request_rows[0].astype(F32), slot_ids.reshape(TOK, SEL).astype(F32), gate_vals.reshape(TOK, SEL)], axis=0)
        small_all = lax.all_gather(small, 'ep', axis=0)
        x_all = lax.all_gather(tokens, 'ep', axis=0)
        dy_all = lax.all_gather(grad_out, 'ep', axis=0)
        asked = lax.dynamic_index_in_dim(small_all[:, :N_DEV], owner, 1, keepdims=False).astype(jnp.int32)
        slot_all = small_all[:, N_DEV:N_DEV + TOK].astype(jnp.int32).reshape(n_tok, SEL)
        gate_all = small_all[:, N_DEV + TOK:].reshape(n_tok, SEL)
        up_rows = up_local[asked]
        down_rows = down_local[asked]
        pre_act = jnp.einsum('qtd,qrd->qtr', x_all, up_rows, preferred_element_type=F32)
        back_dot = jnp.einsum('qtd,qrd->qtr', dy_all, down_rows, preferred_element_type=F32)
        act, slope = gelu_pair(pre_act)
        slope = slope * back_dot
        pair = 2 * TOK
        blk = pl.BlockSpec((pair, SLOTS), lambda i: (i, 0))
        tok_blk = pl.BlockSpec((3, pair, SLOTS), lambda i: (0, i, 0))
        tr_blk = pl.BlockSpec((3, SLOTS, pair), lambda i: (0, i, 0))
        w_tok, c_tok, w_tr, c_tr = pl.pallas_call(
            select_kernel,
            grid=(n_tok // pair,),
            in_specs=[blk] * 4,
            out_specs=[tok_blk, tok_blk, tr_blk, tr_blk],
            out_shape=[jax.ShapeDtypeStruct((3, n_tok, SLOTS), BF16)] * 2 + [jax.ShapeDtypeStruct((3, n_tok // pair * SLOTS, pair), BF16)] * 2,
            scratch_shapes=[pltpu.VMEM((SEL, pair), jnp.int32), pltpu.VMEM((SEL, pair), F32), pltpu.VMEM((SEL, pair), F32)],
        )(act.reshape(n_tok, SLOTS), slope.reshape(n_tok, SLOTS), slot_all, gate_all)
        core = owner % 2
        chip = owner // 2
        half = width // 2
        masks = jnp.where(core == 0, jnp.array([0, 1, 2, 3]), jnp.array([0, 2, 1, 3]))
        masks_other = jnp.where(core == 0, jnp.array([0, 2, 1, 3]), jnp.array([0, 1, 2, 3]))
        order = jnp.stack([chip ^ masks, chip ^ masks_other, jnp.full((4,), core), jnp.full((4,), 1 - core)]).astype(jnp.int32)
        coef_of = lambda m: pl.BlockSpec((3, TOK, SLOTS), lambda r, h, o: (0, o[m, r] * 2 + h, 0))
        table_of = lambda m: pl.BlockSpec((None, SLOTS, half), lambda r, h, o: (o[m, r] * 2 + h, 0, o[2 + m, 0]))
        out_blk = pl.BlockSpec((None, TOK, width), lambda r, h, o: (r, h, 0))
        mine, other = pl.pallas_call(
            token_kernel,
            grid_spec=pltpu.PrefetchScalarGridSpec(
                num_scalar_prefetch=1,
                grid=(4, 2),
                in_specs=[coef_of(0), coef_of(0), table_of(0), table_of(0), coef_of(1), coef_of(1), table_of(1), table_of(1)],
                out_specs=[out_blk, out_blk],
            ),
            out_shape=[jax.ShapeDtypeStruct((4, 2 * TOK, width), F32)] * 2,
            compiler_params=pltpu.CompilerParams(vmem_limit_bytes=VMEM_BYTES),
        )(order, w_tok, c_tok, down_rows, up_rows, w_tok, c_tok, down_rows, up_rows)
        partner = [(i, i ^ 1) for i in range(N_DEV)]
        first_hop = [(i, i ^ (2 if i % 2 == 0 else 4)) for i in range(N_DEV)]
        second_hop = [(i, i ^ (4 if i % 2 == 0 else 2)) for i in range(N_DEV)]
        hop = lambda value, pairs: lax.ppermute(value, 'ep', pairs)
        block = 256
        whole = lambda *shape: pl.BlockSpec(shape, lambda i: (0,) * len(shape))
        rows_blk = pl.BlockSpec((block, width), lambda i: (i, 0))

        def grad_rows(coef, tok):
            return pl.pallas_call(
                functools.partial(row_kernel, block),
                grid=(rows_owner // block,),
                in_specs=[whole(N_DEV, SLOTS), whole(*coef.shape), whole(n_tok, width)],
                out_specs=rows_blk,
                out_shape=jax.ShapeDtypeStruct((rows_owner, width), BF16),
                scratch_shapes=[pltpu.VMEM((3, block, n_tok), BF16)],
                compiler_params=pltpu.CompilerParams(vmem_limit_bytes=VMEM_BYTES),
                cost_estimate=pl.CostEstimate(flops=6 * rows_owner * width * n_tok, bytes_accessed=2 * rows_owner * width, transcendentals=0),
            )(asked, coef, tok.reshape(n_tok, width))

        pair_far = mine[3] + hop(other[3], partner)
        pair_first = mine[1] + hop(other[1], partner)
        got_second = hop(pair_far, first_hop)
        got_own = hop(pair_first, first_hop)
        pair_second = mine[2] + hop(other[2], partner)
        pair_own = mine[0] + hop(other[0], partner)
        grad_up = grad_rows(c_tr, x_all)
        got_second, grad_up = lax.optimization_barrier((got_second, grad_up))
        got_last = hop(pair_second + got_second, second_hop)
        grad_down = grad_rows(w_tr, dy_all)
        got_last, got_own, grad_down = lax.optimization_barrier((got_last, got_own, grad_down))
        final = (pair_own + got_own + got_last).astype(BF16).reshape(2, TOK, 2, half)
        keep = lax.dynamic_index_in_dim(final, core, 0, keepdims=False)
        give = lax.dynamic_index_in_dim(final, 1 - core, 0, keepdims=False)
        got = hop(give, partner)
        low = jnp.where(core == 0, keep, got)
        high = jnp.where(core == 0, got, keep)
        token_out = jnp.concatenate([low, high], axis=2)
        return token_out[:, 0], token_out[:, 1], grad_up, grad_down

    return jax.shard_map(per_device, mesh=mesh, in_specs=(tok_spec, tok_spec, tok_spec, tok_spec, tok_spec, table_spec, table_spec), out_specs=(tok_spec, tok_spec, tok_spec, tok_spec), check_vma=False)
```

```python
import functools
import math
import jax
import jax.numpy as jnp
from jax import lax
from jax.experimental import pallas as pl
from jax.experimental.pallas import tpu as pltpu
from jax.sharding import PartitionSpec as P

F32, BF16, I32 = jnp.float32, jnp.bfloat16, jnp.int32
N_DEV, TOK, SLOTS, SEL = 8, 64, 128, 128
PAIR = 2 * TOK
TERMS = 3
CHUNK = 1024
LANES = 128
PAD = 8
VMEM_BYTES = 62 * 1024 * 1024
MESH = pl.DeviceIdType.MESH


def gelu_pair(pre_act):
    normal_cdf = 0.5 * (1.0 + lax.erf(pre_act * (2.0 ** -0.5)))
    normal_pdf = jnp.exp(-0.5 * pre_act * pre_act) * ((2.0 * math.pi) ** -0.5)
    return pre_act * normal_cdf, normal_cdf + pre_act * normal_pdf


def split3(wide):
    high = wide.astype(BF16)
    rest = wide - high.astype(F32)
    mid = rest.astype(BF16)
    low = (rest - mid.astype(F32)).astype(BF16)
    return high, mid, low


def share_kernel(x_ref, dy_ref, slot_ref, gate_ref, req_ref, up_ref, down_ref,
                 x_all, dy_all, slot_all, gate_all, up_rows, down_rows, asked_out,
                 asked, asked_s, table, wide, picked, staged,
                 send_sem, recv_sem, own_sem, smem_sem, in_sem, out_sem):
    me = lax.axis_index("ep")
    n_rows, width = up_ref.shape
    n_ask = N_DEV * SLOTS
    steps = [(ref, out, col) for ref, out in ((up_ref, up_rows), (down_ref, down_rows)) for col in range(0, width, CHUNK)]

    def fetch(k):
        ref, _, col = steps[k]
        return pltpu.make_async_copy(ref.at[:, pl.ds(col, CHUNK)], table.at[k % 2], in_sem.at[k % 2])

    fetch(0).start()
    fetch(1).start()
    barrier = pltpu.get_barrier_semaphore()
    for b in range(1, N_DEV):
        pl.semaphore_signal(barrier, inc=1, device_id={"ep": me ^ b}, device_id_type=MESH)
    pl.semaphore_wait(barrier, N_DEV - 1)

    count = [0]
    sent = []

    def push(src, dst, mask):
        k = count[0]
        count[0] += 1
        copy = pltpu.make_async_remote_copy(src_ref=src, dst_ref=dst, send_sem=send_sem.at[k], recv_sem=recv_sem.at[k],
                                            device_id={"ep": me ^ mask}, device_id_type=MESH)
        copy.start()
        sent.append(copy)
        return copy

    asks = [push(req_ref.at[0, pl.ds(me ^ b, 1)], asked.at[pl.ds(b, 1)], b) for b in range(1, N_DEV)]
    first = [
        push(gate_ref, gate_all.at[4], 4), push(slot_ref, slot_all.at[2], 2),
        push(x_ref, x_all.at[4], 4), push(dy_ref, dy_all.at[2], 2),
    ]
    near = [push(gate_ref, gate_all.at[1], 1), push(slot_ref, slot_all.at[1], 1), push(x_ref, x_all.at[1], 1), push(dy_ref, dy_all.at[1], 1)]
    low, top = pl.ds(0, TOK // 2), pl.ds(TOK // 2, TOK // 2)
    second = [
        push(gate_ref, gate_all.at[2], 2), push(slot_ref, slot_all.at[4], 4),
        push(x_ref.at[low], x_all.at[2, low], 2), push(dy_ref.at[low], dy_all.at[4, low], 4),
    ]
    own = [pltpu.make_async_copy(src, dst.at[0], own_sem.at[k]) for k, (src, dst) in enumerate(((x_ref, x_all), (dy_ref, dy_all), (slot_ref, slot_all), (gate_ref, gate_all)))]
    for copy in own:
        copy.start()

    asked[pl.ds(0, 1), :] = req_ref[0, pl.ds(me, 1), :]
    for copy in asks:
        copy.wait_recv()
    asked_out[...] = asked[...]
    to_smem = pltpu.make_async_copy(asked, asked_s, smem_sem)
    to_smem.start()
    to_smem.wait()

    tiles = CHUNK // LANES
    wide_step, pick_step = n_rows + PAD, n_ask + PAD

    def gather(k):
        fetch(k).wait()

        def fill(t, _):
            r = pl.multiple_of(t * 32, 32)
            for j in range(tiles):
                wide[pl.ds(j * wide_step + r, 32), :] = table[k % 2, pl.ds(r, 32), j * LANES:(j + 1) * LANES].astype(F32)
            return 0

        lax.fori_loop(0, n_rows // 32, fill, 0)
        if k + 2 < len(steps):
            fetch(k + 2).start()

        def pick(t, _):
            for u in range(16):
                r = t * 16 + u
                row = asked_s[r // SLOTS, r % SLOTS]
                picked[pl.ds(r, tiles, stride=pick_step), :] = wide[pl.ds(row, tiles, stride=wide_step), :]
            return 0

        lax.fori_loop(0, n_ask // 16, pick, 0)
        if k >= 2:
            drain_copy(k - 2).wait()

        def drain(t, _):
            r = pl.multiple_of(t * 32, 32)
            for j in range(tiles):
                staged[k % 2, pl.ds(r, 32), j * LANES:(j + 1) * LANES] = picked[pl.ds(j * pick_step + r, 32), :].astype(BF16)
            return 0

        lax.fori_loop(0, n_ask // 32, drain, 0)
        drain_copy(k).start()

    def drain_copy(k):
        _, out, col = steps[k]
        return pltpu.make_async_copy(staged.at[k % 2], out.at[:, pl.ds(col, CHUNK)], out_sem.at[k % 2])

    for k in range(4):
        gather(k)
    for copy in first:
        copy.wait_recv()
    far = [
        push(gate_all.at[4], gate_all.at[6], 2), push(slot_all.at[2], slot_all.at[6], 4),
        push(x_all.at[4], x_all.at[6], 2), push(dy_all.at[2], dy_all.at[6], 4),
    ]
    second += [push(x_ref.at[top], x_all.at[2, top], 2), push(dy_ref.at[top], dy_all.at[4, top], 4)]
    near += [push(gate_all.at[4], gate_all.at[5], 1), push(slot_all.at[2], slot_all.at[3], 1), push(x_all.at[4], x_all.at[5], 1), push(dy_all.at[2], dy_all.at[3], 1)]
    for k in range(4, len(steps)):
        gather(k)
    for copy in far:
        copy.wait_recv()
    near += [push(ref.at[6], ref.at[7], 1) for ref in (gate_all, slot_all, x_all, dy_all)]
    for copy in second:
        copy.wait_recv()
    near += [push(gate_all.at[2], gate_all.at[3], 1), push(slot_all.at[4], slot_all.at[5], 1), push(x_all.at[2], x_all.at[3], 1), push(dy_all.at[4], dy_all.at[5], 1)]
    for copy in near:
        copy.wait_recv()
    for copy in sent:
        copy.wait_send()
    for copy in own:
        copy.wait()
    drain_copy(len(steps) - 2).wait()
    drain_copy(len(steps) - 1).wait()


N_COPIES = 7 + 4 + 4 + 4 + 4 + 2 + 4 + 4 + 4


def block_kernel(core_ref, x_ref, dy_ref, slot_ref, gate_ref, up_ref, down_ref, mine_ref, other_ref, wt_ref, ct_ref, slot_t, w_t, c_t):
    owner = lax.axis_index("ep")
    width = x_ref.shape[2]
    half = width // 2
    dims = (((1,), (1,)), ((), ()))
    up, down = up_ref, down_ref

    def dots(tok, rows):
        full = lax.dot_general(tok.reshape(PAIR, width), rows, dims, preferred_element_type=F32)
        return jnp.concatenate([full[:TOK, :SLOTS], full[TOK:, SLOTS:]], axis=0)

    act, slope = gelu_pair(dots(x_ref[...], up[...]))
    slope = slope * dots(dy_ref[...], down[...])
    local = slot_ref[...].reshape(PAIR, SEL) - owner * SLOTS
    valid = (local >= 0) & (local < SLOTS)
    index = jnp.where(valid, local, 0)
    act = jnp.take_along_axis(act, index, axis=1)
    slope = jnp.take_along_axis(slope, index, axis=1)
    gate = gate_ref[...].reshape(PAIR, SEL)
    w_t[...] = jnp.where(valid, (gate * act).astype(BF16).astype(F32), 0.0).T
    c_t[...] = jnp.where(valid, (gate * slope).astype(BF16).astype(F32), 0.0).T
    slot_t[...] = jnp.where(valid, local, -1).T
    rows = lax.broadcasted_iota(I32, (SLOTS, PAIR), 0)

    def step(s, acc):
        acc_w, acc_c = acc
        hit = rows == slot_t[pl.ds(s, 1), :]
        acc_w += jnp.where(hit, w_t[pl.ds(s, 1), :], 0.0)
        acc_c += jnp.where(hit, c_t[pl.ds(s, 1), :], 0.0)
        return acc_w, acc_c

    zero = jnp.zeros((SLOTS, PAIR), F32)
    acc_w, acc_c = lax.fori_loop(0, SEL, step, (zero, zero), unroll=4)
    for ref, acc in ((wt_ref, acc_w), (ct_ref, acc_c)):
        for k, term in enumerate(split3(acc)[:TERMS]):
            ref[k] = term
    first_half = lax.broadcasted_iota(I32, (PAIR, 2 * SLOTS), 0) < TOK
    first_cols = lax.broadcasted_iota(I32, (PAIR, 2 * SLOTS), 1) < SLOTS

    def spread(acc):
        both = jnp.concatenate([acc.T, acc.T], axis=1)
        return split3(jnp.where(first_half == first_cols, both, 0.0))

    w_terms, c_terms = spread(acc_w), spread(acc_c)
    core = core_ref[0]
    for col in range(0, half, 512):
        for shift, terms, table in ((0, w_terms, down), (half, c_terms, up)):
            here = pl.ds(pl.multiple_of(core * half + col, 512), 512)
            there = pl.ds(pl.multiple_of((1 - core) * half + col, 512), 512)
            dst = slice(shift + col, shift + col + 512)
            mine_ref[:, dst] = sum(jnp.dot(term, table[:, here], preferred_element_type=F32) for term in terms)
            part = sum(jnp.dot(term, table[:, there], preferred_element_type=F32) for term in terms)
            other_ref[:TOK, dst] = part[TOK:]
            other_ref[TOK:, dst] = part[:TOK]


def row_kernel(block, req_ref, near_ref, far_ref, x_ref, out_ref, lhs):
    first = pl.program_id(0) * block
    rows = lax.broadcasted_iota(I32, (block, SLOTS), 0) + first
    chips = [near_ref.at[2], near_ref.at[0], near_ref.at[1], far_ref.at[0]]
    for q in range(N_DEV):
        pick = jnp.where(rows == req_ref[pl.ds(q, 1), :], 1.0, 0.0).astype(BF16)
        cols = slice(q * TOK, (q + 1) * TOK)
        half = slice((q % 2) * TOK, (q % 2 + 1) * TOK)
        for k in range(TERMS):
            full = jnp.dot(pick, chips[q // 2][k], preferred_element_type=F32)
            lhs[k, :, cols] = full[:, half].astype(BF16)
    width = x_ref.shape[1]
    for col in range(0, width, 512):
        out_ref[:, col:col + 512] = sum(jnp.dot(lhs[k], x_ref[:, col:col + 512], preferred_element_type=F32) for k in range(TERMS)).astype(BF16)


def solution(mesh):
    tok_spec = P(('dp', 'ep'))
    table_spec = P('ep')

    def per_device(tokens, slot_ids, request_rows, gate_vals, grad_out, up_local, down_local):
        width = tokens.shape[1]
        rows_owner = up_local.shape[0]
        n_tok = N_DEV * TOK
        half = width // 2
        core = lax.axis_index('ep') % 2
        vmem, anyw = pl.BlockSpec(memory_space=pltpu.VMEM), pl.BlockSpec(memory_space=pl.ANY)
        shape = jax.ShapeDtypeStruct
        x_all, dy_all, slot_all, gate_all, up_rows, down_rows, asked = pl.pallas_call(
            share_kernel,
            in_specs=[vmem] * 5 + [anyw] * 2,
            out_specs=[anyw] * 6 + [vmem],
            out_shape=[shape((N_DEV, TOK, width), BF16)] * 2 + [shape((N_DEV, TOK, SEL), I32), shape((N_DEV, TOK, SEL), F32)]
            + [shape((N_DEV * SLOTS, width), BF16)] * 2 + [shape((N_DEV, SLOTS), I32)],
            scratch_shapes=[
                pltpu.VMEM((N_DEV, SLOTS), I32), pltpu.SMEM((N_DEV, SLOTS), I32),
                pltpu.VMEM((2, rows_owner, CHUNK), BF16),
                pltpu.VMEM((CHUNK // LANES * (rows_owner + PAD), LANES), F32),
                pltpu.VMEM((CHUNK // LANES * (N_DEV * SLOTS + PAD), LANES), F32),
                pltpu.VMEM((2, N_DEV * SLOTS, CHUNK), BF16),
                pltpu.SemaphoreType.DMA((N_COPIES,)), pltpu.SemaphoreType.DMA((N_COPIES,)),
                pltpu.SemaphoreType.DMA((4,)), pltpu.SemaphoreType.DMA,
                pltpu.SemaphoreType.DMA((2,)), pltpu.SemaphoreType.DMA((2,)),
            ],
            compiler_params=pltpu.CompilerParams(collective_id=0, has_side_effects=True, vmem_limit_bytes=VMEM_BYTES),
        )(tokens, grad_out, slot_ids.reshape(TOK, SEL), gate_vals.reshape(TOK, SEL), request_rows, up_local, down_local)

        core_arr = core.reshape(1).astype(I32)

        def blocks(n, chip, mine_at, other_at):
            tok = pl.BlockSpec((2, TOK, width), lambda i, c: (chip(i), 0, 0))
            side = pl.BlockSpec((2, TOK, SEL), lambda i, c: (chip(i), 0, 0))
            table = pl.BlockSpec((2 * SLOTS, width), lambda i, c: (chip(i), 0))
            coef = pl.BlockSpec((None, TERMS, SLOTS, PAIR), lambda i, c: (i, 0, 0, 0))
            return pl.pallas_call(
                block_kernel,
                grid_spec=pltpu.PrefetchScalarGridSpec(
                    num_scalar_prefetch=1,
                    grid=(n,),
                    in_specs=[tok, tok, side, side, table, table],
                    out_specs=[pl.BlockSpec((None, PAIR, width), lambda i, c: (mine_at(i, c[0]), 0, 0)),
                               pl.BlockSpec((None, PAIR, width), lambda i, c: (other_at(i, c[0]), 0, 0)), coef, coef],
                    scratch_shapes=[pltpu.VMEM((SEL, PAIR), I32), pltpu.VMEM((SEL, PAIR), F32), pltpu.VMEM((SEL, PAIR), F32)],
                ),
                out_shape=[shape((n, PAIR, width), F32)] * 2 + [shape((n, TERMS, SLOTS, PAIR), BF16)] * 2,
                compiler_params=pltpu.CompilerParams(vmem_limit_bytes=VMEM_BYTES),
                cost_estimate=pl.CostEstimate(flops=n * 10 ** 10, bytes_accessed=10 ** 6, transcendentals=0),
            )(core_arr, x_all, dy_all, slot_all, gate_all, up_rows, down_rows)

        def near_slot(i, c):
            return jnp.where(i == 2, 2, i ^ c)

        mine_far, other_far, w_far, c_far = blocks(1, lambda i: i + 3, lambda i, c: i, lambda i, c: i)
        mine, other, w_near, c_near = blocks(3, lambda i: lax.rem(i + 1, 3), near_slot, lambda i, c: near_slot(i, 1 - c))
        partner = [(i, i ^ 1) for i in range(N_DEV)]
        first_hop = [(i, i ^ (2 if i % 2 == 0 else 4)) for i in range(N_DEV)]
        second_hop = [(i, i ^ (4 if i % 2 == 0 else 2)) for i in range(N_DEV)]
        hop = lambda value, pairs: lax.ppermute(value, 'ep', pairs)
        block = 256
        whole = lambda *dims: pl.BlockSpec(dims, lambda i: (0,) * len(dims))

        def grad_rows(coef_near, coef_far, tok):
            return pl.pallas_call(
                functools.partial(row_kernel, block),
                grid=(rows_owner // block,),
                in_specs=[whole(N_DEV, SLOTS), whole(*coef_near.shape), whole(*coef_far.shape), whole(n_tok, width)],
                out_specs=pl.BlockSpec((block, width), lambda i: (i, 0)),
                out_shape=shape((rows_owner, width), BF16),
                scratch_shapes=[pltpu.VMEM((TERMS, block, n_tok), BF16)],
                compiler_params=pltpu.CompilerParams(vmem_limit_bytes=VMEM_BYTES),
                cost_estimate=pl.CostEstimate(flops=6 * rows_owner * width * n_tok, bytes_accessed=2 * rows_owner * width, transcendentals=0),
            )(asked, coef_near, coef_far, tok.reshape(n_tok, width))

        got_far = hop(other_far, partner)
        got_far, mine = lax.optimization_barrier((got_far, mine))
        got_second = hop(mine_far[0] + got_far[0], first_hop)
        got = hop(other, partner)
        got_own = hop(mine[0] + got[0], first_hop)
        grad_up = grad_rows(c_near, c_far, x_all)
        got_second, grad_up = lax.optimization_barrier((got_second, grad_up))
        got_last = hop(mine[1] + got[1] + got_second, second_hop)
        grad_down = grad_rows(w_near, w_far, dy_all)
        got_last, got_own, grad_down = lax.optimization_barrier((got_last, got_own, grad_down))
        final = (mine[2] + got[2] + got_own + got_last).astype(BF16).reshape(2, TOK, 2, half)
        keep, give = final[0], final[1]
        back = hop(give, partner)
        low = jnp.where(core == 0, keep, back)
        high = jnp.where(core == 0, back, keep)
        token_out = jnp.concatenate([low, high], axis=2)
        return token_out[:, 0], token_out[:, 1], grad_up, grad_down

    return jax.shard_map(per_device, mesh=mesh, in_specs=(tok_spec, tok_spec, tok_spec, tok_spec, tok_spec, table_spec, table_spec), out_specs=(tok_spec, tok_spec, tok_spec, tok_spec), check_vma=False)
```

```python
import functools
import math
import jax
import jax.numpy as jnp
from jax import lax
from jax.experimental import pallas as pl
from jax.experimental.pallas import tpu as pltpu
from jax.sharding import PartitionSpec as P

F32, BF16, I32 = jnp.float32, jnp.bfloat16, jnp.int32
N_DEV, TOK, SLOTS, SEL = 8, 64, 128, 128
PAIR = 2 * TOK
TERMS = 3
CHUNK = 1024
LANES = 128
PAD = 8
VMEM_BYTES = 62 * 1024 * 1024
MESH = pl.DeviceIdType.MESH


def gelu_pair(pre_act):
    normal_cdf = 0.5 * (1.0 + lax.erf(pre_act * (2.0 ** -0.5)))
    normal_pdf = jnp.exp(-0.5 * pre_act * pre_act) * ((2.0 * math.pi) ** -0.5)
    return pre_act * normal_cdf, normal_cdf + pre_act * normal_pdf


def split3(wide):
    high = wide.astype(BF16)
    rest = wide - high.astype(F32)
    mid = rest.astype(BF16)
    low = (rest - mid.astype(F32)).astype(BF16)
    return high, mid, low


def share_kernel(x_ref, dy_ref, slot_ref, gate_ref, req_ref, up_ref, down_ref,
                 x_all, dy_all, slot_all, gate_all, up_rows, down_rows, asked_out,
                 asked, asked_s, table, wide, picked, staged,
                 send_sem, recv_sem, own_sem, smem_sem, in_sem, out_sem):
    me = lax.axis_index("ep")
    n_rows, width = up_ref.shape
    n_ask = N_DEV * SLOTS
    steps = [(ref, out, col) for ref, out in ((up_ref, up_rows), (down_ref, down_rows)) for col in range(0, width, CHUNK)]

    def fetch(k):
        ref, _, col = steps[k]
        return pltpu.make_async_copy(ref.at[:, pl.ds(col, CHUNK)], table.at[k % 2], in_sem.at[k % 2])

    fetch(0).start()
    fetch(1).start()
    barrier = pltpu.get_barrier_semaphore()
    for b in range(1, N_DEV):
        pl.semaphore_signal(barrier, inc=1, device_id={"ep": me ^ b}, device_id_type=MESH)
    pl.semaphore_wait(barrier, N_DEV - 1)

    count = [0]
    sent = []

    def push(src, dst, mask):
        k = count[0]
        count[0] += 1
        copy = pltpu.make_async_remote_copy(src_ref=src, dst_ref=dst, send_sem=send_sem.at[k], recv_sem=recv_sem.at[k],
                                            device_id={"ep": me ^ mask}, device_id_type=MESH)
        copy.start()
        sent.append(copy)
        return copy

    asks = [push(req_ref.at[0, pl.ds(me ^ b, 1)], asked.at[pl.ds(b, 1)], b) for b in range(1, N_DEV)]
    first = [
        push(gate_ref, gate_all.at[4], 4), push(slot_ref, slot_all.at[2], 2),
        push(x_ref, x_all.at[4], 4), push(dy_ref, dy_all.at[2], 2),
    ]
    near = [push(gate_ref, gate_all.at[1], 1), push(slot_ref, slot_all.at[1], 1), push(x_ref, x_all.at[1], 1), push(dy_ref, dy_all.at[1], 1)]
    low, top = pl.ds(0, TOK // 2), pl.ds(TOK // 2, TOK // 2)
    second = [
        push(gate_ref, gate_all.at[2], 2), push(slot_ref, slot_all.at[4], 4),
        push(x_ref.at[low], x_all.at[2, low], 2), push(dy_ref.at[low], dy_all.at[4, low], 4),
    ]
    own = [pltpu.make_async_copy(src, dst.at[0], own_sem.at[k]) for k, (src, dst) in enumerate(((x_ref, x_all), (dy_ref, dy_all), (slot_ref, slot_all), (gate_ref, gate_all)))]
    for copy in own:
        copy.start()

    asked[pl.ds(0, 1), :] = req_ref[0, pl.ds(me, 1), :]
    for copy in asks:
        copy.wait_recv()
    asked_out[...] = asked[...]
    to_smem = pltpu.make_async_copy(asked, asked_s, smem_sem)
    to_smem.start()
    to_smem.wait()

    tiles = CHUNK // LANES
    wide_step, pick_step = n_rows + PAD, n_ask + PAD

    def gather(k):
        fetch(k).wait()

        def fill(t, _):
            r = pl.multiple_of(t * 32, 32)
            for j in range(tiles):
                wide[pl.ds(j * wide_step + r, 32), :] = table[k % 2, pl.ds(r, 32), j * LANES:(j + 1) * LANES].astype(F32)
            return 0

        lax.fori_loop(0, n_rows // 32, fill, 0)
        if k + 2 < len(steps):
            fetch(k + 2).start()

        def pick_device(b, _):
            def pick(t, _):
                for u in range(16):
                    row = asked_s[b, t * 16 + u]
                    picked[pl.ds(b * SLOTS + t * 16 + u, tiles, stride=pick_step), :] = wide[pl.ds(row, tiles, stride=wide_step), :]
                return 0

            return lax.fori_loop(0, SLOTS // 16, pick, 0)

        lax.fori_loop(0, N_DEV, pick_device, 0)
        if k >= 2:
            drain_copy(k - 2).wait()

        def drain(t, _):
            r = pl.multiple_of(t * 32, 32)
            for j in range(tiles):
                staged[k % 2, pl.ds(r, 32), j * LANES:(j + 1) * LANES] = picked[pl.ds(j * pick_step + r, 32), :].astype(BF16)
            return 0

        lax.fori_loop(0, n_ask // 32, drain, 0)
        drain_copy(k).start()

    def drain_copy(k):
        _, out, col = steps[k]
        return pltpu.make_async_copy(staged.at[k % 2], out.at[:, pl.ds(col, CHUNK)], out_sem.at[k % 2])

    for k in range(4):
        gather(k)
    for copy in first:
        copy.wait_recv()
    far = [
        push(gate_all.at[4], gate_all.at[6], 2), push(slot_all.at[2], slot_all.at[6], 4),
        push(x_all.at[4], x_all.at[6], 2), push(dy_all.at[2], dy_all.at[6], 4),
    ]
    second += [push(x_ref.at[top], x_all.at[2, top], 2), push(dy_ref.at[top], dy_all.at[4, top], 4)]
    near += [push(gate_all.at[4], gate_all.at[5], 1), push(slot_all.at[2], slot_all.at[3], 1), push(x_all.at[4], x_all.at[5], 1), push(dy_all.at[2], dy_all.at[3], 1)]
    for k in range(4, len(steps)):
        gather(k)
    for copy in far:
        copy.wait_recv()
    near += [push(ref.at[6], ref.at[7], 1) for ref in (gate_all, slot_all, x_all, dy_all)]
    for copy in second:
        copy.wait_recv()
    near += [push(gate_all.at[2], gate_all.at[3], 1), push(slot_all.at[4], slot_all.at[5], 1), push(x_all.at[2], x_all.at[3], 1), push(dy_all.at[4], dy_all.at[5], 1)]
    for copy in near:
        copy.wait_recv()
    for copy in sent:
        copy.wait_send()
    for copy in own:
        copy.wait()
    drain_copy(len(steps) - 2).wait()
    drain_copy(len(steps) - 1).wait()


N_COPIES = 7 + 4 + 4 + 4 + 4 + 2 + 4 + 4 + 4


def block_kernel(core_ref, x_ref, dy_ref, slot_ref, gate_ref, up_ref, down_ref, mine_ref, other_ref, wt_ref, ct_ref, slot_t, w_t, c_t):
    owner = lax.axis_index("ep")
    width = x_ref.shape[2]
    half = width // 2
    dims = (((1,), (1,)), ((), ()))
    up, down = up_ref, down_ref

    def dots(tok, rows):
        full = lax.dot_general(tok.reshape(PAIR, width), rows, dims, preferred_element_type=F32)
        return jnp.concatenate([full[:TOK, :SLOTS], full[TOK:, SLOTS:]], axis=0)

    act, slope = gelu_pair(dots(x_ref[...], up[...]))
    slope = slope * dots(dy_ref[...], down[...])
    local = slot_ref[...].reshape(PAIR, SEL) - owner * SLOTS
    valid = (local >= 0) & (local < SLOTS)
    index = jnp.where(valid, local, 0)
    act = jnp.take_along_axis(act, index, axis=1)
    slope = jnp.take_along_axis(slope, index, axis=1)
    gate = gate_ref[...].reshape(PAIR, SEL)
    w_t[...] = jnp.where(valid, (gate * act).astype(BF16).astype(F32), 0.0).T
    c_t[...] = jnp.where(valid, (gate * slope).astype(BF16).astype(F32), 0.0).T
    slot_t[...] = jnp.where(valid, local, -1).T
    rows = lax.broadcasted_iota(I32, (SLOTS, PAIR), 0)

    def step(s, acc):
        acc_w, acc_c = acc
        hit = rows == slot_t[pl.ds(s, 1), :]
        acc_w += jnp.where(hit, w_t[pl.ds(s, 1), :], 0.0)
        acc_c += jnp.where(hit, c_t[pl.ds(s, 1), :], 0.0)
        return acc_w, acc_c

    zero = jnp.zeros((SLOTS, PAIR), F32)
    acc_w, acc_c = lax.fori_loop(0, SEL, step, (zero, zero), unroll=4)
    for ref, acc in ((wt_ref, acc_w), (ct_ref, acc_c)):
        terms = split3(acc)
        for j in range(2):
            ref[j] = jnp.concatenate([term[:, j * TOK:(j + 1) * TOK] for term in terms], axis=1)
    first_half = lax.broadcasted_iota(I32, (PAIR, 2 * SLOTS), 0) < TOK
    first_cols = lax.broadcasted_iota(I32, (PAIR, 2 * SLOTS), 1) < SLOTS

    def spread(acc):
        both = jnp.concatenate([acc.T, acc.T], axis=1)
        return split3(jnp.where(first_half == first_cols, both, 0.0))

    w_terms, c_terms = spread(acc_w), spread(acc_c)
    core = core_ref[0]
    for col in range(0, half, 512):
        for shift, terms, table in ((0, w_terms, down), (half, c_terms, up)):
            here = pl.ds(pl.multiple_of(core * half + col, 512), 512)
            there = pl.ds(pl.multiple_of((1 - core) * half + col, 512), 512)
            dst = slice(shift + col, shift + col + 512)
            mine_ref[:, dst] = sum(jnp.dot(term, table[:, here], preferred_element_type=F32) for term in terms)
            part = sum(jnp.dot(term, table[:, there], preferred_element_type=F32) for term in terms)
            other_ref[:TOK, dst] = part[TOK:]
            other_ref[TOK:, dst] = part[:TOK]


def row_kernel(asked_ref, near_ref, far_ref, x_ref, out_ref, wide, part):
    n_rows, cols = out_ref.shape
    tiles = cols // LANES
    wide_step, part_step = n_rows + PAD, SLOTS + PAD

    def clear(t, _):
        r = pl.multiple_of(t * 32, 32)
        for j in range(tiles):
            wide[pl.ds(j * wide_step + r, 32), :] = jnp.zeros((32, LANES), F32)
        return 0

    lax.fori_loop(0, n_rows // 32, clear, 0)
    chips = [near_ref.at[2], near_ref.at[0], near_ref.at[1], far_ref.at[0]]
    for q in range(N_DEV):
        tok = x_ref[q * TOK:(q + 1) * TOK, :]
        full = jnp.dot(chips[q // 2][q % 2], jnp.concatenate([tok] * TERMS, axis=0), preferred_element_type=F32)
        for j in range(tiles):
            part[pl.ds(j * part_step, SLOTS), :] = full[:, j * LANES:(j + 1) * LANES]

        def add(t, _):
            rows = [asked_ref[q, t * 16 + u] for u in range(16)]
            sums = [wide[pl.ds(rows[u], tiles, stride=wide_step), :] + part[pl.ds(t * 16 + u, tiles, stride=part_step), :] for u in range(16)]
            for u in range(16):
                wide[pl.ds(rows[u], tiles, stride=wide_step), :] = sums[u]
            return 0

        lax.fori_loop(0, SLOTS // 16, add, 0)

    def drain(t, _):
        r = pl.multiple_of(t * 32, 32)
        for j in range(tiles):
            out_ref[pl.ds(r, 32), j * LANES:(j + 1) * LANES] = wide[pl.ds(j * wide_step + r, 32), :].astype(BF16)
        return 0

    lax.fori_loop(0, n_rows // 32, drain, 0)


def solution(mesh):
    tok_spec = P(('dp', 'ep'))
    table_spec = P('ep')

    def per_device(tokens, slot_ids, request_rows, gate_vals, grad_out, up_local, down_local):
        width = tokens.shape[1]
        rows_owner = up_local.shape[0]
        n_tok = N_DEV * TOK
        half = width // 2
        core = lax.axis_index('ep') % 2
        vmem, anyw = pl.BlockSpec(memory_space=pltpu.VMEM), pl.BlockSpec(memory_space=pl.ANY)
        shape = jax.ShapeDtypeStruct
        x_all, dy_all, slot_all, gate_all, up_rows, down_rows, asked = pl.pallas_call(
            share_kernel,
            in_specs=[vmem] * 5 + [anyw] * 2,
            out_specs=[anyw] * 6 + [vmem],
            out_shape=[shape((N_DEV, TOK, width), BF16)] * 2 + [shape((N_DEV, TOK, SEL), I32), shape((N_DEV, TOK, SEL), F32)]
            + [shape((N_DEV * SLOTS, width), BF16)] * 2 + [shape((N_DEV, SLOTS), I32)],
            scratch_shapes=[
                pltpu.VMEM((N_DEV, SLOTS), I32), pltpu.SMEM((N_DEV, SLOTS), I32),
                pltpu.VMEM((2, rows_owner, CHUNK), BF16),
                pltpu.VMEM((CHUNK // LANES * (rows_owner + PAD), LANES), F32),
                pltpu.VMEM((CHUNK // LANES * (N_DEV * SLOTS + PAD), LANES), F32),
                pltpu.VMEM((2, N_DEV * SLOTS, CHUNK), BF16),
                pltpu.SemaphoreType.DMA((N_COPIES,)), pltpu.SemaphoreType.DMA((N_COPIES,)),
                pltpu.SemaphoreType.DMA((4,)), pltpu.SemaphoreType.DMA,
                pltpu.SemaphoreType.DMA((2,)), pltpu.SemaphoreType.DMA((2,)),
            ],
            compiler_params=pltpu.CompilerParams(collective_id=0, has_side_effects=True, vmem_limit_bytes=VMEM_BYTES),
        )(tokens, grad_out, slot_ids.reshape(TOK, SEL), gate_vals.reshape(TOK, SEL), request_rows, up_local, down_local)

        core_arr = core.reshape(1).astype(I32)

        def blocks(n, chip, mine_at, other_at):
            tok = pl.BlockSpec((2, TOK, width), lambda i, c: (chip(i), 0, 0))
            side = pl.BlockSpec((2, TOK, SEL), lambda i, c: (chip(i), 0, 0))
            table = pl.BlockSpec((2 * SLOTS, width), lambda i, c: (chip(i), 0))
            coef = pl.BlockSpec((None, 2, SLOTS, TERMS * TOK), lambda i, c: (i, 0, 0, 0))
            return pl.pallas_call(
                block_kernel,
                grid_spec=pltpu.PrefetchScalarGridSpec(
                    num_scalar_prefetch=1,
                    grid=(n,),
                    in_specs=[tok, tok, side, side, table, table],
                    out_specs=[pl.BlockSpec((None, PAIR, width), lambda i, c: (mine_at(i, c[0]), 0, 0)),
                               pl.BlockSpec((None, PAIR, width), lambda i, c: (other_at(i, c[0]), 0, 0)), coef, coef],
                    scratch_shapes=[pltpu.VMEM((SEL, PAIR), I32), pltpu.VMEM((SEL, PAIR), F32), pltpu.VMEM((SEL, PAIR), F32)],
                ),
                out_shape=[shape((n, PAIR, width), F32)] * 2 + [shape((n, 2, SLOTS, TERMS * TOK), BF16)] * 2,
                compiler_params=pltpu.CompilerParams(vmem_limit_bytes=VMEM_BYTES),
                cost_estimate=pl.CostEstimate(flops=n * 10 ** 10, bytes_accessed=10 ** 6, transcendentals=0),
            )(core_arr, x_all, dy_all, slot_all, gate_all, up_rows, down_rows)

        def near_slot(i, c):
            return jnp.where(i == 2, 2, i ^ c)

        mine_far, other_far, w_far, c_far = blocks(1, lambda i: i + 3, lambda i, c: i, lambda i, c: i)
        mine, other, w_near, c_near = blocks(3, lambda i: lax.rem(i + 1, 3), near_slot, lambda i, c: near_slot(i, 1 - c))
        partner = [(i, i ^ 1) for i in range(N_DEV)]
        first_hop = [(i, i ^ (2 if i % 2 == 0 else 4)) for i in range(N_DEV)]
        second_hop = [(i, i ^ (4 if i % 2 == 0 else 2)) for i in range(N_DEV)]
        hop = lambda value, pairs: lax.ppermute(value, 'ep', pairs)
        whole = lambda *dims: pl.BlockSpec(dims, lambda i, a: (0,) * len(dims))

        def grad_rows(coef_near, coef_far, tok):
            return pl.pallas_call(
                row_kernel,
                grid_spec=pltpu.PrefetchScalarGridSpec(
                    num_scalar_prefetch=1,
                    grid=(width // CHUNK,),
                    in_specs=[whole(*coef_near.shape), whole(*coef_far.shape), pl.BlockSpec((n_tok, CHUNK), lambda i, a: (0, i))],
                    out_specs=pl.BlockSpec((rows_owner, CHUNK), lambda i, a: (0, i)),
                    scratch_shapes=[pltpu.VMEM((CHUNK // LANES * (rows_owner + PAD), LANES), F32), pltpu.VMEM((CHUNK // LANES * (SLOTS + PAD), LANES), F32)],
                ),
                out_shape=shape((rows_owner, width), BF16),
                compiler_params=pltpu.CompilerParams(vmem_limit_bytes=VMEM_BYTES),
                cost_estimate=pl.CostEstimate(flops=6 * rows_owner * width * n_tok, bytes_accessed=2 * rows_owner * width, transcendentals=0),
            )(asked, coef_near, coef_far, tok.reshape(n_tok, width))

        got_far = hop(other_far, partner)
        got_far, mine = lax.optimization_barrier((got_far, mine))
        got_second = hop(mine_far[0] + got_far[0], first_hop)
        got = hop(other, partner)
        got_own = hop(mine[0] + got[0], first_hop)
        grad_up = grad_rows(c_near, c_far, x_all)
        got_second, grad_up = lax.optimization_barrier((got_second, grad_up))
        got_last = hop(mine[1] + got[1] + got_second, second_hop)
        grad_down = grad_rows(w_near, w_far, dy_all)
        got_last, got_own, grad_down = lax.optimization_barrier((got_last, got_own, grad_down))
        final = (mine[2] + got[2] + got_own + got_last).astype(BF16).reshape(2, TOK, 2, half)
        keep, give = final[0], final[1]
        back = hop(give, partner)
        low = jnp.where(core == 0, keep, back)
        high = jnp.where(core == 0, back, keep)
        token_out = jnp.concatenate([low, high], axis=2)
        return token_out[:, 0], token_out[:, 1], grad_up, grad_down

    return jax.shard_map(per_device, mesh=mesh, in_specs=(tok_spec, tok_spec, tok_spec, tok_spec, tok_spec, table_spec, table_spec), out_specs=(tok_spec, tok_spec, tok_spec, tok_spec), check_vma=False)
```

```python
import functools
import math
import jax
import jax.numpy as jnp
from jax import lax
from jax.experimental import pallas as pl
from jax.experimental.pallas import tpu as pltpu
from jax.sharding import PartitionSpec as P

F32, BF16, I32 = jnp.float32, jnp.bfloat16, jnp.int32
N_DEV, TOK, SLOTS, SEL = 8, 64, 128, 128
PAIR = 2 * TOK
TERMS = 3
CHUNK = 1024
ROW_CHUNK = 2048
LANES = 128
PAD = 4
VMEM_BYTES = 62 * 1024 * 1024
MESH = pl.DeviceIdType.MESH


def gelu_pair(pre_act):
    normal_cdf = 0.5 * (1.0 + lax.erf(pre_act * (2.0 ** -0.5)))
    normal_pdf = jnp.exp(-0.5 * pre_act * pre_act) * ((2.0 * math.pi) ** -0.5)
    return pre_act * normal_cdf, normal_cdf + pre_act * normal_pdf


def split3(wide):
    high = wide.astype(BF16)
    rest = wide - high.astype(F32)
    mid = rest.astype(BF16)
    low = (rest - mid.astype(F32)).astype(BF16)
    return high, mid, low


N_COPIES = 64


def layer_kernel(x_ref, dy_ref, slot_ref, gate_ref, req_ref, up_ref, down_ref,
                 x_out, dy_out, c_out, w_out, asked_out, first_sum, second_sum, own_mine, own_got,
                 x_all, dy_all, slot_all, gate_all, up_rows, down_rows, pair_recv, hop_recv, asked, asked_s, slot_t, w_t, c_t,
                 send_sem, recv_sem, own_sem, smem_sem, in_sem, out_sem):
    me = lax.axis_index("ep")
    core = lax.rem(me, 2)
    n_rows, width = up_ref.shape
    half = width // 2
    steps = [(ref, out, col) for ref, out in ((up_ref, up_rows), (down_ref, down_rows)) for col in range(0, width, CHUNK)]
    tiles = CHUNK // LANES
    wide_step, pick_step = n_rows + PAD, N_DEV * SLOTS + PAD
    sent = []

    def descriptor(k, src, dst, mask):
        view = lambda ref, index: ref if index is None else ref.at[index]
        return pltpu.make_async_remote_copy(src_ref=view(*src), dst_ref=view(*dst), send_sem=send_sem.at[k], recv_sem=recv_sem.at[k],
                                            device_id={"ep": me ^ mask}, device_id_type=MESH)

    def push(src, src_index, dst, dst_index, mask):
        spec = (len(sent), (src, src_index), (dst, dst_index), mask)
        descriptor(*spec).start()
        sent.append(spec)
        return spec

    def arrive(specs):
        for spec in specs:
            descriptor(*spec).wait_recv()

    def leave(specs):
        for spec in specs:
            descriptor(*spec).wait_send()

    own = [pltpu.make_async_copy(src, dst.at[0], own_sem.at[k]) for k, (src, dst) in enumerate(((x_ref, x_all), (dy_ref, dy_all), (slot_ref, slot_all), (gate_ref, gate_all)))]
    barrier = pltpu.get_barrier_semaphore()
    for b in range(1, N_DEV):
        pl.semaphore_signal(barrier, inc=1, device_id={"ep": me ^ b}, device_id_type=MESH)
    for copy in own:
        copy.start()
    pl.semaphore_wait(barrier, N_DEV - 1)

    asks = [push(req_ref, (0, pl.ds(me ^ b, 1)), asked, pl.ds(b, 1), b) for b in range(1, N_DEV)]
    first = [
        push(gate_ref, None, gate_all, 4, 4), push(slot_ref, None, slot_all, 2, 2),
        push(x_ref, None, x_all, 4, 4), push(dy_ref, None, dy_all, 2, 2),
    ]
    near_own = [push(gate_ref, None, gate_all, 1, 1), push(slot_ref, None, slot_all, 1, 1), push(x_ref, None, x_all, 1, 1), push(dy_ref, None, dy_all, 1, 1)]
    low, top = pl.ds(0, TOK // 2), pl.ds(TOK // 2, TOK // 2)
    second = [
        push(gate_ref, None, gate_all, 2, 2), push(slot_ref, None, slot_all, 4, 4),
        push(x_ref, low, x_all, (2, low), 2), push(dy_ref, low, dy_all, (4, low), 4),
    ]
    asked[pl.ds(0, 1), :] = req_ref[0, pl.ds(me, 1), :]
    arrive(asks)
    asked_out[...] = asked[...]
    to_smem = pltpu.make_async_copy(asked, asked_s, smem_sem)
    to_smem.start()
    to_smem.wait()

    def gather_all(table, wide, picked):
        def fetch(k):
            ref, _, col = steps[k]
            return pltpu.make_async_copy(ref.at[:, pl.ds(col, CHUNK)], table.at[k % 2], in_sem.at[k % 2])

        fetch(0).start()
        fetch(1).start()
        for k in range(len(steps)):
            if k == len(steps) // 2:
                arrive(first)
                far = [
                    push(gate_all, 4, gate_all, 6, 2), push(slot_all, 2, slot_all, 6, 4),
                    push(x_all, 4, x_all, 6, 2), push(dy_all, 2, dy_all, 6, 4),
                ]
                second.extend([push(x_ref, top, x_all, (2, top), 2), push(dy_ref, top, dy_all, (4, top), 4)])
                near_first = [push(gate_all, 4, gate_all, 5, 1), push(slot_all, 2, slot_all, 3, 1), push(x_all, 4, x_all, 5, 1), push(dy_all, 2, dy_all, 3, 1)]
            fetch(k).wait()

            def fill(t, _):
                r = pl.multiple_of(t * 32, 32)
                for j in range(tiles):
                    wide[pl.ds(j * wide_step + r, 32), :] = table[k % 2, pl.ds(r, 32), j * LANES:(j + 1) * LANES].astype(F32)
                return 0

            lax.fori_loop(0, n_rows // 32, fill, 0)
            if k + 2 < len(steps):
                fetch(k + 2).start()

            def pick_device(b, _):
                def pick(t, _):
                    for u in range(16):
                        row = asked_s[b, t * 16 + u]
                        picked[pl.ds(b * SLOTS + t * 16 + u, tiles, stride=pick_step), :] = wide[pl.ds(row, tiles, stride=wide_step), :]
                    return 0

                return lax.fori_loop(0, SLOTS // 16, pick, 0)

            lax.fori_loop(0, N_DEV, pick_device, 0)
            _, rows_ref, col = steps[k]

            def drain(t, _):
                r = pl.multiple_of(t * 32, 32)
                for j in range(tiles):
                    rows_ref[pl.ds(r, 32), col + j * LANES:col + (j + 1) * LANES] = picked[pl.ds(j * pick_step + r, 32), :].astype(BF16)
                return 0

            lax.fori_loop(0, N_DEV * SLOTS // 32, drain, 0)
        return far, near_first

    kept = []
    pl.run_scoped(
        lambda *bufs: kept.append(gather_all(*bufs)),
        pltpu.VMEM((2, n_rows, CHUNK), BF16), pltpu.VMEM((tiles * wide_step, LANES), F32), pltpu.VMEM((tiles * pick_step, LANES), F32),
    )
    far, near_first = kept[0]
    for copy in own:
        copy.wait()
    dims = (((1,), (1,)), ((), ()))
    row_iota = lax.broadcasted_iota(I32, (SLOTS, PAIR), 0)
    block_diag = (lax.broadcasted_iota(I32, (PAIR, 2 * SLOTS), 0) < TOK) == (lax.broadcasted_iota(I32, (PAIR, 2 * SLOTS), 1) < SLOTS)

    def block(r, mine, other):
        toks, rows = pl.ds(2 * r, 2), pl.ds(2 * r * SLOTS, 2 * SLOTS)

        def dots(tok, table):
            full = lax.dot_general(tok[toks].reshape(PAIR, width), table[rows, :], dims, preferred_element_type=F32)
            return jnp.concatenate([full[:TOK, :SLOTS], full[TOK:, SLOTS:]], axis=0)

        act, slope = gelu_pair(dots(x_all, up_rows))
        slope = slope * dots(dy_all, down_rows)
        local = slot_all[toks].reshape(PAIR, SEL) - me * SLOTS
        valid = (local >= 0) & (local < SLOTS)
        index = jnp.where(valid, local, 0)
        act = jnp.take_along_axis(act, index, axis=1)
        slope = jnp.take_along_axis(slope, index, axis=1)
        gate = gate_all[toks].reshape(PAIR, SEL)
        w_t[...] = jnp.where(valid, (gate * act).astype(BF16).astype(F32), 0.0).T
        c_t[...] = jnp.where(valid, (gate * slope).astype(BF16).astype(F32), 0.0).T
        slot_t[...] = jnp.where(valid, local, -1).T

        def step(s, acc):
            acc_w, acc_c = acc
            hit = row_iota == slot_t[pl.ds(s, 1), :]
            acc_w += jnp.where(hit, w_t[pl.ds(s, 1), :], 0.0)
            acc_c += jnp.where(hit, c_t[pl.ds(s, 1), :], 0.0)
            return acc_w, acc_c

        zero = jnp.zeros((SLOTS, PAIR), F32)
        acc_w, acc_c = lax.fori_loop(0, SEL, step, (zero, zero), unroll=4)
        for ref, acc in ((w_out, acc_w), (c_out, acc_c)):
            terms = split3(acc)
            for j in range(2):
                ref[2 * r + j] = jnp.concatenate([term[:, j * TOK:(j + 1) * TOK] for term in terms], axis=1)

        def spread(acc):
            both = jnp.concatenate([acc.T, acc.T], axis=1)
            return split3(jnp.where(block_diag, both, 0.0))

        w_terms, c_terms = spread(acc_w), spread(acc_c)
        for col in range(0, half, 512):
            for shift, terms, table in ((0, w_terms, down_rows), (half, c_terms, up_rows)):
                here = pl.ds(pl.multiple_of(core * half + col, 512), 512)
                there = pl.ds(pl.multiple_of((1 - core) * half + col, 512), 512)
                dst = slice(shift + col, shift + col + 512)
                mine[:, dst] = sum(jnp.dot(term, table[rows, here], preferred_element_type=F32) for term in terms)
                part = sum(jnp.dot(term, table[rows, there], preferred_element_type=F32) for term in terms)
                other[:TOK, dst] = part[TOK:]
                other[TOK:, dst] = part[:TOK]

    def add_into(dst, src):
        def add(t, _):
            r = pl.ds(pl.multiple_of(t * 16, 16), 16)
            dst[r, :] = dst[r, :] + src[r, :]
            return 0

        lax.fori_loop(0, PAIR // 16, add, 0)

    def blocks(mine, other):
        save = lambda src, dst, k: pltpu.make_async_copy(src, dst, out_sem.at[k])
        arrive(far)
        near_far = [push(ref, 6, ref, 7, 1) for ref in (gate_all, slot_all, x_all, dy_all)]
        arrive(near_own + near_first + near_far)
        block(3, mine.at[3], other.at[0])
        pair_far = push(other, 0, pair_recv, 0, 1)
        block(0, mine.at[0], other.at[1])
        pair_own = push(other, 1, own_got, None, 1)
        saves = [save(mine.at[0], own_mine, 0)]
        saves[0].start()
        arrive([pair_far])
        add_into(mine.at[3], pair_recv.at[0])
        hop = push(mine, 3, hop_recv, None, 2 + 2 * core)
        arrive(second)
        near_second = [push(gate_all, 2, gate_all, 3, 1), push(slot_all, 4, slot_all, 5, 1), push(x_all, 2, x_all, 3, 1), push(dy_all, 4, dy_all, 5, 1)]
        arrive(near_second)
        for k, (src, dst) in enumerate(((x_all, x_out), (dy_all, dy_out))):
            saves.append(save(src, dst, 1 + k))
            saves[-1].start()
        leave([pair_far])
        block(1, mine.at[1], other.at[0])
        pair_x = push(other, 0, pair_recv, 1, 1)
        leave([pair_own])
        block(2, mine.at[2], other.at[1])
        pair_y = push(other, 1, pair_recv, 2, 1)
        arrive([pair_x])
        add_into(mine.at[1], pair_recv.at[1])
        arrive([pair_y])
        add_into(mine.at[2], pair_recv.at[2])
        saves.append(save(mine.at[1 + core], first_sum, 3))
        saves[-1].start()
        arrive([hop])
        add_into(mine.at[2 - core], hop_recv)
        saves.append(save(mine.at[2 - core], second_sum, 4))
        saves[-1].start()
        arrive([pair_own])
        leave([spec for spec in sent if spec is not pair_far and spec is not pair_own])
        for copy in saves:
            copy.wait()

    pl.run_scoped(blocks, pltpu.VMEM((4, PAIR, width), F32), pltpu.VMEM((2, PAIR, width), F32))


def row_kernel(asked_ref, coef_ref, x_ref, out_ref, wide, part):
    n_rows, cols = out_ref.shape
    tiles = cols // LANES
    wide_step, part_step = n_rows + PAD, SLOTS + PAD

    def clear(t, _):
        r = pl.multiple_of(t * 32, 32)
        for j in range(tiles):
            wide[pl.ds(j * wide_step + r, 32), :] = jnp.zeros((32, LANES), F32)
        return 0

    lax.fori_loop(0, n_rows // 32, clear, 0)
    for q in range(N_DEV):
        tok = x_ref[q * TOK:(q + 1) * TOK, :]
        full = jnp.dot(coef_ref[q], jnp.concatenate([tok] * TERMS, axis=0), preferred_element_type=F32)
        for j in range(tiles):
            part[pl.ds(j * part_step, SLOTS), :] = full[:, j * LANES:(j + 1) * LANES]

        def add(t, _):
            rows = [asked_ref[q, t * 16 + u] for u in range(16)]
            sums = [wide[pl.ds(rows[u], tiles, stride=wide_step), :] + part[pl.ds(t * 16 + u, tiles, stride=part_step), :] for u in range(16)]
            for u in range(16):
                wide[pl.ds(rows[u], tiles, stride=wide_step), :] = sums[u]
            return 0

        lax.fori_loop(0, SLOTS // 16, add, 0)

    def drain(t, _):
        r = pl.multiple_of(t * 32, 32)
        for j in range(tiles):
            out_ref[pl.ds(r, 32), j * LANES:(j + 1) * LANES] = wide[pl.ds(j * wide_step + r, 32), :].astype(BF16)
        return 0

    lax.fori_loop(0, n_rows // 32, drain, 0)


def solution(mesh):
    tok_spec = P(('dp', 'ep'))
    table_spec = P('ep')

    def per_device(tokens, slot_ids, request_rows, gate_vals, grad_out, up_local, down_local):
        width = tokens.shape[1]
        rows_owner = up_local.shape[0]
        n_tok = N_DEV * TOK
        half = width // 2
        core = lax.axis_index('ep') % 2
        vmem, anyw = pl.BlockSpec(memory_space=pltpu.VMEM), pl.BlockSpec(memory_space=pl.ANY)
        shape = jax.ShapeDtypeStruct
        sums = shape((PAIR, width), F32)
        x_all, dy_all, c_terms, w_terms, asked, first_sum, second_sum, own_mine, own_got = pl.pallas_call(
            layer_kernel,
            in_specs=[anyw, anyw, vmem, vmem, vmem, anyw, anyw],
            out_specs=[anyw] * 2 + [vmem] * 3 + [anyw] * 4,
            out_shape=[shape((N_DEV, TOK, width), BF16)] * 2 + [shape((N_DEV, SLOTS, TERMS * TOK), BF16)] * 2 + [shape((N_DEV, SLOTS), I32)] + [sums] * 4,
            scratch_shapes=[
                pltpu.VMEM((N_DEV, TOK, width), BF16), pltpu.VMEM((N_DEV, TOK, width), BF16),
                pltpu.VMEM((N_DEV, TOK, SEL), I32), pltpu.VMEM((N_DEV, TOK, SEL), F32),
                pltpu.VMEM((N_DEV * SLOTS, width), BF16), pltpu.VMEM((N_DEV * SLOTS, width), BF16),
                pltpu.VMEM((3, PAIR, width), F32), pltpu.VMEM((PAIR, width), F32),
                pltpu.VMEM((N_DEV, SLOTS), I32), pltpu.SMEM((N_DEV, SLOTS), I32),
                pltpu.VMEM((SEL, PAIR), I32), pltpu.VMEM((SEL, PAIR), F32), pltpu.VMEM((SEL, PAIR), F32),
                pltpu.SemaphoreType.DMA((N_COPIES,)), pltpu.SemaphoreType.DMA((N_COPIES,)),
                pltpu.SemaphoreType.DMA((4,)), pltpu.SemaphoreType.DMA,
                pltpu.SemaphoreType.DMA((2,)), pltpu.SemaphoreType.DMA((5,)),
            ],
            compiler_params=pltpu.CompilerParams(collective_id=0, has_side_effects=True, vmem_limit_bytes=VMEM_BYTES),
        )(tokens, grad_out, slot_ids.reshape(TOK, SEL), gate_vals.reshape(TOK, SEL), request_rows, up_local, down_local)

        partner = [(i, i ^ 1) for i in range(N_DEV)]
        first_hop = [(i, i ^ (2 if i % 2 == 0 else 4)) for i in range(N_DEV)]
        second_hop = [(i, i ^ (4 if i % 2 == 0 else 2)) for i in range(N_DEV)]
        hop = lambda value, pairs: lax.ppermute(value, 'ep', pairs)

        def grad_rows(coef, tok):
            return pl.pallas_call(
                row_kernel,
                grid_spec=pltpu.PrefetchScalarGridSpec(
                    num_scalar_prefetch=1,
                    grid=(width // ROW_CHUNK,),
                    in_specs=[pl.BlockSpec(coef.shape, lambda i, a: (0, 0, 0)), pl.BlockSpec((n_tok, ROW_CHUNK), lambda i, a: (0, i))],
                    out_specs=pl.BlockSpec((rows_owner, ROW_CHUNK), lambda i, a: (0, i)),
                    scratch_shapes=[pltpu.VMEM((ROW_CHUNK // LANES * (rows_owner + PAD), LANES), F32), pltpu.VMEM((ROW_CHUNK // LANES * (SLOTS + PAD), LANES), F32)],
                ),
                out_shape=shape((rows_owner, width), BF16),
                compiler_params=pltpu.CompilerParams(vmem_limit_bytes=VMEM_BYTES),
                cost_estimate=pl.CostEstimate(flops=6 * rows_owner * width * n_tok, bytes_accessed=2 * rows_owner * width, transcendentals=0),
            )(asked, coef, tok.reshape(n_tok, width))

        got_own = hop(first_sum, first_hop)
        got_last = hop(second_sum, second_hop)
        grad_up = grad_rows(c_terms, x_all)
        grad_down = grad_rows(w_terms, dy_all)
        got_last, got_own, grad_up, grad_down = lax.optimization_barrier((got_last, got_own, grad_up, grad_down))
        final = (own_mine + own_got + got_own + got_last).astype(BF16).reshape(2, TOK, 2, half)
        keep, give = final[0], final[1]
        back = hop(give, partner)
        low = jnp.where(core == 0, keep, back)
        high = jnp.where(core == 0, back, keep)
        token_out = jnp.concatenate([low, high], axis=2)
        return token_out[:, 0], token_out[:, 1], grad_up, grad_down

    return jax.shard_map(per_device, mesh=mesh, in_specs=(tok_spec, tok_spec, tok_spec, tok_spec, tok_spec, table_spec, table_spec), out_specs=(tok_spec, tok_spec, tok_spec, tok_spec), check_vma=False)
```

```python
import functools
import math
import jax
import jax.numpy as jnp
from jax import lax
from jax.experimental import pallas as pl
from jax.experimental.pallas import tpu as pltpu
from jax.sharding import PartitionSpec as P

F32, BF16, I32 = jnp.float32, jnp.bfloat16, jnp.int32
N_DEV, TOK, SLOTS, SEL = 8, 64, 128, 128
PAIR = 2 * TOK
TERMS = 3
CHUNK = 1024
ROW_CHUNK = 2048
LANES = 128
PAD = 4
VMEM_BYTES = 62 * 1024 * 1024
MESH = pl.DeviceIdType.MESH


def gelu_pair(pre_act):
    normal_cdf = 0.5 * (1.0 + lax.erf(pre_act * (2.0 ** -0.5)))
    normal_pdf = jnp.exp(-0.5 * pre_act * pre_act) * ((2.0 * math.pi) ** -0.5)
    return pre_act * normal_cdf, normal_cdf + pre_act * normal_pdf


def split3(wide):
    high = wide.astype(BF16)
    rest = wide - high.astype(F32)
    mid = rest.astype(BF16)
    low = (rest - mid.astype(F32)).astype(BF16)
    return high, mid, low


N_COPIES = 64
SIDE_STEP, FAR_STEP, REST_STEP = 1, 4, 6
COLS = 512


def layer_kernel(x_ref, dy_ref, slot_ref, gate_ref, req_ref, up_ref, down_ref,
                 x_out, dy_out, c_out, w_out, asked_out, first_sum, second_sum, own_sum,
                 x_all, dy_all, slot_all, gate_all, up_rows, down_rows, pair_recv, hop_recv, asked, asked_s, slot_t, w_t, c_t,
                 send_sem, recv_sem, own_sem, smem_sem, in_sem, out_sem):
    me = lax.axis_index("ep")
    core = lax.rem(me, 2)
    n_rows, width = up_ref.shape
    half = width // 2
    steps = [(ref, out, col) for ref, out in ((up_ref, up_rows), (down_ref, down_rows)) for col in range(0, width, CHUNK)]
    tiles = CHUNK // LANES
    wide_step, pick_step = n_rows + PAD, N_DEV * SLOTS + PAD
    sent = []

    def descriptor(k, src, dst, mask):
        view = lambda ref, index: ref if index is None else ref.at[index]
        return pltpu.make_async_remote_copy(src_ref=view(*src), dst_ref=view(*dst), send_sem=send_sem.at[k], recv_sem=recv_sem.at[k],
                                            device_id={"ep": me ^ mask}, device_id_type=MESH)

    def push(src, src_index, dst, dst_index, mask):
        spec = (len(sent), (src, src_index), (dst, dst_index), mask)
        descriptor(*spec).start()
        sent.append(spec)
        return spec

    def arrive(specs):
        for spec in specs:
            descriptor(*spec).wait_recv()

    def leave(specs):
        for spec in specs:
            descriptor(*spec).wait_send()

    own = [pltpu.make_async_copy(src, dst.at[0], own_sem.at[k]) for k, (src, dst) in enumerate(((x_ref, x_all), (dy_ref, dy_all)))]
    slot_all[0] = slot_ref[...].reshape(SEL, TOK).T
    gate_all[0] = gate_ref[...].reshape(SEL, TOK).T
    barrier = pltpu.get_barrier_semaphore()
    for b in range(1, N_DEV):
        pl.semaphore_signal(barrier, inc=1, device_id={"ep": me ^ b}, device_id_type=MESH)
    for copy in own:
        copy.start()
    pl.semaphore_wait(barrier, N_DEV - 1)

    asks = [push(req_ref, (0, pl.ds(me ^ b, 1)), asked, pl.ds(b, 1), b) for b in range(1, N_DEV)]
    first = [push(x_ref, None, x_all, 4, 4), push(dy_ref, None, dy_all, 2, 2)]
    near_own = [push(x_ref, None, x_all, 1, 1), push(dy_ref, None, dy_all, 1, 1)]
    low, top = pl.ds(0, TOK // 2), pl.ds(TOK // 2, TOK // 2)
    second = [push(x_ref, low, x_all, (2, low), 2), push(dy_ref, low, dy_all, (4, low), 4)]
    asked[pl.ds(0, 1), :] = req_ref[0, pl.ds(me, 1), :]
    arrive(asks)
    asked_out[...] = asked[...]
    to_smem = pltpu.make_async_copy(asked, asked_s, smem_sem)
    to_smem.start()
    to_smem.wait()

    def gather_all(table, wide, picked):
        def fetch(k):
            ref, _, col = steps[k]
            return pltpu.make_async_copy(ref.at[:, pl.ds(col, CHUNK)], table.at[k % 2], in_sem.at[k % 2])

        fetch(0).start()
        fetch(1).start()
        for k in range(len(steps)):
            if k == SIDE_STEP:
                side = [push(gate_all, 0, gate_all, 4, 4), push(slot_all, 0, slot_all, 2, 2)]
                near_own.extend([push(gate_all, 0, gate_all, 1, 1), push(slot_all, 0, slot_all, 1, 1)])
            if k == FAR_STEP:
                arrive(first)
                far = [push(x_all, 4, x_all, 6, 2), push(dy_all, 2, dy_all, 6, 4)]
                near_first = [push(x_all, 4, x_all, 5, 1), push(dy_all, 2, dy_all, 3, 1)]
            if k == REST_STEP:
                arrive(side)
                far.extend([push(gate_all, 4, gate_all, 6, 2), push(slot_all, 2, slot_all, 6, 4)])
                near_first.extend([push(gate_all, 4, gate_all, 5, 1), push(slot_all, 2, slot_all, 3, 1)])
                second.extend([push(gate_all, 0, gate_all, 2, 2), push(slot_all, 0, slot_all, 4, 4)])
                second.extend([push(x_ref, top, x_all, (2, top), 2), push(dy_ref, top, dy_all, (4, top), 4)])
            fetch(k).wait()

            def fill(t, _):
                r = pl.multiple_of(t * 32, 32)
                for j in range(tiles):
                    wide[pl.ds(j * wide_step + r, 32), :] = table[k % 2, pl.ds(r, 32), j * LANES:(j + 1) * LANES].astype(F32)
                return 0

            lax.fori_loop(0, n_rows // 32, fill, 0)
            if k + 2 < len(steps):
                fetch(k + 2).start()

            def pick_device(b, _):
                def pick(t, _):
                    for u in range(16):
                        row = asked_s[b, t * 16 + u]
                        picked[pl.ds(b * SLOTS + t * 16 + u, tiles, stride=pick_step), :] = wide[pl.ds(row, tiles, stride=wide_step), :]
                    return 0

                return lax.fori_loop(0, SLOTS // 16, pick, 0)

            lax.fori_loop(0, N_DEV, pick_device, 0)
            _, rows_ref, col = steps[k]

            def drain(t, _):
                r = pl.multiple_of(t * 32, 32)
                for j in range(tiles):
                    rows_ref[pl.ds(r, 32), col + j * LANES:col + (j + 1) * LANES] = picked[pl.ds(j * pick_step + r, 32), :].astype(BF16)
                return 0

            lax.fori_loop(0, N_DEV * SLOTS // 32, drain, 0)
        return far, near_first

    kept = []
    pl.run_scoped(
        lambda *bufs: kept.append(gather_all(*bufs)),
        pltpu.VMEM((2, n_rows, CHUNK), BF16), pltpu.VMEM((tiles * wide_step, LANES), F32), pltpu.VMEM((tiles * pick_step, LANES), F32),
    )
    far, near_first = kept[0]
    for copy in own:
        copy.wait()
    dims = (((1,), (1,)), ((), ()))
    row_iota = lax.broadcasted_iota(I32, (SLOTS, PAIR), 0)
    block_diag = (lax.broadcasted_iota(I32, (PAIR, 2 * SLOTS), 0) < TOK) == (lax.broadcasted_iota(I32, (PAIR, 2 * SLOTS), 1) < SLOTS)

    def front(r):
        toks, rows = pl.ds(2 * r, 2), pl.ds(2 * r * SLOTS, 2 * SLOTS)

        def dots(tok, table):
            full = lax.dot_general(tok[toks].reshape(PAIR, width), table[rows, :], dims, preferred_element_type=F32)
            return jnp.concatenate([full[:TOK, :SLOTS], full[TOK:, SLOTS:]], axis=0)

        act, slope = gelu_pair(dots(x_all, up_rows))
        slope = slope * dots(dy_all, down_rows)
        local = slot_all[toks].reshape(PAIR, SEL) - me * SLOTS
        valid = (local >= 0) & (local < SLOTS)
        index = jnp.where(valid, local, 0)
        act = jnp.take_along_axis(act, index, axis=1)
        slope = jnp.take_along_axis(slope, index, axis=1)
        gate = gate_all[toks].reshape(PAIR, SEL)
        w_t[...] = jnp.where(valid, (gate * act).astype(BF16).astype(F32), 0.0).T
        c_t[...] = jnp.where(valid, (gate * slope).astype(BF16).astype(F32), 0.0).T
        slot_t[...] = jnp.where(valid, local, -1).T

        def step(s, acc):
            acc_w, acc_c = acc
            hit = row_iota == slot_t[pl.ds(s, 1), :]
            acc_w += jnp.where(hit, w_t[pl.ds(s, 1), :], 0.0)
            acc_c += jnp.where(hit, c_t[pl.ds(s, 1), :], 0.0)
            return acc_w, acc_c

        zero = jnp.zeros((SLOTS, PAIR), F32)
        acc_w, acc_c = lax.fori_loop(0, SEL, step, (zero, zero), unroll=4)
        for ref, acc in ((w_out, acc_w), (c_out, acc_c)):
            terms = split3(acc)
            for j in range(2):
                ref[2 * r + j] = jnp.concatenate([term[:, j * TOK:(j + 1) * TOK] for term in terms], axis=1)

        def spread(acc):
            both = jnp.concatenate([acc.T, acc.T], axis=1)
            return split3(jnp.where(block_diag, both, 0.0))

        return spread(acc_w), spread(acc_c)

    def columns(r, terms, col, mine, other):
        rows = pl.ds(2 * r * SLOTS, 2 * SLOTS)
        table, terms = (down_rows, terms[0]) if col < half else (up_rows, terms[1])
        here = pl.ds(pl.multiple_of(core * half + col % half, COLS), COLS)
        there = pl.ds(pl.multiple_of((1 - core) * half + col % half, COLS), COLS)
        mine[:, col:col + COLS] = sum(jnp.dot(term, table[rows, here], preferred_element_type=F32) for term in terms)
        part = sum(jnp.dot(term, table[rows, there], preferred_element_type=F32) for term in terms)
        other[:TOK, col:col + COLS] = part[TOK:]
        other[TOK:, col:col + COLS] = part[:TOK]

    def block(r, mine, other):
        terms = front(r)
        for col in range(0, width, COLS):
            columns(r, terms, col, mine, other)

    def add_into(dst, src, cols=slice(None), step=16):
        def add(t, _):
            r = pl.ds(pl.multiple_of(t * step, step), step)
            dst[r, cols] = dst[r, cols] + src[r, cols]
            return 0

        lax.fori_loop(0, PAIR // step, add, 0)

    def blocks(mine, other):
        save = lambda src, dst, k: pltpu.make_async_copy(src, dst, out_sem.at[k])
        arrive(far)
        near_far = [push(ref, 6, ref, 7, 1) for ref in (gate_all, slot_all, x_all, dy_all)]
        arrive(near_own + near_first + near_far)
        terms = front(3)
        pair_far, hop = [], []
        chunks = [pl.ds(col, COLS) for col in range(0, width, COLS)]
        every = slice(None)
        for cols in chunks:
            columns(3, terms, cols.start, mine.at[3], other.at[0])
            pair_far.append(push(other, (0, every, cols), pair_recv, (0, every, cols), 1))
        for k, cols in enumerate(chunks):
            arrive([pair_far[k]])
            add_into(mine.at[3], pair_recv.at[0], cols, 64)
            hop.append(push(mine, (3, every, cols), hop_recv, (every, cols), 2 + 2 * core))
        block(0, mine.at[0], other.at[1])
        pair_own = push(other, 1, pair_recv, 3, 1)
        saves = []
        arrive(second)
        near_second = [push(gate_all, 2, gate_all, 3, 1), push(slot_all, 4, slot_all, 5, 1), push(x_all, 2, x_all, 3, 1), push(dy_all, 4, dy_all, 5, 1)]
        arrive(near_second)
        for k, (src, dst) in enumerate(((x_all, x_out), (dy_all, dy_out))):
            saves.append(save(src, dst, 1 + k))
            saves[-1].start()
        leave(pair_far)
        block(1, mine.at[1], other.at[0])
        pair_x = push(other, 0, pair_recv, 1, 1)
        leave([pair_own])
        block(2, mine.at[2], other.at[1])
        pair_y = push(other, 1, pair_recv, 2, 1)
        arrive([pair_x])
        add_into(mine.at[1], pair_recv.at[1])
        arrive([pair_y])
        add_into(mine.at[2], pair_recv.at[2])
        saves.append(save(mine.at[1 + core], first_sum, 3))
        saves[-1].start()
        arrive([pair_own])
        add_into(mine.at[0], pair_recv.at[3])
        saves.append(save(mine.at[0], own_sum, 0))
        saves[-1].start()
        for k, cols in enumerate(chunks):
            arrive([hop[k]])
            add_into(mine.at[2 - core], hop_recv, cols, 64)
        saves.append(save(mine.at[2 - core], second_sum, 4))
        saves[-1].start()
        leave([spec for spec in sent if spec not in pair_far and spec is not pair_own])
        for copy in saves:
            copy.wait()

    pl.run_scoped(blocks, pltpu.VMEM((4, PAIR, width), F32), pltpu.VMEM((2, PAIR, width), F32))


def row_kernel(asked_ref, coef_ref, x_ref, out_ref, wide, part):
    n_rows, cols = out_ref.shape
    tiles = cols // LANES
    wide_step, part_step = n_rows + PAD, SLOTS + PAD

    def clear(t, _):
        r = pl.multiple_of(t * 32, 32)
        for j in range(tiles):
            wide[pl.ds(j * wide_step + r, 32), :] = jnp.zeros((32, LANES), F32)
        return 0

    lax.fori_loop(0, n_rows // 32, clear, 0)
    for q in range(N_DEV):
        tok = x_ref[q * TOK:(q + 1) * TOK, :]
        full = jnp.dot(coef_ref[q], jnp.concatenate([tok] * TERMS, axis=0), preferred_element_type=F32)
        for j in range(tiles):
            part[pl.ds(j * part_step, SLOTS), :] = full[:, j * LANES:(j + 1) * LANES]

        def add(t, _):
            rows = [asked_ref[q, t * 16 + u] for u in range(16)]
            sums = [wide[pl.ds(rows[u], tiles, stride=wide_step), :] + part[pl.ds(t * 16 + u, tiles, stride=part_step), :] for u in range(16)]
            for u in range(16):
                wide[pl.ds(rows[u], tiles, stride=wide_step), :] = sums[u]
            return 0

        lax.fori_loop(0, SLOTS // 16, add, 0)

    def drain(t, _):
        r = pl.multiple_of(t * 32, 32)
        for j in range(tiles):
            out_ref[pl.ds(r, 32), j * LANES:(j + 1) * LANES] = wide[pl.ds(j * wide_step + r, 32), :].astype(BF16)
        return 0

    lax.fori_loop(0, n_rows // 32, drain, 0)


def solution(mesh):
    tok_spec = P(('dp', 'ep'))
    table_spec = P('ep')

    def per_device(tokens, slot_ids, request_rows, gate_vals, grad_out, up_local, down_local):
        width = tokens.shape[1]
        rows_owner = up_local.shape[0]
        n_tok = N_DEV * TOK
        half = width // 2
        core = lax.axis_index('ep') % 2
        vmem, anyw = pl.BlockSpec(memory_space=pltpu.VMEM), pl.BlockSpec(memory_space=pl.ANY)
        shape = jax.ShapeDtypeStruct
        sums = shape((PAIR, width), F32)
        x_all, dy_all, c_terms, w_terms, asked, first_sum, second_sum, own_sum = pl.pallas_call(
            layer_kernel,
            in_specs=[anyw, anyw, vmem, vmem, vmem, anyw, anyw],
            out_specs=[anyw] * 2 + [vmem] * 3 + [anyw] * 3,
            out_shape=[shape((N_DEV, TOK, width), BF16)] * 2 + [shape((N_DEV, SLOTS, TERMS * TOK), BF16)] * 2 + [shape((N_DEV, SLOTS), I32)] + [sums] * 3,
            scratch_shapes=[
                pltpu.VMEM((N_DEV, TOK, width), BF16), pltpu.VMEM((N_DEV, TOK, width), BF16),
                pltpu.VMEM((N_DEV, TOK, SEL), I32), pltpu.VMEM((N_DEV, TOK, SEL), F32),
                pltpu.VMEM((N_DEV * SLOTS, width), BF16), pltpu.VMEM((N_DEV * SLOTS, width), BF16),
                pltpu.VMEM((4, PAIR, width), F32), pltpu.VMEM((PAIR, width), F32),
                pltpu.VMEM((N_DEV, SLOTS), I32), pltpu.SMEM((N_DEV, SLOTS), I32),
                pltpu.VMEM((SEL, PAIR), I32), pltpu.VMEM((SEL, PAIR), F32), pltpu.VMEM((SEL, PAIR), F32),
                pltpu.SemaphoreType.DMA((N_COPIES,)), pltpu.SemaphoreType.DMA((N_COPIES,)),
                pltpu.SemaphoreType.DMA((2,)), pltpu.SemaphoreType.DMA,
                pltpu.SemaphoreType.DMA((2,)), pltpu.SemaphoreType.DMA((5,)),
            ],
            compiler_params=pltpu.CompilerParams(collective_id=0, has_side_effects=True, vmem_limit_bytes=VMEM_BYTES),
        )(tokens, grad_out, slot_ids.transpose(1, 2, 0), gate_vals.transpose(1, 2, 0), request_rows, up_local, down_local)

        partner = [(i, i ^ 1) for i in range(N_DEV)]
        first_hop = [(i, i ^ (2 if i % 2 == 0 else 4)) for i in range(N_DEV)]
        second_hop = [(i, i ^ (4 if i % 2 == 0 else 2)) for i in range(N_DEV)]
        hop = lambda value, pairs: lax.ppermute(value, 'ep', pairs)

        def grad_rows(coef, tok):
            return pl.pallas_call(
                row_kernel,
                grid_spec=pltpu.PrefetchScalarGridSpec(
                    num_scalar_prefetch=1,
                    grid=(width // ROW_CHUNK,),
                    in_specs=[pl.BlockSpec(coef.shape, lambda i, a: (0, 0, 0)), pl.BlockSpec((n_tok, ROW_CHUNK), lambda i, a: (0, i))],
                    out_specs=pl.BlockSpec((rows_owner, ROW_CHUNK), lambda i, a: (0, i)),
                    scratch_shapes=[pltpu.VMEM((ROW_CHUNK // LANES * (rows_owner + PAD), LANES), F32), pltpu.VMEM((ROW_CHUNK // LANES * (SLOTS + PAD), LANES), F32)],
                ),
                out_shape=shape((rows_owner, width), BF16),
                compiler_params=pltpu.CompilerParams(vmem_limit_bytes=VMEM_BYTES),
                cost_estimate=pl.CostEstimate(flops=6 * rows_owner * width * n_tok, bytes_accessed=2 * rows_owner * width, transcendentals=0),
            )(asked, coef, tok.reshape(n_tok, width))

        got_own = hop(first_sum, first_hop)
        got_last = hop(second_sum, second_hop)
        grad_up = grad_rows(c_terms, x_all)
        grad_down = grad_rows(w_terms, dy_all)
        got_last, got_own, grad_up, grad_down = lax.optimization_barrier((got_last, got_own, grad_up, grad_down))
        keep, give = [(own_sum[rows] + got_own[rows] + got_last[rows]).astype(BF16).reshape(TOK, 2, half) for rows in (slice(0, TOK), slice(TOK, PAIR))]
        back = hop(give, partner)
        low = jnp.where(core == 0, keep, back)
        high = jnp.where(core == 0, back, keep)
        token_out = jnp.concatenate([low, high], axis=2)
        return token_out[:, 0], token_out[:, 1], grad_up, grad_down

    return jax.shard_map(per_device, mesh=mesh, in_specs=(tok_spec, tok_spec, tok_spec, tok_spec, tok_spec, table_spec, table_spec), out_specs=(tok_spec, tok_spec, tok_spec, tok_spec), check_vma=False)
```

```python
import functools
import math
import jax
import jax.numpy as jnp
from jax import lax
from jax.experimental import pallas as pl
from jax.experimental.pallas import tpu as pltpu
from jax.sharding import PartitionSpec as P

F32, BF16, I32 = jnp.float32, jnp.bfloat16, jnp.int32
N_DEV, TOK, SLOTS, SEL = 8, 64, 128, 128
PAIR = 2 * TOK
TERMS = 3
CHUNK = 2048
ROW_CHUNK = 2048
LOW = 16
LANES = 128
PAD = 4
VMEM_BYTES = 62 * 1024 * 1024
MESH = pl.DeviceIdType.MESH


def gelu_pair(pre_act):
    normal_cdf = 0.5 * (1.0 + lax.erf(pre_act * (2.0 ** -0.5)))
    normal_pdf = jnp.exp(-0.5 * pre_act * pre_act) * ((2.0 * math.pi) ** -0.5)
    return pre_act * normal_cdf, normal_cdf + pre_act * normal_pdf


def split3(wide):
    high = wide.astype(BF16)
    rest = wide - high.astype(F32)
    mid = rest.astype(BF16)
    low = (rest - mid.astype(F32)).astype(BF16)
    return high, mid, low


N_COPIES = 64
SIDE_STEP, FAR_STEP, REST_STEP = 1, 4, 6
COLS = 512


def layer_kernel(x_ref, dy_ref, slot_ref, gate_ref, req_ref, up_ref, down_ref,
                 x_out, dy_out, c_out, w_out, asked_out, first_sum, second_sum, own_sum,
                 x_all, dy_all, slot_all, gate_all, up_rows, down_rows, pair_recv, hop_recv, asked, asked_s, slot_t, w_t, c_t,
                 send_sem, recv_sem, own_sem, smem_sem, in_sem, out_sem):
    me = lax.axis_index("ep")
    core = lax.rem(me, 2)
    n_rows, width = up_ref.shape
    half = width // 2
    steps = [(ref, out, col) for ref, out in ((up_ref, up_rows), (down_ref, down_rows)) for col in range(0, width, CHUNK)]
    tiles = CHUNK // LANES
    wide_step, pick_step = n_rows + PAD, SLOTS + PAD
    sent = []

    def descriptor(k, src, dst, mask):
        view = lambda ref, index: ref if index is None else ref.at[index]
        return pltpu.make_async_remote_copy(src_ref=view(*src), dst_ref=view(*dst), send_sem=send_sem.at[k], recv_sem=recv_sem.at[k],
                                            device_id={"ep": me ^ mask}, device_id_type=MESH)

    def push(src, src_index, dst, dst_index, mask):
        spec = (len(sent), (src, src_index), (dst, dst_index), mask)
        descriptor(*spec).start()
        sent.append(spec)
        return spec

    def arrive(specs):
        for spec in specs:
            descriptor(*spec).wait_recv()

    def leave(specs):
        for spec in specs:
            descriptor(*spec).wait_send()

    own = [pltpu.make_async_copy(src, dst.at[0], own_sem.at[k]) for k, (src, dst) in enumerate(((x_ref, x_all), (dy_ref, dy_all)))]
    slot_all[0] = slot_ref[...].reshape(SEL, TOK).T
    gate_all[0] = gate_ref[...].reshape(SEL, TOK).T
    barrier = pltpu.get_barrier_semaphore()
    for b in range(1, N_DEV):
        pl.semaphore_signal(barrier, inc=1, device_id={"ep": me ^ b}, device_id_type=MESH)
    for copy in own:
        copy.start()
    pl.semaphore_wait(barrier, N_DEV - 1)

    asks = [push(req_ref, (0, pl.ds(me ^ b, 1)), asked, pl.ds(b, 1), b) for b in range(1, N_DEV)]
    first = [push(x_ref, None, x_all, 4, 4), push(dy_ref, None, dy_all, 2, 2)]
    near_own = [push(x_ref, None, x_all, 1, 1), push(dy_ref, None, dy_all, 1, 1)]
    low, top = pl.ds(0, LOW), pl.ds(LOW, TOK - LOW)
    second = [push(x_ref, low, x_all, (2, low), 2), push(dy_ref, low, dy_all, (4, low), 4)]
    asked[pl.ds(0, 1), :] = req_ref[0, pl.ds(me, 1), :]
    arrive(asks)
    asked_out[...] = asked[...]
    to_smem = pltpu.make_async_copy(asked, asked_s, smem_sem)
    to_smem.start()
    to_smem.wait()

    def gather_all(table, wide, picked):
        def fetch(k):
            ref, _, col = steps[k]
            return pltpu.make_async_copy(ref.at[:, pl.ds(col, CHUNK)], table, in_sem.at[0])

        fetch(0).start()
        for sub in range(2 * len(steps)):
            if sub == SIDE_STEP:
                side = [push(gate_all, 0, gate_all, 4, 4), push(slot_all, 0, slot_all, 2, 2)]
                near_own.extend([push(gate_all, 0, gate_all, 1, 1), push(slot_all, 0, slot_all, 1, 1)])
            if sub == FAR_STEP:
                arrive(first)
                far = [push(x_all, 4, x_all, 6, 2), push(dy_all, 2, dy_all, 6, 4)]
                near_first = [push(x_all, 4, x_all, 5, 1), push(dy_all, 2, dy_all, 3, 1)]
            if sub == REST_STEP:
                arrive(side)
                far.extend([push(gate_all, 4, gate_all, 6, 2), push(slot_all, 2, slot_all, 6, 4)])
                near_first.extend([push(gate_all, 4, gate_all, 5, 1), push(slot_all, 2, slot_all, 3, 1)])
                second.extend([push(gate_all, 0, gate_all, 2, 2), push(slot_all, 0, slot_all, 4, 4)])
                second.extend([push(x_ref, top, x_all, (2, top), 2), push(dy_ref, top, dy_all, (4, top), 4)])
            k = sub // 2
            if sub % 2 == 0:
                fetch(k).wait()

                def fill(t, _):
                    r = pl.multiple_of(t * 32, 32)
                    for j in range(tiles):
                        wide[pl.ds(j * wide_step + r, 32), :] = table[pl.ds(r, 32), j * LANES:(j + 1) * LANES].astype(F32)
                    return 0

                lax.fori_loop(0, n_rows // 32, fill, 0)
                if k + 1 < len(steps):
                    fetch(k + 1).start()
            else:
                _, rows_ref, col = steps[k]

                def pick_device(b, _):
                    def pick(t, _):
                        for u in range(16):
                            row = asked_s[b, t * 16 + u]
                            picked[pl.ds(t * 16 + u, tiles, stride=pick_step), :] = wide[pl.ds(row, tiles, stride=wide_step), :]
                        return 0

                    lax.fori_loop(0, SLOTS // 16, pick, 0)

                    def drain(t, _):
                        r = pl.multiple_of(t * 32, 32)
                        into = pl.multiple_of(b * SLOTS + t * 32, 32)
                        for j in range(tiles):
                            rows_ref[pl.ds(into, 32), col + j * LANES:col + (j + 1) * LANES] = picked[pl.ds(j * pick_step + r, 32), :].astype(BF16)
                        return 0

                    return lax.fori_loop(0, SLOTS // 32, drain, 0)

                lax.fori_loop(0, N_DEV, pick_device, 0)
        return far, near_first

    kept = []
    pl.run_scoped(
        lambda *bufs: kept.append(gather_all(*bufs)),
        pltpu.VMEM((n_rows, CHUNK), BF16), pltpu.VMEM((tiles * wide_step, LANES), F32), pltpu.VMEM((tiles * pick_step, LANES), F32),
    )
    far, near_first = kept[0]
    for copy in own:
        copy.wait()
    dims = (((1,), (1,)), ((), ()))
    row_iota = lax.broadcasted_iota(I32, (SLOTS, PAIR), 0)
    block_diag = (lax.broadcasted_iota(I32, (PAIR, 2 * SLOTS), 0) < TOK) == (lax.broadcasted_iota(I32, (PAIR, 2 * SLOTS), 1) < SLOTS)

    def front(r):
        toks, rows = pl.ds(2 * r, 2), pl.ds(2 * r * SLOTS, 2 * SLOTS)

        def dots(tok, table):
            full = lax.dot_general(tok[toks].reshape(PAIR, width), table[rows, :], dims, preferred_element_type=F32)
            return jnp.concatenate([full[:TOK, :SLOTS], full[TOK:, SLOTS:]], axis=0)

        act, slope = gelu_pair(dots(x_all, up_rows))
        slope = slope * dots(dy_all, down_rows)
        local = slot_all[toks].reshape(PAIR, SEL) - me * SLOTS
        valid = (local >= 0) & (local < SLOTS)
        index = jnp.where(valid, local, 0)
        act = jnp.take_along_axis(act, index, axis=1)
        slope = jnp.take_along_axis(slope, index, axis=1)
        gate = gate_all[toks].reshape(PAIR, SEL)
        w_t[...] = jnp.where(valid, (gate * act).astype(BF16).astype(F32), 0.0).T
        c_t[...] = jnp.where(valid, (gate * slope).astype(BF16).astype(F32), 0.0).T
        slot_t[...] = jnp.where(valid, local, -1).T

        def step(s, acc):
            acc_w, acc_c = acc
            hit = row_iota == slot_t[pl.ds(s, 1), :]
            acc_w += jnp.where(hit, w_t[pl.ds(s, 1), :], 0.0)
            acc_c += jnp.where(hit, c_t[pl.ds(s, 1), :], 0.0)
            return acc_w, acc_c

        zero = jnp.zeros((SLOTS, PAIR), F32)
        acc_w, acc_c = lax.fori_loop(0, SEL, step, (zero, zero), unroll=4)
        for ref, acc in ((w_out, acc_w), (c_out, acc_c)):
            terms = split3(acc)
            for j in range(2):
                ref[2 * r + j] = jnp.concatenate([term[:, j * TOK:(j + 1) * TOK] for term in terms], axis=1)

        def spread(acc):
            both = jnp.concatenate([acc.T, acc.T], axis=1)
            return split3(jnp.where(block_diag, both, 0.0))

        return spread(acc_w), spread(acc_c)

    def columns(r, terms, col, mine, other):
        rows = pl.ds(2 * r * SLOTS, 2 * SLOTS)
        table, terms = (down_rows, terms[0]) if col < half else (up_rows, terms[1])
        here = pl.ds(pl.multiple_of(core * half + col % half, COLS), COLS)
        there = pl.ds(pl.multiple_of((1 - core) * half + col % half, COLS), COLS)
        mine[:, col:col + COLS] = sum(jnp.dot(term, table[rows, here], preferred_element_type=F32) for term in terms)
        part = sum(jnp.dot(term, table[rows, there], preferred_element_type=F32) for term in terms)
        other[:TOK, col:col + COLS] = part[TOK:]
        other[TOK:, col:col + COLS] = part[:TOK]

    def block(r, mine, other):
        terms = front(r)
        for col in range(0, width, COLS):
            columns(r, terms, col, mine, other)

    def add_into(dst, src, cols=slice(None), step=16):
        def add(t, _):
            r = pl.ds(pl.multiple_of(t * step, step), step)
            dst[r, cols] = dst[r, cols] + src[r, cols]
            return 0

        lax.fori_loop(0, PAIR // step, add, 0)

    def blocks(mine, other):
        save = lambda src, dst, k: pltpu.make_async_copy(src, dst, out_sem.at[k])
        arrive(near_own)
        block(0, mine.at[0], other.at[1])
        pair_own = push(other, 1, pair_recv, 3, 1)
        arrive(far)
        near_far = [push(ref, 6, ref, 7, 1) for ref in (gate_all, slot_all, x_all, dy_all)]
        arrive(near_first + near_far)
        terms = front(3)
        pair_far, hop = [], []
        chunks = [pl.ds(col, COLS) for col in range(0, width, COLS)]
        every = slice(None)
        for cols in chunks:
            columns(3, terms, cols.start, mine.at[3], other.at[0])
            pair_far.append(push(other, (0, every, cols), pair_recv, (0, every, cols), 1))
        for k, cols in enumerate(chunks):
            arrive([pair_far[k]])
            add_into(mine.at[3], pair_recv.at[0], cols, 64)
            hop.append(push(mine, (3, every, cols), hop_recv, (every, cols), 2 + 2 * core))
        saves = []
        arrive([pair_own])
        add_into(mine.at[0], pair_recv.at[3])
        saves.append(save(mine.at[0], own_sum, 0))
        saves[-1].start()
        arrive(second)
        near_second = [push(gate_all, 2, gate_all, 3, 1), push(slot_all, 4, slot_all, 5, 1), push(x_all, 2, x_all, 3, 1), push(dy_all, 4, dy_all, 5, 1)]
        arrive(near_second)
        for k, (src, dst) in enumerate(((x_all, x_out), (dy_all, dy_out))):
            saves.append(save(src, dst, 1 + k))
            saves[-1].start()
        leave(pair_far)
        block(1, mine.at[1], other.at[0])
        pair_x = push(other, 0, pair_recv, 1, 1)
        leave([pair_own])
        block(2, mine.at[2], other.at[1])
        pair_y = push(other, 1, pair_recv, 2, 1)
        arrive([pair_x])
        add_into(mine.at[1], pair_recv.at[1])
        arrive([pair_y])
        add_into(mine.at[2], pair_recv.at[2])
        saves.append(save(mine.at[1 + core], first_sum, 3))
        saves[-1].start()
        for k, cols in enumerate(chunks):
            arrive([hop[k]])
            add_into(mine.at[2 - core], hop_recv, cols, 64)
        saves.append(save(mine.at[2 - core], second_sum, 4))
        saves[-1].start()
        leave([spec for spec in sent if spec not in pair_far and spec is not pair_own])
        for copy in saves:
            copy.wait()

    pl.run_scoped(blocks, pltpu.VMEM((4, PAIR, width), F32), pltpu.VMEM((2, PAIR, width), F32))


def row_kernel(asked_ref, coef_ref, x_ref, out_ref, wide, part):
    n_rows, cols = out_ref.shape
    tiles = cols // LANES
    wide_step, part_step = n_rows + PAD, SLOTS + PAD

    def clear(t, _):
        r = pl.multiple_of(t * 32, 32)
        for j in range(tiles):
            wide[pl.ds(j * wide_step + r, 32), :] = jnp.zeros((32, LANES), F32)
        return 0

    lax.fori_loop(0, n_rows // 32, clear, 0)
    for q in range(N_DEV):
        tok = x_ref[q * TOK:(q + 1) * TOK, :]
        full = jnp.dot(coef_ref[q], jnp.concatenate([tok] * TERMS, axis=0), preferred_element_type=F32)
        for j in range(tiles):
            part[pl.ds(j * part_step, SLOTS), :] = full[:, j * LANES:(j + 1) * LANES]

        def add(t, _):
            rows = [asked_ref[q, t * 16 + u] for u in range(16)]
            sums = [wide[pl.ds(rows[u], tiles, stride=wide_step), :] + part[pl.ds(t * 16 + u, tiles, stride=part_step), :] for u in range(16)]
            for u in range(16):
                wide[pl.ds(rows[u], tiles, stride=wide_step), :] = sums[u]
            return 0

        lax.fori_loop(0, SLOTS // 16, add, 0)

    def drain(t, _):
        r = pl.multiple_of(t * 32, 32)
        for j in range(tiles):
            out_ref[pl.ds(r, 32), j * LANES:(j + 1) * LANES] = wide[pl.ds(j * wide_step + r, 32), :].astype(BF16)
        return 0

    lax.fori_loop(0, n_rows // 32, drain, 0)


def solution(mesh):
    tok_spec = P(('dp', 'ep'))
    table_spec = P('ep')

    def per_device(tokens, slot_ids, request_rows, gate_vals, grad_out, up_local, down_local):
        width = tokens.shape[1]
        rows_owner = up_local.shape[0]
        n_tok = N_DEV * TOK
        half = width // 2
        core = lax.axis_index('ep') % 2
        vmem, anyw = pl.BlockSpec(memory_space=pltpu.VMEM), pl.BlockSpec(memory_space=pl.ANY)
        shape = jax.ShapeDtypeStruct
        sums = shape((PAIR, width), F32)
        x_all, dy_all, c_terms, w_terms, asked, first_sum, second_sum, own_sum = pl.pallas_call(
            layer_kernel,
            in_specs=[anyw, anyw, vmem, vmem, vmem, anyw, anyw],
            out_specs=[anyw] * 2 + [vmem] * 3 + [anyw] * 3,
            out_shape=[shape((N_DEV, TOK, width), BF16)] * 2 + [shape((N_DEV, SLOTS, TERMS * TOK), BF16)] * 2 + [shape((N_DEV, SLOTS), I32)] + [sums] * 3,
            scratch_shapes=[
                pltpu.VMEM((N_DEV, TOK, width), BF16), pltpu.VMEM((N_DEV, TOK, width), BF16),
                pltpu.VMEM((N_DEV, TOK, SEL), I32), pltpu.VMEM((N_DEV, TOK, SEL), F32),
                pltpu.VMEM((N_DEV * SLOTS, width), BF16), pltpu.VMEM((N_DEV * SLOTS, width), BF16),
                pltpu.VMEM((4, PAIR, width), F32), pltpu.VMEM((PAIR, width), F32),
                pltpu.VMEM((N_DEV, SLOTS), I32), pltpu.SMEM((N_DEV, SLOTS), I32),
                pltpu.VMEM((SEL, PAIR), I32), pltpu.VMEM((SEL, PAIR), F32), pltpu.VMEM((SEL, PAIR), F32),
                pltpu.SemaphoreType.DMA((N_COPIES,)), pltpu.SemaphoreType.DMA((N_COPIES,)),
                pltpu.SemaphoreType.DMA((2,)), pltpu.SemaphoreType.DMA,
                pltpu.SemaphoreType.DMA((1,)), pltpu.SemaphoreType.DMA((5,)),
            ],
            compiler_params=pltpu.CompilerParams(collective_id=0, has_side_effects=True, vmem_limit_bytes=VMEM_BYTES),
        )(tokens, grad_out, slot_ids.transpose(1, 2, 0), gate_vals.transpose(1, 2, 0), request_rows, up_local, down_local)

        partner = [(i, i ^ 1) for i in range(N_DEV)]
        first_hop = [(i, i ^ (2 if i % 2 == 0 else 4)) for i in range(N_DEV)]
        second_hop = [(i, i ^ (4 if i % 2 == 0 else 2)) for i in range(N_DEV)]
        hop = lambda value, pairs: lax.ppermute(value, 'ep', pairs)

        def grad_rows(coef, tok):
            return pl.pallas_call(
                row_kernel,
                grid_spec=pltpu.PrefetchScalarGridSpec(
                    num_scalar_prefetch=1,
                    grid=(width // ROW_CHUNK,),
                    in_specs=[pl.BlockSpec(coef.shape, lambda i, a: (0, 0, 0)), pl.BlockSpec((n_tok, ROW_CHUNK), lambda i, a: (0, i))],
                    out_specs=pl.BlockSpec((rows_owner, ROW_CHUNK), lambda i, a: (0, i)),
                    scratch_shapes=[pltpu.VMEM((ROW_CHUNK // LANES * (rows_owner + PAD), LANES), F32), pltpu.VMEM((ROW_CHUNK // LANES * (SLOTS + PAD), LANES), F32)],
                ),
                out_shape=shape((rows_owner, width), BF16),
                compiler_params=pltpu.CompilerParams(vmem_limit_bytes=VMEM_BYTES),
                cost_estimate=pl.CostEstimate(flops=6 * rows_owner * width * n_tok, bytes_accessed=2 * rows_owner * width, transcendentals=0),
            )(asked, coef, tok.reshape(n_tok, width))

        got_own = hop(first_sum, first_hop)
        got_last = hop(second_sum, second_hop)
        grad_up = grad_rows(c_terms, x_all)
        grad_down = grad_rows(w_terms, dy_all)
        got_last, got_own, grad_up, grad_down = lax.optimization_barrier((got_last, got_own, grad_up, grad_down))
        keep, give = [(own_sum[rows] + got_own[rows] + got_last[rows]).astype(BF16).reshape(TOK, 2, half) for rows in (slice(0, TOK), slice(TOK, PAIR))]
        back = hop(give, partner)
        low = jnp.where(core == 0, keep, back)
        high = jnp.where(core == 0, back, keep)
        token_out = jnp.concatenate([low, high], axis=2)
        return token_out[:, 0], token_out[:, 1], grad_up, grad_down

    return jax.shard_map(per_device, mesh=mesh, in_specs=(tok_spec, tok_spec, tok_spec, tok_spec, tok_spec, table_spec, table_spec), out_specs=(tok_spec, tok_spec, tok_spec, tok_spec), check_vma=False)
```

```python
import functools
import math
import jax
import jax.numpy as jnp
from jax import lax
from jax.experimental import pallas as pl
from jax.experimental.pallas import tpu as pltpu
from jax.sharding import PartitionSpec as P

F32, BF16, I32 = jnp.float32, jnp.bfloat16, jnp.int32
N_DEV, TOK, SLOTS, SEL = 8, 64, 128, 128
PAIR = 2 * TOK
TERMS = 3
CHUNK = 2048
ROW_CHUNK = 1024
GROUP = 16
LOW = 16
LANES = 128
PAD = 4
VMEM_BYTES = 62 * 1024 * 1024
MESH = pl.DeviceIdType.MESH


def gelu_pair(pre_act):
    normal_cdf = 0.5 * (1.0 + lax.erf(pre_act * (2.0 ** -0.5)))
    normal_pdf = jnp.exp(-0.5 * pre_act * pre_act) * ((2.0 * math.pi) ** -0.5)
    return pre_act * normal_cdf, normal_cdf + pre_act * normal_pdf


def split3(wide):
    high = wide.astype(BF16)
    rest = wide - high.astype(F32)
    mid = rest.astype(BF16)
    low = (rest - mid.astype(F32)).astype(BF16)
    return high, mid, low


N_COPIES = 64
SIDE_STEP, FAR_STEP, REST_STEP = 1, 4, 6
COLS = 512


def layer_kernel(x_ref, dy_ref, slot_ref, gate_ref, req_ref, up_ref, down_ref,
                 x_out, dy_out, c_out, w_out, asked_out, first_sum, second_sum, own_sum,
                 x_all, dy_all, slot_all, gate_all, up_rows, down_rows, pair_recv, hop_recv, asked, asked_s, slot_t, w_t, c_t,
                 send_sem, recv_sem, own_sem, smem_sem, in_sem, out_sem):
    me = lax.axis_index("ep")
    core = lax.rem(me, 2)
    n_rows, width = up_ref.shape
    half = width // 2
    steps = [(ref, out, col) for ref, out in ((up_ref, up_rows), (down_ref, down_rows)) for col in range(0, width, CHUNK)]
    tiles = CHUNK // LANES
    wide_step, pick_step = n_rows + PAD, SLOTS + PAD
    sent = []

    def descriptor(k, src, dst, mask):
        view = lambda ref, index: ref if index is None else ref.at[index]
        return pltpu.make_async_remote_copy(src_ref=view(*src), dst_ref=view(*dst), send_sem=send_sem.at[k], recv_sem=recv_sem.at[k],
                                            device_id={"ep": me ^ mask}, device_id_type=MESH)

    def push(src, src_index, dst, dst_index, mask):
        spec = (len(sent), (src, src_index), (dst, dst_index), mask)
        descriptor(*spec).start()
        sent.append(spec)
        return spec

    def arrive(specs):
        for spec in specs:
            descriptor(*spec).wait_recv()

    def leave(specs):
        for spec in specs:
            descriptor(*spec).wait_send()

    own = [pltpu.make_async_copy(src, dst.at[0], own_sem.at[k]) for k, (src, dst) in enumerate(((x_ref, x_all), (dy_ref, dy_all)))]
    slot_all[0] = slot_ref[...].reshape(SEL, TOK).T
    gate_all[0] = gate_ref[...].reshape(SEL, TOK).T
    barrier = pltpu.get_barrier_semaphore()
    for b in range(1, N_DEV):
        pl.semaphore_signal(barrier, inc=1, device_id={"ep": me ^ b}, device_id_type=MESH)
    for copy in own:
        copy.start()
    pl.semaphore_wait(barrier, N_DEV - 1)

    asks = [push(req_ref, (0, pl.ds(me ^ b, 1)), asked, pl.ds(b, 1), b) for b in range(1, N_DEV)]
    first = [push(x_ref, None, x_all, 4, 4), push(dy_ref, None, dy_all, 2, 2)]
    near_own = [push(x_ref, None, x_all, 1, 1), push(dy_ref, None, dy_all, 1, 1)]
    low, top = pl.ds(0, LOW), pl.ds(LOW, TOK - LOW)
    second = [push(x_ref, low, x_all, (2, low), 2), push(dy_ref, low, dy_all, (4, low), 4)]
    asked[pl.ds(0, 1), :] = req_ref[0, pl.ds(me, 1), :]
    arrive(asks)
    asked_out[...] = asked[...]
    to_smem = pltpu.make_async_copy(asked, asked_s, smem_sem)
    to_smem.start()
    to_smem.wait()

    def gather_all(table, wide, picked):
        def fetch(k):
            ref, _, col = steps[k]
            return pltpu.make_async_copy(ref.at[:, pl.ds(col, CHUNK)], table, in_sem.at[0])

        fetch(0).start()
        for sub in range(2 * len(steps)):
            if sub == SIDE_STEP:
                side = [push(gate_all, 0, gate_all, 4, 4), push(slot_all, 0, slot_all, 2, 2)]
                near_own.extend([push(gate_all, 0, gate_all, 1, 1), push(slot_all, 0, slot_all, 1, 1)])
            if sub == FAR_STEP:
                arrive(first)
                far = [push(x_all, 4, x_all, 6, 2), push(dy_all, 2, dy_all, 6, 4)]
                near_first = [push(x_all, 4, x_all, 5, 1), push(dy_all, 2, dy_all, 3, 1)]
            if sub == REST_STEP:
                arrive(side)
                far.extend([push(gate_all, 4, gate_all, 6, 2), push(slot_all, 2, slot_all, 6, 4)])
                near_first.extend([push(gate_all, 4, gate_all, 5, 1), push(slot_all, 2, slot_all, 3, 1)])
                second.extend([push(gate_all, 0, gate_all, 2, 2), push(slot_all, 0, slot_all, 4, 4)])
                second.extend([push(x_ref, top, x_all, (2, top), 2), push(dy_ref, top, dy_all, (4, top), 4)])
            k = sub // 2
            if sub % 2 == 0:
                fetch(k).wait()

                def fill(t, _):
                    r = pl.multiple_of(t * 32, 32)
                    for j in range(tiles):
                        wide[pl.ds(j * wide_step + r, 32), :] = table[pl.ds(r, 32), j * LANES:(j + 1) * LANES].astype(F32)
                    return 0

                lax.fori_loop(0, n_rows // 32, fill, 0)
                if k + 1 < len(steps):
                    fetch(k + 1).start()
            else:
                _, rows_ref, col = steps[k]

                def pick_device(b, _):
                    def pick(t, _):
                        for u in range(16):
                            row = asked_s[b, t * 16 + u]
                            picked[pl.ds(t * 16 + u, tiles, stride=pick_step), :] = wide[pl.ds(row, tiles, stride=wide_step), :]
                        return 0

                    lax.fori_loop(0, SLOTS // 16, pick, 0)

                    def drain(t, _):
                        r = pl.multiple_of(t * 32, 32)
                        into = pl.multiple_of(b * SLOTS + t * 32, 32)
                        for j in range(tiles):
                            rows_ref[pl.ds(into, 32), col + j * LANES:col + (j + 1) * LANES] = picked[pl.ds(j * pick_step + r, 32), :].astype(BF16)
                        return 0

                    return lax.fori_loop(0, SLOTS // 32, drain, 0)

                lax.fori_loop(0, N_DEV, pick_device, 0)
        return far, near_first

    kept = []
    pl.run_scoped(
        lambda *bufs: kept.append(gather_all(*bufs)),
        pltpu.VMEM((n_rows, CHUNK), BF16), pltpu.VMEM((tiles * wide_step, LANES), F32), pltpu.VMEM((tiles * pick_step, LANES), F32),
    )
    far, near_first = kept[0]
    for copy in own:
        copy.wait()
    dims = (((1,), (1,)), ((), ()))
    row_iota = lax.broadcasted_iota(I32, (SLOTS, PAIR), 0)
    block_diag = (lax.broadcasted_iota(I32, (PAIR, 2 * SLOTS), 0) < TOK) == (lax.broadcasted_iota(I32, (PAIR, 2 * SLOTS), 1) < SLOTS)

    def front(r):
        toks, rows = pl.ds(2 * r, 2), pl.ds(2 * r * SLOTS, 2 * SLOTS)

        def dots(tok, table):
            full = lax.dot_general(tok[toks].reshape(PAIR, width), table[rows, :], dims, preferred_element_type=F32)
            return jnp.concatenate([full[:TOK, :SLOTS], full[TOK:, SLOTS:]], axis=0)

        act, slope = gelu_pair(dots(x_all, up_rows))
        slope = slope * dots(dy_all, down_rows)
        local = slot_all[toks].reshape(PAIR, SEL) - me * SLOTS
        valid = (local >= 0) & (local < SLOTS)
        index = jnp.where(valid, local, 0)
        act = jnp.take_along_axis(act, index, axis=1)
        slope = jnp.take_along_axis(slope, index, axis=1)
        gate = gate_all[toks].reshape(PAIR, SEL)
        w_t[...] = jnp.where(valid, (gate * act).astype(BF16).astype(F32), 0.0).T
        c_t[...] = jnp.where(valid, (gate * slope).astype(BF16).astype(F32), 0.0).T
        slot_t[...] = jnp.where(valid, local, -1).T

        def step(s, acc):
            acc_w, acc_c = acc
            hit = row_iota == slot_t[pl.ds(s, 1), :]
            acc_w += jnp.where(hit, w_t[pl.ds(s, 1), :], 0.0)
            acc_c += jnp.where(hit, c_t[pl.ds(s, 1), :], 0.0)
            return acc_w, acc_c

        zero = jnp.zeros((SLOTS, PAIR), F32)
        acc_w, acc_c = lax.fori_loop(0, SEL, step, (zero, zero), unroll=4)
        for ref, acc in ((w_out, acc_w), (c_out, acc_c)):
            terms = split3(acc)
            for j in range(2):
                ref[2 * r + j] = jnp.concatenate([term[:, j * TOK:(j + 1) * TOK] for term in terms], axis=1)

        def spread(acc):
            both = jnp.concatenate([acc.T, acc.T], axis=1)
            return split3(jnp.where(block_diag, both, 0.0))

        return spread(acc_w), spread(acc_c)

    def columns(r, terms, col, mine, other):
        rows = pl.ds(2 * r * SLOTS, 2 * SLOTS)
        table, terms = (down_rows, terms[0]) if col < half else (up_rows, terms[1])
        here = pl.ds(pl.multiple_of(core * half + col % half, COLS), COLS)
        there = pl.ds(pl.multiple_of((1 - core) * half + col % half, COLS), COLS)
        mine[:, col:col + COLS] = sum(jnp.dot(term, table[rows, here], preferred_element_type=F32) for term in terms)
        part = sum(jnp.dot(term, table[rows, there], preferred_element_type=F32) for term in terms)
        other[:TOK, col:col + COLS] = part[TOK:]
        other[TOK:, col:col + COLS] = part[:TOK]

    def block(r, mine, other):
        terms = front(r)
        for col in range(0, width, COLS):
            columns(r, terms, col, mine, other)

    def add_into(dst, src, cols=slice(None), step=16):
        def add(t, _):
            r = pl.ds(pl.multiple_of(t * step, step), step)
            dst[r, cols] = dst[r, cols] + src[r, cols]
            return 0

        lax.fori_loop(0, PAIR // step, add, 0)

    def blocks(mine, other):
        save = lambda src, dst, k: pltpu.make_async_copy(src, dst, out_sem.at[k])
        arrive(near_own)
        arrive(far)
        near_far = [push(ref, 6, ref, 7, 1) for ref in (gate_all, slot_all, x_all, dy_all)]
        arrive(near_first + near_far)
        terms = front(3)
        pair_far, hop = [], []
        chunks = [pl.ds(col, COLS) for col in range(0, width, COLS)]
        every = slice(None)
        for cols in chunks:
            columns(3, terms, cols.start, mine.at[3], other.at[0])
            pair_far.append(push(other, (0, every, cols), pair_recv, (0, every, cols), 1))
        for k, cols in enumerate(chunks):
            arrive([pair_far[k]])
            add_into(mine.at[3], pair_recv.at[0], cols, 64)
            hop.append(push(mine, (3, every, cols), hop_recv, (every, cols), 2 + 2 * core))
        saves = []
        arrive(second)
        near_second = [push(gate_all, 2, gate_all, 3, 1), push(slot_all, 4, slot_all, 5, 1), push(x_all, 2, x_all, 3, 1), push(dy_all, 4, dy_all, 5, 1)]
        arrive(near_second)
        for k, (src, dst) in enumerate(((x_all, x_out), (dy_all, dy_out))):
            saves.append(save(src, dst, 1 + k))
            saves[-1].start()
        leave(pair_far)
        block(1, mine.at[1], other.at[0])
        pair_x = push(other, 0, pair_recv, 1, 1)
        block(2, mine.at[2], other.at[1])
        pair_y = push(other, 1, pair_recv, 2, 1)
        leave([pair_x])
        block(0, mine.at[0], other.at[0])
        pair_own = push(other, 0, pair_recv, 3, 1)
        arrive([pair_x])
        add_into(mine.at[1], pair_recv.at[1])
        arrive([pair_y])
        add_into(mine.at[2], pair_recv.at[2])
        saves.append(save(mine.at[1 + core], first_sum, 3))
        saves[-1].start()
        arrive([pair_own])
        add_into(mine.at[0], pair_recv.at[3])
        saves.append(save(mine.at[0], own_sum, 0))
        saves[-1].start()
        for k, cols in enumerate(chunks):
            arrive([hop[k]])
            add_into(mine.at[2 - core], hop_recv, cols, 64)
        saves.append(save(mine.at[2 - core], second_sum, 4))
        saves[-1].start()
        leave([spec for spec in sent if spec not in pair_far and spec is not pair_x])
        for copy in saves:
            copy.wait()

    pl.run_scoped(blocks, pltpu.VMEM((4, PAIR, width), F32), pltpu.VMEM((2, PAIR, width), F32))


def row_kernel(asked_ref, c_ref, w_ref, x_ref, dy_ref, du_ref, dv_ref, wide_u, wide_v, part_u, part_v):
    n_rows, cols = du_ref.shape
    tiles = cols // LANES
    wide_step, part_step = n_rows + PAD, SLOTS + PAD
    part_size = tiles * part_step

    def clear(t, _):
        r = pl.multiple_of(t * 32, 32)
        for j in range(tiles):
            for wide in (wide_u, wide_v):
                wide[pl.ds(j * wide_step + r, 32), :] = jnp.zeros((32, LANES), F32)
        return 0

    lax.fori_loop(0, n_rows // 32, clear, 0)

    def product(q, slot):
        for coef, tok, part in ((c_ref, x_ref, part_u), (w_ref, dy_ref, part_v)):
            rows = tok[pl.ds(pl.multiple_of(q * TOK, TOK), TOK), :]
            full = jnp.dot(coef[q], jnp.concatenate([rows] * TERMS, axis=0), preferred_element_type=F32)
            for j in range(tiles):
                part[pl.ds(slot * part_size + j * part_step, SLOTS), :] = full[:, j * LANES:(j + 1) * LANES]

    product(0, 0)

    def device(q, _):
        product(lax.rem(q + 1, N_DEV), lax.rem(q + 1, 2))
        base = lax.rem(q, 2) * part_size
        for t in range(0, SLOTS, GROUP):
            rows = [asked_ref[q, t + u] for u in range(GROUP)]
            sums = [[wide[pl.ds(row, tiles, stride=wide_step), :] + part[pl.ds(base + t + u, tiles, stride=part_step), :]
                     for wide, part in ((wide_u, part_u), (wide_v, part_v))] for u, row in enumerate(rows)]
            for row, pair in zip(rows, sums):
                for wide, value in zip((wide_u, wide_v), pair):
                    wide[pl.ds(row, tiles, stride=wide_step), :] = value
        return 0

    lax.fori_loop(0, N_DEV, device, 0)

    def drain(t, _):
        r = pl.multiple_of(t * 32, 32)
        for j in range(tiles):
            for wide, out in ((wide_u, du_ref), (wide_v, dv_ref)):
                out[pl.ds(r, 32), j * LANES:(j + 1) * LANES] = wide[pl.ds(j * wide_step + r, 32), :].astype(BF16)
        return 0

    lax.fori_loop(0, n_rows // 32, drain, 0)


def solution(mesh):
    tok_spec = P(('dp', 'ep'))
    table_spec = P('ep')

    def per_device(tokens, slot_ids, request_rows, gate_vals, grad_out, up_local, down_local):
        width = tokens.shape[1]
        rows_owner = up_local.shape[0]
        n_tok = N_DEV * TOK
        half = width // 2
        core = lax.axis_index('ep') % 2
        vmem, anyw = pl.BlockSpec(memory_space=pltpu.VMEM), pl.BlockSpec(memory_space=pl.ANY)
        shape = jax.ShapeDtypeStruct
        sums = shape((PAIR, width), F32)
        x_all, dy_all, c_terms, w_terms, asked, first_sum, second_sum, own_sum = pl.pallas_call(
            layer_kernel,
            in_specs=[anyw, anyw, vmem, vmem, vmem, anyw, anyw],
            out_specs=[anyw] * 2 + [vmem] * 3 + [anyw] * 3,
            out_shape=[shape((N_DEV, TOK, width), BF16)] * 2 + [shape((N_DEV, SLOTS, TERMS * TOK), BF16)] * 2 + [shape((N_DEV, SLOTS), I32)] + [sums] * 3,
            scratch_shapes=[
                pltpu.VMEM((N_DEV, TOK, width), BF16), pltpu.VMEM((N_DEV, TOK, width), BF16),
                pltpu.VMEM((N_DEV, TOK, SEL), I32), pltpu.VMEM((N_DEV, TOK, SEL), F32),
                pltpu.VMEM((N_DEV * SLOTS, width), BF16), pltpu.VMEM((N_DEV * SLOTS, width), BF16),
                pltpu.VMEM((4, PAIR, width), F32), pltpu.VMEM((PAIR, width), F32),
                pltpu.VMEM((N_DEV, SLOTS), I32), pltpu.SMEM((N_DEV, SLOTS), I32),
                pltpu.VMEM((SEL, PAIR), I32), pltpu.VMEM((SEL, PAIR), F32), pltpu.VMEM((SEL, PAIR), F32),
                pltpu.SemaphoreType.DMA((N_COPIES,)), pltpu.SemaphoreType.DMA((N_COPIES,)),
                pltpu.SemaphoreType.DMA((2,)), pltpu.SemaphoreType.DMA,
                pltpu.SemaphoreType.DMA((1,)), pltpu.SemaphoreType.DMA((5,)),
            ],
            compiler_params=pltpu.CompilerParams(collective_id=0, has_side_effects=True, vmem_limit_bytes=VMEM_BYTES),
        )(tokens, grad_out, slot_ids.transpose(1, 2, 0), gate_vals.transpose(1, 2, 0), request_rows, up_local, down_local)

        partner = [(i, i ^ 1) for i in range(N_DEV)]
        first_hop = [(i, i ^ (2 if i % 2 == 0 else 4)) for i in range(N_DEV)]
        second_hop = [(i, i ^ (4 if i % 2 == 0 else 2)) for i in range(N_DEV)]
        hop = lambda value, pairs: lax.ppermute(value, 'ep', pairs)

        def grad_rows():
            coef = pl.BlockSpec((N_DEV, SLOTS, TERMS * TOK), lambda i, a: (0, 0, 0))
            tok = pl.BlockSpec((n_tok, ROW_CHUNK), lambda i, a: (0, i))
            out = pl.BlockSpec((rows_owner, ROW_CHUNK), lambda i, a: (0, i))
            tiles = ROW_CHUNK // LANES
            return pl.pallas_call(
                row_kernel,
                grid_spec=pltpu.PrefetchScalarGridSpec(
                    num_scalar_prefetch=1,
                    grid=(width // ROW_CHUNK,),
                    in_specs=[coef, coef, tok, tok],
                    out_specs=[out, out],
                    scratch_shapes=[pltpu.VMEM((tiles * (rows_owner + PAD), LANES), F32)] * 2 + [pltpu.VMEM((2 * tiles * (SLOTS + PAD), LANES), F32)] * 2,
                ),
                out_shape=[shape((rows_owner, width), BF16)] * 2,
                compiler_params=pltpu.CompilerParams(vmem_limit_bytes=VMEM_BYTES),
                cost_estimate=pl.CostEstimate(flops=12 * rows_owner * width * n_tok, bytes_accessed=4 * rows_owner * width, transcendentals=0),
            )(asked, c_terms, w_terms, x_all.reshape(n_tok, width), dy_all.reshape(n_tok, width))

        got_own = hop(first_sum, first_hop)
        got_last = hop(second_sum, second_hop)
        grad_up, grad_down = grad_rows()
        got_last, got_own, grad_up, grad_down = lax.optimization_barrier((got_last, got_own, grad_up, grad_down))
        keep, give = [(own_sum[rows] + got_own[rows] + got_last[rows]).astype(BF16).reshape(TOK, 2, half) for rows in (slice(0, TOK), slice(TOK, PAIR))]
        back = hop(give, partner)
        low = jnp.where(core == 0, keep, back)
        high = jnp.where(core == 0, back, keep)
        token_out = jnp.concatenate([low, high], axis=2)
        return token_out[:, 0], token_out[:, 1], grad_up, grad_down

    return jax.shard_map(per_device, mesh=mesh, in_specs=(tok_spec, tok_spec, tok_spec, tok_spec, tok_spec, table_spec, table_spec), out_specs=(tok_spec, tok_spec, tok_spec, tok_spec), check_vma=False)
```

```python
import functools
import math
import jax
import jax.numpy as jnp
from jax import lax
from jax.experimental import pallas as pl
from jax.experimental.pallas import tpu as pltpu
from jax.sharding import PartitionSpec as P

F32, BF16, I32 = jnp.float32, jnp.bfloat16, jnp.int32
N_DEV, TOK, SLOTS, SEL = 8, 64, 128, 128
PAIR = 2 * TOK
TERMS = 3
CHUNK = 2048
ROW_CHUNK = 1024
GROUP = 16
LOW = 16
LANES = 128
PAD = 4
VMEM_BYTES = 62 * 1024 * 1024
MESH = pl.DeviceIdType.MESH


def gelu_pair(pre_act):
    normal_cdf = 0.5 * (1.0 + lax.erf(pre_act * (2.0 ** -0.5)))
    normal_pdf = jnp.exp(-0.5 * pre_act * pre_act) * ((2.0 * math.pi) ** -0.5)
    return pre_act * normal_cdf, normal_cdf + pre_act * normal_pdf


def split3(wide):
    high = wide.astype(BF16)
    rest = wide - high.astype(F32)
    mid = rest.astype(BF16)
    low = (rest - mid.astype(F32)).astype(BF16)
    return high, mid, low


N_COPIES = 64
SIDE_STEP, FAR_STEP, REST_STEP = 1, 4, 6
COLS = 512
PART = 32


def layer_kernel(x_ref, dy_ref, slot_ref, gate_ref, req_ref, up_ref, down_ref,
                 x_out, dy_out, c_out, w_out, asked_out, first_keep, first_cross, second_keep, second_cross, own_keep, own_cross,
                 x_all, dy_all, slot_all, gate_all, up_rows, down_rows, pair_recv, hop_recv, part_recv, asked, asked_s, slot_t, w_t, c_t,
                 send_sem, recv_sem, own_sem, smem_sem, in_sem, out_sem):
    me = lax.axis_index("ep")
    core = lax.rem(me, 2)
    n_rows, width = up_ref.shape
    half = width // 2
    steps = [(ref, out, col) for ref, out in ((up_ref, up_rows), (down_ref, down_rows)) for col in range(0, width, CHUNK)]
    tiles = CHUNK // LANES
    wide_step, pick_step = n_rows + PAD, SLOTS + PAD
    sent = []

    def descriptor(k, src, dst, mask):
        view = lambda ref, index: ref if index is None else ref.at[index]
        return pltpu.make_async_remote_copy(src_ref=view(*src), dst_ref=view(*dst), send_sem=send_sem.at[k], recv_sem=recv_sem.at[k],
                                            device_id={"ep": me ^ mask}, device_id_type=MESH)

    def push(src, src_index, dst, dst_index, mask):
        spec = (len(sent), (src, src_index), (dst, dst_index), mask)
        descriptor(*spec).start()
        sent.append(spec)
        return spec

    def arrive(specs):
        for spec in specs:
            descriptor(*spec).wait_recv()

    def leave(specs):
        for spec in specs:
            descriptor(*spec).wait_send()

    own = [pltpu.make_async_copy(src, dst.at[0], own_sem.at[k]) for k, (src, dst) in enumerate(((x_ref, x_all), (dy_ref, dy_all)))]
    slot_all[0] = slot_ref[...].reshape(SEL, TOK).T
    gate_all[0] = gate_ref[...].reshape(SEL, TOK).T
    barrier = pltpu.get_barrier_semaphore()
    for b in range(1, N_DEV):
        pl.semaphore_signal(barrier, inc=1, device_id={"ep": me ^ b}, device_id_type=MESH)
    for copy in own:
        copy.start()
    pl.semaphore_wait(barrier, N_DEV - 1)

    asks = [push(req_ref, (0, pl.ds(me ^ b, 1)), asked, pl.ds(b, 1), b) for b in range(1, N_DEV)]
    first = [push(x_ref, None, x_all, 4, 4), push(dy_ref, None, dy_all, 2, 2)]
    near_own = [push(x_ref, None, x_all, 1, 1), push(dy_ref, None, dy_all, 1, 1)]
    low, top = pl.ds(0, LOW), pl.ds(LOW, TOK - LOW)
    second = [push(x_ref, low, x_all, (2, low), 2), push(dy_ref, low, dy_all, (4, low), 4)]
    asked[pl.ds(0, 1), :] = req_ref[0, pl.ds(me, 1), :]
    arrive(asks)
    asked_out[...] = asked[...]
    to_smem = pltpu.make_async_copy(asked, asked_s, smem_sem)
    to_smem.start()
    to_smem.wait()

    def gather_all(table, wide, picked):
        def fetch(k):
            ref, _, col = steps[k]
            return pltpu.make_async_copy(ref.at[:, pl.ds(col, CHUNK)], table, in_sem.at[0])

        fetch(0).start()
        for sub in range(2 * len(steps)):
            if sub == SIDE_STEP:
                side = [push(gate_all, 0, gate_all, 4, 4), push(slot_all, 0, slot_all, 2, 2)]
                near_own.extend([push(gate_all, 0, gate_all, 1, 1), push(slot_all, 0, slot_all, 1, 1)])
            if sub == FAR_STEP:
                arrive(first)
                far = [push(x_all, 4, x_all, 6, 2), push(dy_all, 2, dy_all, 6, 4)]
                near_first = [push(x_all, 4, x_all, 5, 1), push(dy_all, 2, dy_all, 3, 1)]
            if sub == REST_STEP:
                arrive(side)
                far.extend([push(gate_all, 4, gate_all, 6, 2), push(slot_all, 2, slot_all, 6, 4)])
                near_first.extend([push(gate_all, 4, gate_all, 5, 1), push(slot_all, 2, slot_all, 3, 1)])
                second.extend([push(gate_all, 0, gate_all, 2, 2), push(slot_all, 0, slot_all, 4, 4)])
                second.extend([push(x_ref, top, x_all, (2, top), 2), push(dy_ref, top, dy_all, (4, top), 4)])
            k = sub // 2
            if sub % 2 == 0:
                fetch(k).wait()

                def fill(t, _):
                    r = pl.multiple_of(t * 32, 32)
                    for j in range(tiles):
                        wide[pl.ds(j * wide_step + r, 32), :] = table[pl.ds(r, 32), j * LANES:(j + 1) * LANES].astype(F32)
                    return 0

                lax.fori_loop(0, n_rows // 32, fill, 0)
                if k + 1 < len(steps):
                    fetch(k + 1).start()
            else:
                _, rows_ref, col = steps[k]

                def pick_device(b, _):
                    def pick(t, _):
                        for u in range(16):
                            row = asked_s[b, t * 16 + u]
                            picked[pl.ds(t * 16 + u, tiles, stride=pick_step), :] = wide[pl.ds(row, tiles, stride=wide_step), :]
                        return 0

                    lax.fori_loop(0, SLOTS // 16, pick, 0)

                    def drain(t, _):
                        r = pl.multiple_of(t * 32, 32)
                        into = pl.multiple_of(b * SLOTS + t * 32, 32)
                        for j in range(tiles):
                            rows_ref[pl.ds(into, 32), col + j * LANES:col + (j + 1) * LANES] = picked[pl.ds(j * pick_step + r, 32), :].astype(BF16)
                        return 0

                    return lax.fori_loop(0, SLOTS // 32, drain, 0)

                lax.fori_loop(0, N_DEV, pick_device, 0)
        return far, near_first

    kept = []
    pl.run_scoped(
        lambda *bufs: kept.append(gather_all(*bufs)),
        pltpu.VMEM((n_rows, CHUNK), BF16), pltpu.VMEM((tiles * wide_step, LANES), F32), pltpu.VMEM((tiles * pick_step, LANES), F32),
    )
    far, near_first = kept[0]
    for copy in own:
        copy.wait()
    dims = (((1,), (1,)), ((), ()))
    row_iota = lax.broadcasted_iota(I32, (SLOTS, PAIR), 0)
    block_diag = (lax.broadcasted_iota(I32, (PAIR, 2 * SLOTS), 0) < TOK) == (lax.broadcasted_iota(I32, (PAIR, 2 * SLOTS), 1) < SLOTS)

    def front(r):
        toks, rows = pl.ds(2 * r, 2), pl.ds(2 * r * SLOTS, 2 * SLOTS)

        def dots(tok, table):
            full = lax.dot_general(tok[toks].reshape(PAIR, width), table[rows, :], dims, preferred_element_type=F32)
            return jnp.concatenate([full[:TOK, :SLOTS], full[TOK:, SLOTS:]], axis=0)

        act, slope = gelu_pair(dots(x_all, up_rows))
        slope = slope * dots(dy_all, down_rows)
        local = slot_all[toks].reshape(PAIR, SEL) - me * SLOTS
        valid = (local >= 0) & (local < SLOTS)
        index = jnp.where(valid, local, 0)
        act = jnp.take_along_axis(act, index, axis=1)
        slope = jnp.take_along_axis(slope, index, axis=1)
        gate = gate_all[toks].reshape(PAIR, SEL)
        w_t[...] = jnp.where(valid, (gate * act).astype(BF16).astype(F32), 0.0).T
        c_t[...] = jnp.where(valid, (gate * slope).astype(BF16).astype(F32), 0.0).T
        slot_t[...] = jnp.where(valid, local, -1).T

        def step(s, acc):
            acc_w, acc_c = acc
            hit = row_iota == slot_t[pl.ds(s, 1), :]
            acc_w += jnp.where(hit, w_t[pl.ds(s, 1), :], 0.0)
            acc_c += jnp.where(hit, c_t[pl.ds(s, 1), :], 0.0)
            return acc_w, acc_c

        zero = jnp.zeros((SLOTS, PAIR), F32)
        acc_w, acc_c = lax.fori_loop(0, SEL, step, (zero, zero), unroll=4)
        for ref, acc in ((w_out, acc_w), (c_out, acc_c)):
            terms = split3(acc)
            for j in range(2):
                ref[2 * r + j] = jnp.concatenate([term[:, j * TOK:(j + 1) * TOK] for term in terms], axis=1)

        def spread(acc):
            both = jnp.concatenate([acc.T, acc.T], axis=1)
            return split3(jnp.where(block_diag, both, 0.0))

        return spread(acc_w), spread(acc_c)

    def columns(r, terms, col, mine, other):
        rows = pl.ds(2 * r * SLOTS, 2 * SLOTS)
        table, terms = (down_rows, terms[0]) if col < half else (up_rows, terms[1])
        here = pl.ds(pl.multiple_of(core * half + col % half, COLS), COLS)
        there = pl.ds(pl.multiple_of((1 - core) * half + col % half, COLS), COLS)
        mine[:, col:col + COLS] = sum(jnp.dot(term, table[rows, here], preferred_element_type=F32) for term in terms)
        part = sum(jnp.dot(term, table[rows, there], preferred_element_type=F32) for term in terms)
        other[:TOK, col:col + COLS] = part[TOK:]
        other[TOK:, col:col + COLS] = part[:TOK]

    def block(r, mine, other):
        terms = front(r)
        for col in range(0, width, COLS):
            columns(r, terms, col, mine, other)

    def add_into(dst, src, cols=slice(None), step=16):
        def add(t, _):
            r = pl.ds(pl.multiple_of(t * step, step), step)
            dst[r, cols] = dst[r, cols] + src[r, cols]
            return 0

        lax.fori_loop(0, PAIR // step, add, 0)

    def blocks(mine, other):
        save = lambda src, dst, k: pltpu.make_async_copy(src, dst, out_sem.at[k])
        arrive(near_own)
        arrive(far)
        near_far = [push(ref, 6, ref, 7, 1) for ref in (gate_all, slot_all, x_all, dy_all)]
        arrive(near_first + near_far)
        terms = front(3)
        pair_far, hop = [], []
        chunks = [pl.ds(col, COLS) for col in range(0, width, COLS)]
        every = slice(None)
        for cols in chunks:
            columns(3, terms, cols.start, mine.at[3], other.at[0])
            pair_far.append(push(other, (0, every, cols), pair_recv, (0, every, cols), 1))
        for k, cols in enumerate(chunks):
            arrive([pair_far[k]])
            add_into(mine.at[3], pair_recv.at[0], cols, 64)
            hop.append(push(mine, (3, every, cols), hop_recv, (every, cols), 2 + 2 * core))
        saves = []
        arrive(second)
        near_second = [push(gate_all, 2, gate_all, 3, 1), push(slot_all, 4, slot_all, 5, 1), push(x_all, 2, x_all, 3, 1), push(dy_all, 4, dy_all, 5, 1)]
        arrive(near_second)
        for k, (src, dst) in enumerate(((x_all, x_out), (dy_all, dy_out))):
            saves.append(save(src, dst, 1 + k))
            saves[-1].start()
        leave(pair_far)
        block(1, mine.at[1], other.at[0])
        pair_x = push(other, 0, pair_recv, 1, 1)
        block(2, mine.at[2], other.at[1])
        pair_y = push(other, 1, pair_recv, 2, 1)
        arrive([pair_x])
        add_into(mine.at[1], pair_recv.at[1])
        arrive([pair_y])
        add_into(mine.at[2], pair_recv.at[2])
        near, cross = pl.ds(0, TOK), pl.ds(TOK, TOK)
        part = push(mine, (1 + core, pl.ds(0, PART)), part_recv, None, 2 + 2 * core)
        saves.append(save(mine.at[1 + core, pl.ds(PART, TOK - PART)], first_keep, 0))
        saves.append(save(mine.at[1 + core, cross], first_cross, 3))
        for copy in saves[-2:]:
            copy.start()
        leave([pair_x])
        block(0, mine.at[0], other.at[0])
        pair_own = push(other, 0, pair_recv, 3, 1)
        arrive([pair_own])
        add_into(mine.at[0], pair_recv.at[3])
        mine_cross = push(mine, (0, cross), own_cross, None, 1)
        for k, cols in enumerate(chunks):
            arrive([hop[k]])
            add_into(mine.at[2 - core], hop_recv, cols, 64)
            for n, (rows, dst) in enumerate(((near, second_keep), (cross, second_cross))):
                saves.append(save(mine.at[2 - core, rows, cols], dst.at[:, cols], 5 + 2 * k + n))
                saves[-1].start()
        arrive([part])

        def add_part(t, _):
            r = pl.ds(pl.multiple_of(t * 16, 16), 16)
            mine[0, r, :] = mine[0, r, :] + part_recv[r, :]
            return 0

        lax.fori_loop(0, PART // 16, add_part, 0)
        saves.append(save(mine.at[0, near], own_keep, 4))
        saves[-1].start()
        arrive([mine_cross])
        leave([spec for spec in sent if spec not in pair_far and spec is not pair_x])
        for copy in saves:
            copy.wait()

    pl.run_scoped(blocks, pltpu.VMEM((4, PAIR, width), F32), pltpu.VMEM((2, PAIR, width), F32))


def row_kernel(asked_ref, c_ref, w_ref, x_ref, dy_ref, du_ref, dv_ref, wide_u, wide_v, part_u, part_v):
    n_rows, cols = du_ref.shape
    tiles = cols // LANES
    wide_step, part_step = n_rows + PAD, SLOTS + PAD
    part_size = tiles * part_step

    def clear(t, _):
        r = pl.multiple_of(t * 32, 32)
        for j in range(tiles):
            for wide in (wide_u, wide_v):
                wide[pl.ds(j * wide_step + r, 32), :] = jnp.zeros((32, LANES), F32)
        return 0

    lax.fori_loop(0, n_rows // 32, clear, 0)

    def product(q, slot):
        for coef, tok, part in ((c_ref, x_ref, part_u), (w_ref, dy_ref, part_v)):
            rows = tok[pl.ds(pl.multiple_of(q * TOK, TOK), TOK), :]
            full = jnp.dot(coef[q], jnp.concatenate([rows] * TERMS, axis=0), preferred_element_type=F32)
            for j in range(tiles):
                part[pl.ds(slot * part_size + j * part_step, SLOTS), :] = full[:, j * LANES:(j + 1) * LANES]

    product(0, 0)

    def device(q, _):
        product(lax.rem(q + 1, N_DEV), lax.rem(q + 1, 2))
        base = lax.rem(q, 2) * part_size
        for t in range(0, SLOTS, GROUP):
            rows = [asked_ref[q, t + u] for u in range(GROUP)]
            sums = [[wide[pl.ds(row, tiles, stride=wide_step), :] + part[pl.ds(base + t + u, tiles, stride=part_step), :]
                     for wide, part in ((wide_u, part_u), (wide_v, part_v))] for u, row in enumerate(rows)]
            for row, pair in zip(rows, sums):
                for wide, value in zip((wide_u, wide_v), pair):
                    wide[pl.ds(row, tiles, stride=wide_step), :] = value
        return 0

    lax.fori_loop(0, N_DEV, device, 0)

    def drain(t, _):
        r = pl.multiple_of(t * 32, 32)
        for j in range(tiles):
            for wide, out in ((wide_u, du_ref), (wide_v, dv_ref)):
                out[pl.ds(r, 32), j * LANES:(j + 1) * LANES] = wide[pl.ds(j * wide_step + r, 32), :].astype(BF16)
        return 0

    lax.fori_loop(0, n_rows // 32, drain, 0)


def join_kernel(fk_ref, fc_ref, sk_ref, sc_ref, ok_ref, oc_ref, y_ref, dx_ref):
    core = lax.rem(lax.axis_index("ep"), 2)
    half = y_ref.shape[1] // 2
    late = (pl.program_id(0) * y_ref.shape[0] >= PART).astype(F32)
    keep = ok_ref[...] + sk_ref[...]
    keep = jnp.where(late > 0, keep + fk_ref[...], keep).astype(BF16)
    cross = (oc_ref[...] + fc_ref[...] + sc_ref[...]).astype(BF16)
    here = pl.ds(pl.multiple_of(core * half, half), half)
    there = pl.ds(pl.multiple_of((1 - core) * half, half), half)
    for ref, cols in ((y_ref, slice(0, half)), (dx_ref, slice(half, 2 * half))):
        ref[:, here] = keep[:, cols]
        ref[:, there] = cross[:, cols]


def solution(mesh):
    tok_spec = P(('dp', 'ep'))
    table_spec = P('ep')

    def per_device(tokens, slot_ids, request_rows, gate_vals, grad_out, up_local, down_local):
        width = tokens.shape[1]
        rows_owner = up_local.shape[0]
        n_tok = N_DEV * TOK
        half = width // 2
        core = lax.axis_index('ep') % 2
        vmem, anyw = pl.BlockSpec(memory_space=pltpu.VMEM), pl.BlockSpec(memory_space=pl.ANY)
        shape = jax.ShapeDtypeStruct
        sums = shape((TOK, width), F32)
        x_all, dy_all, c_terms, w_terms, asked, first_keep, first_cross, second_keep, second_cross, own_keep, own_cross = pl.pallas_call(
            layer_kernel,
            in_specs=[anyw, anyw, vmem, vmem, vmem, anyw, anyw],
            out_specs=[anyw] * 2 + [vmem] * 3 + [anyw] * 6,
            out_shape=[shape((N_DEV, TOK, width), BF16)] * 2 + [shape((N_DEV, SLOTS, TERMS * TOK), BF16)] * 2 + [shape((N_DEV, SLOTS), I32)] + [shape((TOK - PART, width), F32)] + [sums] * 5,
            scratch_shapes=[
                pltpu.VMEM((N_DEV, TOK, width), BF16), pltpu.VMEM((N_DEV, TOK, width), BF16),
                pltpu.VMEM((N_DEV, TOK, SEL), I32), pltpu.VMEM((N_DEV, TOK, SEL), F32),
                pltpu.VMEM((N_DEV * SLOTS, width), BF16), pltpu.VMEM((N_DEV * SLOTS, width), BF16),
                pltpu.VMEM((4, PAIR, width), F32), pltpu.VMEM((PAIR, width), F32), pltpu.VMEM((PART, width), F32),
                pltpu.VMEM((N_DEV, SLOTS), I32), pltpu.SMEM((N_DEV, SLOTS), I32),
                pltpu.VMEM((SEL, PAIR), I32), pltpu.VMEM((SEL, PAIR), F32), pltpu.VMEM((SEL, PAIR), F32),
                pltpu.SemaphoreType.DMA((N_COPIES,)), pltpu.SemaphoreType.DMA((N_COPIES,)),
                pltpu.SemaphoreType.DMA((2,)), pltpu.SemaphoreType.DMA,
                pltpu.SemaphoreType.DMA((1,)), pltpu.SemaphoreType.DMA((5 + 2 * width // COLS,)),
            ],
            compiler_params=pltpu.CompilerParams(collective_id=0, has_side_effects=True, vmem_limit_bytes=VMEM_BYTES),
        )(tokens, grad_out, slot_ids.transpose(1, 2, 0), gate_vals.transpose(1, 2, 0), request_rows, up_local, down_local)

        first_hop = [(i, i ^ (2 if i % 2 == 0 else 4)) for i in range(N_DEV)]
        second_hop = [(i, i ^ (4 if i % 2 == 0 else 2)) for i in range(N_DEV)]
        over = lambda pairs: [(i, j ^ 1) for i, j in pairs]
        hop = lambda value, pairs: lax.ppermute(value, 'ep', pairs)

        def grad_rows():
            coef = pl.BlockSpec((N_DEV, SLOTS, TERMS * TOK), lambda i, a: (0, 0, 0))
            tok = pl.BlockSpec((n_tok, ROW_CHUNK), lambda i, a: (0, i))
            out = pl.BlockSpec((rows_owner, ROW_CHUNK), lambda i, a: (0, i))
            tiles = ROW_CHUNK // LANES
            return pl.pallas_call(
                row_kernel,
                grid_spec=pltpu.PrefetchScalarGridSpec(
                    num_scalar_prefetch=1,
                    grid=(width // ROW_CHUNK,),
                    in_specs=[coef, coef, tok, tok],
                    out_specs=[out, out],
                    scratch_shapes=[pltpu.VMEM((tiles * (rows_owner + PAD), LANES), F32)] * 2 + [pltpu.VMEM((2 * tiles * (SLOTS + PAD), LANES), F32)] * 2,
                ),
                out_shape=[shape((rows_owner, width), BF16)] * 2,
                compiler_params=pltpu.CompilerParams(vmem_limit_bytes=VMEM_BYTES),
                cost_estimate=pl.CostEstimate(flops=12 * rows_owner * width * n_tok, bytes_accessed=4 * rows_owner * width, transcendentals=0),
            )(asked, c_terms, w_terms, x_all.reshape(n_tok, width), dy_all.reshape(n_tok, width))

        got = (hop(first_keep, first_hop), hop(first_cross, over(first_hop)), hop(second_keep, second_hop), hop(second_cross, over(second_hop)))
        grad_up, grad_down = grad_rows()
        got, grad_up, grad_down = lax.optimization_barrier((got, grad_up, grad_down))
        block = 16
        rows = pl.BlockSpec((block, width), lambda i: (i, 0))
        late = pl.BlockSpec((block, width), lambda i: (jnp.maximum(i - PART // block, 0), 0))
        out_tokens, grad_tokens = pl.pallas_call(
            join_kernel,
            grid=(TOK // block,),
            in_specs=[late] + [rows] * 5,
            out_specs=[rows, rows],
            out_shape=[shape((TOK, width), BF16)] * 2,
            compiler_params=pltpu.CompilerParams(vmem_limit_bytes=VMEM_BYTES),
        )(*got, own_keep, own_cross)
        return out_tokens, grad_tokens, grad_up, grad_down

    return jax.shard_map(per_device, mesh=mesh, in_specs=(tok_spec, tok_spec, tok_spec, tok_spec, tok_spec, table_spec, table_spec), out_specs=(tok_spec, tok_spec, tok_spec, tok_spec), check_vma=False)
```

```python
import functools
import math
import jax
import jax.numpy as jnp
from jax import lax
from jax.experimental import pallas as pl
from jax.experimental.pallas import tpu as pltpu
from jax.sharding import PartitionSpec as P

F32, BF16, I32 = jnp.float32, jnp.bfloat16, jnp.int32
N_DEV, TOK, SLOTS, SEL = 8, 64, 128, 128
PAIR = 2 * TOK
TERMS = 3
CHUNK = 2048
ROW_CHUNK = 1024
GROUP = 16
LOW = 16
LANES = 128
PAD = 4
VMEM_BYTES = 62 * 1024 * 1024
MESH = pl.DeviceIdType.MESH


def gelu_pair(pre_act):
    normal_cdf = 0.5 * (1.0 + lax.erf(pre_act * (2.0 ** -0.5)))
    normal_pdf = jnp.exp(-0.5 * pre_act * pre_act) * ((2.0 * math.pi) ** -0.5)
    return pre_act * normal_cdf, normal_cdf + pre_act * normal_pdf


def split3(wide):
    high = wide.astype(BF16)
    rest = wide - high.astype(F32)
    mid = rest.astype(BF16)
    low = (rest - mid.astype(F32)).astype(BF16)
    return high, mid, low


N_COPIES = 64
SIDE_STEP, FAR_STEP, REST_STEP = 1, 4, 6
COLS = 512
PART = 32
TERM_SEM = 5 + 16


def layer_kernel(x_ref, dy_ref, slot_in, gate_in, req_in, up_ref, down_ref,
                 x_out, dy_out, c_out, w_out, asked_out, first_part, first_keep, first_cross, second_keep, second_cross, own_keep, own_cross,
                 x_all, dy_all, slot_all, gate_all, up_rows, down_rows, pair_recv, hop_recv, slot_ref, gate_ref, req_ref, c_buf, w_buf, asked, asked_s, slot_t, w_t, c_t,
                 send_sem, recv_sem, own_sem, smem_sem, in_sem, out_sem):
    me = lax.axis_index("ep")
    core = lax.rem(me, 2)
    n_rows, width = up_ref.shape
    half = width // 2
    steps = [(ref, out, col) for ref, out in ((up_ref, up_rows), (down_ref, down_rows)) for col in range(0, width, CHUNK)]
    tiles = CHUNK // LANES
    wide_step, pick_step = n_rows + PAD, SLOTS + PAD
    sent = []

    def descriptor(k, src, dst, mask):
        view = lambda ref, index: ref if index is None else ref.at[index]
        return pltpu.make_async_remote_copy(src_ref=view(*src), dst_ref=view(*dst), send_sem=send_sem.at[k], recv_sem=recv_sem.at[k],
                                            device_id={"ep": me ^ mask}, device_id_type=MESH)

    def push(src, src_index, dst, dst_index, mask):
        spec = (len(sent), (src, src_index), (dst, dst_index), mask)
        descriptor(*spec).start()
        sent.append(spec)
        return spec

    def arrive(specs):
        for spec in specs:
            descriptor(*spec).wait_recv()

    def leave(specs):
        for spec in specs:
            descriptor(*spec).wait_send()

    own = [pltpu.make_async_copy(src, dst.at[0], own_sem.at[k]) for k, (src, dst) in enumerate(((x_ref, x_all), (dy_ref, dy_all)))]
    small = [pltpu.make_async_copy(src, dst, own_sem.at[2 + k]) for k, (src, dst) in enumerate(((slot_in, slot_ref), (gate_in, gate_ref), (req_in, req_ref)))]
    barrier = pltpu.get_barrier_semaphore()
    for b in range(1, N_DEV):
        pl.semaphore_signal(barrier, inc=1, device_id={"ep": me ^ b}, device_id_type=MESH)
    for copy in small + own:
        copy.start()
    for copy in small:
        copy.wait()
    slot_all[0] = slot_ref[...].reshape(SEL, TOK).T
    gate_all[0] = gate_ref[...].reshape(SEL, TOK).T
    pl.semaphore_wait(barrier, N_DEV - 1)

    asks = [push(req_ref, (0, pl.ds(me ^ b, 1)), asked, pl.ds(b, 1), b) for b in range(1, N_DEV)]
    first = [push(x_ref, None, x_all, 4, 4), push(dy_ref, None, dy_all, 2, 2)]
    near_own = [push(x_ref, None, x_all, 1, 1), push(dy_ref, None, dy_all, 1, 1)]
    low, top = pl.ds(0, LOW), pl.ds(LOW, TOK - LOW)
    second = [push(x_ref, low, x_all, (2, low), 2), push(dy_ref, low, dy_all, (4, low), 4)]
    asked[pl.ds(0, 1), :] = req_ref[0, pl.ds(me, 1), :]
    arrive(asks)
    to_smem = pltpu.make_async_copy(asked, asked_s, smem_sem)
    to_smem.start()
    to_smem.wait()
    keep_asked = pltpu.make_async_copy(asked, asked_out, own_sem.at[5])
    keep_asked.start()

    def gather_all(table, wide, picked):
        def fetch(k):
            ref, _, col = steps[k]
            return pltpu.make_async_copy(ref.at[:, pl.ds(col, CHUNK)], table, in_sem.at[0])

        fetch(0).start()
        for sub in range(2 * len(steps)):
            if sub == SIDE_STEP:
                side = [push(gate_all, 0, gate_all, 4, 4), push(slot_all, 0, slot_all, 2, 2)]
                near_own.extend([push(gate_all, 0, gate_all, 1, 1), push(slot_all, 0, slot_all, 1, 1)])
            if sub == FAR_STEP:
                arrive(first)
                far = [push(x_all, 4, x_all, 6, 2), push(dy_all, 2, dy_all, 6, 4)]
                near_first = [push(x_all, 4, x_all, 5, 1), push(dy_all, 2, dy_all, 3, 1)]
            if sub == REST_STEP:
                arrive(side)
                far.extend([push(gate_all, 4, gate_all, 6, 2), push(slot_all, 2, slot_all, 6, 4)])
                near_first.extend([push(gate_all, 4, gate_all, 5, 1), push(slot_all, 2, slot_all, 3, 1)])
                second.extend([push(gate_all, 0, gate_all, 2, 2), push(slot_all, 0, slot_all, 4, 4)])
                second.extend([push(x_ref, top, x_all, (2, top), 2), push(dy_ref, top, dy_all, (4, top), 4)])
            k = sub // 2
            if sub % 2 == 0:
                fetch(k).wait()

                def fill(t, _):
                    r = pl.multiple_of(t * 32, 32)
                    for j in range(tiles):
                        wide[pl.ds(j * wide_step + r, 32), :] = table[pl.ds(r, 32), j * LANES:(j + 1) * LANES].astype(F32)
                    return 0

                lax.fori_loop(0, n_rows // 32, fill, 0)
                if k + 1 < len(steps):
                    fetch(k + 1).start()
            else:
                _, rows_ref, col = steps[k]

                def pick_device(b, _):
                    def pick(t, _):
                        for u in range(16):
                            row = asked_s[b, t * 16 + u]
                            picked[pl.ds(t * 16 + u, tiles, stride=pick_step), :] = wide[pl.ds(row, tiles, stride=wide_step), :]
                        return 0

                    lax.fori_loop(0, SLOTS // 16, pick, 0)

                    def drain(t, _):
                        r = pl.multiple_of(t * 32, 32)
                        into = pl.multiple_of(b * SLOTS + t * 32, 32)
                        for j in range(tiles):
                            rows_ref[pl.ds(into, 32), col + j * LANES:col + (j + 1) * LANES] = picked[pl.ds(j * pick_step + r, 32), :].astype(BF16)
                        return 0

                    return lax.fori_loop(0, SLOTS // 32, drain, 0)

                lax.fori_loop(0, N_DEV, pick_device, 0)
        return far, near_first

    kept = []
    pl.run_scoped(
        lambda *bufs: kept.append(gather_all(*bufs)),
        pltpu.VMEM((n_rows, CHUNK), BF16), pltpu.VMEM((tiles * wide_step, LANES), F32), pltpu.VMEM((tiles * pick_step, LANES), F32),
    )
    far, near_first = kept[0]
    for copy in own:
        copy.wait()
    keep_asked.wait()
    dims = (((1,), (1,)), ((), ()))
    row_iota = lax.broadcasted_iota(I32, (SLOTS, PAIR), 0)
    block_diag = (lax.broadcasted_iota(I32, (PAIR, 2 * SLOTS), 0) < TOK) == (lax.broadcasted_iota(I32, (PAIR, 2 * SLOTS), 1) < SLOTS)

    def front(r):
        toks, rows = pl.ds(2 * r, 2), pl.ds(2 * r * SLOTS, 2 * SLOTS)

        def dots(tok, table):
            full = lax.dot_general(tok[toks].reshape(PAIR, width), table[rows, :], dims, preferred_element_type=F32)
            return jnp.concatenate([full[:TOK, :SLOTS], full[TOK:, SLOTS:]], axis=0)

        act, slope = gelu_pair(dots(x_all, up_rows))
        slope = slope * dots(dy_all, down_rows)
        local = slot_all[toks].reshape(PAIR, SEL) - me * SLOTS
        valid = (local >= 0) & (local < SLOTS)
        index = jnp.where(valid, local, 0)
        act = jnp.take_along_axis(act, index, axis=1)
        slope = jnp.take_along_axis(slope, index, axis=1)
        gate = gate_all[toks].reshape(PAIR, SEL)
        w_t[...] = jnp.where(valid, (gate * act).astype(BF16).astype(F32), 0.0).T
        c_t[...] = jnp.where(valid, (gate * slope).astype(BF16).astype(F32), 0.0).T
        slot_t[...] = jnp.where(valid, local, -1).T

        def step(s, acc):
            acc_w, acc_c = acc
            hit = row_iota == slot_t[pl.ds(s, 1), :]
            acc_w += jnp.where(hit, w_t[pl.ds(s, 1), :], 0.0)
            acc_c += jnp.where(hit, c_t[pl.ds(s, 1), :], 0.0)
            return acc_w, acc_c

        zero = jnp.zeros((SLOTS, PAIR), F32)
        acc_w, acc_c = lax.fori_loop(0, SEL, step, (zero, zero), unroll=4)
        for ref, acc in ((w_buf, acc_w), (c_buf, acc_c)):
            terms = split3(acc)
            for j in range(2):
                ref[2 * r + j] = jnp.concatenate([term[:, j * TOK:(j + 1) * TOK] for term in terms], axis=1)

        def spread(acc):
            both = jnp.concatenate([acc.T, acc.T], axis=1)
            return split3(jnp.where(block_diag, both, 0.0))

        return spread(acc_w), spread(acc_c)

    def columns(r, terms, col, mine, other):
        rows = pl.ds(2 * r * SLOTS, 2 * SLOTS)
        table, terms = (down_rows, terms[0]) if col < half else (up_rows, terms[1])
        here = pl.ds(pl.multiple_of(core * half + col % half, COLS), COLS)
        there = pl.ds(pl.multiple_of((1 - core) * half + col % half, COLS), COLS)
        mine[:, col:col + COLS] = sum(jnp.dot(term, table[rows, here], preferred_element_type=F32) for term in terms)
        part = sum(jnp.dot(term, table[rows, there], preferred_element_type=F32) for term in terms)
        other[:TOK, col:col + COLS] = part[TOK:]
        other[TOK:, col:col + COLS] = part[:TOK]

    def block(r, mine, other):
        terms = front(r)
        for col in range(0, width, COLS):
            columns(r, terms, col, mine, other)

    def add_into(dst, src, cols=slice(None), step=16):
        def add(t, _):
            r = pl.ds(pl.multiple_of(t * step, step), step)
            dst[r, cols] = dst[r, cols] + src[r, cols]
            return 0

        lax.fori_loop(0, PAIR // step, add, 0)

    def blocks(mine, other):
        save = lambda src, dst, k: pltpu.make_async_copy(src, dst, out_sem.at[k])
        saves = []

        def keep_terms(r):
            for n, (src, dst) in enumerate(((c_buf, c_out), (w_buf, w_out))):
                saves.append(save(src.at[pl.ds(2 * r, 2)], dst.at[pl.ds(2 * r, 2)], TERM_SEM + 2 * r + n))
                saves[-1].start()

        arrive(near_own)
        arrive(far)
        near_far = [push(ref, 6, ref, 7, 1) for ref in (gate_all, slot_all, x_all, dy_all)]
        arrive(near_first + near_far)
        terms = front(3)
        pair_far, hop = [], []
        chunks = [pl.ds(col, COLS) for col in range(0, width, COLS)]
        every = slice(None)
        for cols in chunks:
            columns(3, terms, cols.start, mine.at[3], other.at[0])
            pair_far.append(push(other, (0, every, cols), pair_recv, (0, every, cols), 1))
        for k, cols in enumerate(chunks):
            arrive([pair_far[k]])
            add_into(mine.at[3], pair_recv.at[0], cols, 64)
            hop.append(push(mine, (3, every, cols), hop_recv, (every, cols), 2 + 2 * core))
        keep_terms(3)
        arrive(second)
        near_second = [push(gate_all, 2, gate_all, 3, 1), push(slot_all, 4, slot_all, 5, 1), push(x_all, 2, x_all, 3, 1), push(dy_all, 4, dy_all, 5, 1)]
        arrive(near_second)
        for k, (src, dst) in enumerate(((x_all, x_out), (dy_all, dy_out))):
            saves.append(save(src, dst, 1 + k))
            saves[-1].start()
        leave(pair_far)
        block(1, mine.at[1], other.at[0])
        pair_x = push(other, 0, pair_recv, 1, 1)
        keep_terms(1)
        block(2, mine.at[2], other.at[1])
        pair_y = push(other, 1, pair_recv, 2, 1)
        keep_terms(2)
        arrive([pair_x])
        add_into(mine.at[1], pair_recv.at[1])
        arrive([pair_y])
        add_into(mine.at[2], pair_recv.at[2])
        near, cross = pl.ds(0, TOK), pl.ds(TOK, TOK)
        part = push(mine, (1 + core, pl.ds(0, PART)), first_part, None, 2 + 2 * core)
        saves.append(save(mine.at[1 + core, pl.ds(PART, TOK - PART)], first_keep, 0))
        saves.append(save(mine.at[1 + core, cross], first_cross, 3))
        for copy in saves[-2:]:
            copy.start()
        leave([pair_x])
        block(0, mine.at[0], other.at[0])
        pair_own = push(other, 0, pair_recv, 3, 1)
        keep_terms(0)
        arrive([pair_own])
        add_into(mine.at[0], pair_recv.at[3])
        mine_cross = push(mine, (0, cross), own_cross, None, 1)
        saves.append(save(mine.at[0, near], own_keep, 4))
        saves[-1].start()
        for k, cols in enumerate(chunks):
            arrive([hop[k]])
            add_into(mine.at[2 - core], hop_recv, cols, 64)
            for n, (rows, dst) in enumerate(((near, second_keep), (cross, second_cross))):
                saves.append(save(mine.at[2 - core, rows, cols], dst.at[:, cols], 5 + 2 * k + n))
                saves[-1].start()
        arrive([part, mine_cross])
        leave([spec for spec in sent if spec not in pair_far and spec is not pair_x])
        for copy in saves:
            copy.wait()

    pl.run_scoped(blocks, pltpu.VMEM((4, PAIR, width), F32), pltpu.VMEM((2, PAIR, width), F32))


def row_kernel(asked_ref, c_ref, w_ref, x_ref, dy_ref, du_ref, dv_ref, wide_u, wide_v, part_u, part_v):
    n_rows, cols = du_ref.shape
    tiles = cols // LANES
    wide_step, part_step = n_rows + PAD, SLOTS + PAD
    part_size = tiles * part_step

    def clear(t, _):
        r = pl.multiple_of(t * 32, 32)
        for j in range(tiles):
            for wide in (wide_u, wide_v):
                wide[pl.ds(j * wide_step + r, 32), :] = jnp.zeros((32, LANES), F32)
        return 0

    lax.fori_loop(0, n_rows // 32, clear, 0)

    def product(q, slot):
        for coef, tok, part in ((c_ref, x_ref, part_u), (w_ref, dy_ref, part_v)):
            rows = tok[pl.ds(pl.multiple_of(q * TOK, TOK), TOK), :]
            full = jnp.dot(coef[q], jnp.concatenate([rows] * TERMS, axis=0), preferred_element_type=F32)
            for j in range(tiles):
                part[pl.ds(slot * part_size + j * part_step, SLOTS), :] = full[:, j * LANES:(j + 1) * LANES]

    product(0, 0)

    def device(q, _):
        product(lax.rem(q + 1, N_DEV), lax.rem(q + 1, 2))
        base = lax.rem(q, 2) * part_size
        for t in range(0, SLOTS, GROUP):
            rows = [asked_ref[q, t + u] for u in range(GROUP)]
            sums = [[wide[pl.ds(row, tiles, stride=wide_step), :] + part[pl.ds(base + t + u, tiles, stride=part_step), :]
                     for wide, part in ((wide_u, part_u), (wide_v, part_v))] for u, row in enumerate(rows)]
            for row, pair in zip(rows, sums):
                for wide, value in zip((wide_u, wide_v), pair):
                    wide[pl.ds(row, tiles, stride=wide_step), :] = value
        return 0

    lax.fori_loop(0, N_DEV, device, 0)

    def drain(t, _):
        r = pl.multiple_of(t * 32, 32)
        for j in range(tiles):
            for wide, out in ((wide_u, du_ref), (wide_v, dv_ref)):
                out[pl.ds(r, 32), j * LANES:(j + 1) * LANES] = wide[pl.ds(j * wide_step + r, 32), :].astype(BF16)
        return 0

    lax.fori_loop(0, n_rows // 32, drain, 0)


def join_kernel(fp_ref, fk_ref, fc_ref, sk_ref, sc_ref, ok_ref, oc_ref, y_ref, dx_ref):
    core = lax.rem(lax.axis_index("ep"), 2)
    half = y_ref.shape[1] // 2
    late = pl.program_id(0) * y_ref.shape[0] >= PART
    keep = (ok_ref[...] + jnp.where(late, fk_ref[...], fp_ref[...]) + sk_ref[...]).astype(BF16)
    cross = (oc_ref[...] + fc_ref[...] + sc_ref[...]).astype(BF16)
    here = pl.ds(pl.multiple_of(core * half, half), half)
    there = pl.ds(pl.multiple_of((1 - core) * half, half), half)
    for ref, cols in ((y_ref, slice(0, half)), (dx_ref, slice(half, 2 * half))):
        ref[:, here] = keep[:, cols]
        ref[:, there] = cross[:, cols]


def solution(mesh):
    tok_spec = P(('dp', 'ep'))
    table_spec = P('ep')

    def per_device(tokens, slot_ids, request_rows, gate_vals, grad_out, up_local, down_local):
        width = tokens.shape[1]
        rows_owner = up_local.shape[0]
        heads, top_k = slot_ids.shape[1:]
        n_tok = N_DEV * TOK
        half = width // 2
        core = lax.axis_index('ep') % 2
        anyw = pl.BlockSpec(memory_space=pl.ANY)
        shape = jax.ShapeDtypeStruct
        sums = shape((TOK, width), F32)
        x_all, dy_all, c_terms, w_terms, asked, first_part, first_keep, first_cross, second_keep, second_cross, own_keep, own_cross = pl.pallas_call(
            layer_kernel,
            in_specs=[anyw] * 7,
            out_specs=[anyw] * 12,
            out_shape=[shape((N_DEV, TOK, width), BF16)] * 2 + [shape((N_DEV, SLOTS, TERMS * TOK), BF16)] * 2 + [shape((N_DEV, SLOTS), I32)] + [shape((PART, width), F32), shape((TOK - PART, width), F32)] + [sums] * 5,
            scratch_shapes=[
                pltpu.VMEM((N_DEV, TOK, width), BF16), pltpu.VMEM((N_DEV, TOK, width), BF16),
                pltpu.VMEM((N_DEV, TOK, SEL), I32), pltpu.VMEM((N_DEV, TOK, SEL), F32),
                pltpu.VMEM((N_DEV * SLOTS, width), BF16), pltpu.VMEM((N_DEV * SLOTS, width), BF16),
                pltpu.VMEM((4, PAIR, width), F32), pltpu.VMEM((PAIR, width), F32),
                pltpu.VMEM((heads, top_k, TOK), I32), pltpu.VMEM((heads, top_k, TOK), F32), pltpu.VMEM((1, N_DEV, SLOTS), I32),
                pltpu.VMEM((N_DEV, SLOTS, TERMS * TOK), BF16), pltpu.VMEM((N_DEV, SLOTS, TERMS * TOK), BF16),
                pltpu.VMEM((N_DEV, SLOTS), I32), pltpu.SMEM((N_DEV, SLOTS), I32),
                pltpu.VMEM((SEL, PAIR), I32), pltpu.VMEM((SEL, PAIR), F32), pltpu.VMEM((SEL, PAIR), F32),
                pltpu.SemaphoreType.DMA((N_COPIES,)), pltpu.SemaphoreType.DMA((N_COPIES,)),
                pltpu.SemaphoreType.DMA((6,)), pltpu.SemaphoreType.DMA,
                pltpu.SemaphoreType.DMA((1,)), pltpu.SemaphoreType.DMA((TERM_SEM + N_DEV,)),
            ],
            compiler_params=pltpu.CompilerParams(collective_id=0, has_side_effects=True, vmem_limit_bytes=VMEM_BYTES),
        )(tokens, grad_out, slot_ids.transpose(1, 2, 0), gate_vals.transpose(1, 2, 0), request_rows, up_local, down_local)

        first_hop = [(i, i ^ (2 if i % 2 == 0 else 4)) for i in range(N_DEV)]
        second_hop = [(i, i ^ (4 if i % 2 == 0 else 2)) for i in range(N_DEV)]
        over = lambda pairs: [(i, j ^ 1) for i, j in pairs]
        hop = lambda value, pairs: lax.ppermute(value, 'ep', pairs)

        def grad_rows():
            coef = pl.BlockSpec((N_DEV, SLOTS, TERMS * TOK), lambda i, a: (0, 0, 0))
            tok = pl.BlockSpec((n_tok, ROW_CHUNK), lambda i, a: (0, i))
            out = pl.BlockSpec((rows_owner, ROW_CHUNK), lambda i, a: (0, i))
            tiles = ROW_CHUNK // LANES
            return pl.pallas_call(
                row_kernel,
                grid_spec=pltpu.PrefetchScalarGridSpec(
                    num_scalar_prefetch=1,
                    grid=(width // ROW_CHUNK,),
                    in_specs=[coef, coef, tok, tok],
                    out_specs=[out, out],
                    scratch_shapes=[pltpu.VMEM((tiles * (rows_owner + PAD), LANES), F32)] * 2 + [pltpu.VMEM((2 * tiles * (SLOTS + PAD), LANES), F32)] * 2,
                ),
                out_shape=[shape((rows_owner, width), BF16)] * 2,
                compiler_params=pltpu.CompilerParams(vmem_limit_bytes=VMEM_BYTES),
                cost_estimate=pl.CostEstimate(flops=12 * rows_owner * width * n_tok, bytes_accessed=4 * rows_owner * width, transcendentals=0),
            )(asked, c_terms, w_terms, x_all.reshape(n_tok, width), dy_all.reshape(n_tok, width))

        got = (hop(first_keep, first_hop), hop(first_cross, over(first_hop)), hop(second_keep, second_hop), hop(second_cross, over(second_hop)))
        grad_up, grad_down = grad_rows()
        got, grad_up, grad_down = lax.optimization_barrier((got, grad_up, grad_down))
        block = 32
        rows = pl.BlockSpec((block, width), lambda i: (i, 0))
        early = pl.BlockSpec((block, width), lambda i: (0, 0))
        out_tokens, grad_tokens = pl.pallas_call(
            join_kernel,
            grid=(TOK // block,),
            in_specs=[early] * 2 + [rows] * 5,
            out_specs=[rows, rows],
            out_shape=[shape((TOK, width), BF16)] * 2,
            compiler_params=pltpu.CompilerParams(vmem_limit_bytes=16 * 1024 * 1024),
        )(first_part, *got, own_keep, own_cross)
        return out_tokens, grad_tokens, grad_up, grad_down

    return jax.shard_map(per_device, mesh=mesh, in_specs=(tok_spec, tok_spec, tok_spec, tok_spec, tok_spec, table_spec, table_spec), out_specs=(tok_spec, tok_spec, tok_spec, tok_spec), check_vma=False)
```

```python
import functools
import math
import jax
import jax.numpy as jnp
from jax import lax
from jax.experimental import pallas as pl
from jax.experimental.pallas import tpu as pltpu
from jax.sharding import PartitionSpec as P

F32, BF16, I32 = jnp.float32, jnp.bfloat16, jnp.int32
N_DEV, TOK, SLOTS, SEL = 8, 64, 128, 128
PAIR = 2 * TOK
TERMS = 3
CHUNK = 2048
ROW_CHUNK = 1024
GROUP = 16
LOW = 16
LANES = 128
PAD = 4
VMEM_BYTES = 62 * 1024 * 1024
MESH = pl.DeviceIdType.MESH


def gelu_pair(pre_act):
    normal_cdf = 0.5 * (1.0 + lax.erf(pre_act * (2.0 ** -0.5)))
    normal_pdf = jnp.exp(-0.5 * pre_act * pre_act) * ((2.0 * math.pi) ** -0.5)
    return pre_act * normal_cdf, normal_cdf + pre_act * normal_pdf


def split3(wide):
    high = wide.astype(BF16)
    rest = wide - high.astype(F32)
    mid = rest.astype(BF16)
    low = (rest - mid.astype(F32)).astype(BF16)
    return high, mid, low


N_COPIES = 64
SIDE_STEP, FAR_STEP, REST_STEP = 1, 4, 6
COLS = 512
PART = 32
TERM_SEM = 5 + 16


def layer_kernel(x_ref, dy_ref, slot_in, gate_in, req_in, up_ref, down_ref,
                 x_out, dy_out, c_out, w_out, asked_out, first_part, first_keep, first_cross, second_keep, second_cross, own_keep, own_cross,
                 x_all, dy_all, slot_all, gate_all, up_rows, down_rows, pair_recv, hop_recv, slot_ref, gate_ref, req_ref, c_buf, w_buf, asked, asked_s, slot_t, w_t, c_t,
                 send_sem, recv_sem, own_sem, smem_sem, in_sem, out_sem):
    me = lax.axis_index("ep")
    core = lax.rem(me, 2)
    n_rows, width = up_ref.shape
    half = width // 2
    steps = [(ref, out, col) for ref, out in ((up_ref, up_rows), (down_ref, down_rows)) for col in range(0, width, CHUNK)]
    tiles = CHUNK // LANES
    wide_step, pick_step = n_rows + PAD, SLOTS + PAD
    sent = []

    def descriptor(k, src, dst, mask):
        view = lambda ref, index: ref if index is None else ref.at[index]
        return pltpu.make_async_remote_copy(src_ref=view(*src), dst_ref=view(*dst), send_sem=send_sem.at[k], recv_sem=recv_sem.at[k],
                                            device_id={"ep": me ^ mask}, device_id_type=MESH)

    def push(src, src_index, dst, dst_index, mask):
        spec = (len(sent), (src, src_index), (dst, dst_index), mask)
        descriptor(*spec).start()
        sent.append(spec)
        return spec

    def arrive(specs):
        for spec in specs:
            descriptor(*spec).wait_recv()

    def leave(specs):
        for spec in specs:
            descriptor(*spec).wait_send()

    own = [pltpu.make_async_copy(src, dst.at[0], own_sem.at[k]) for k, (src, dst) in enumerate(((x_ref, x_all), (dy_ref, dy_all)))]
    small = [pltpu.make_async_copy(src, dst, own_sem.at[2 + k]) for k, (src, dst) in enumerate(((slot_in, slot_ref), (gate_in, gate_ref), (req_in, req_ref)))]
    barrier = pltpu.get_barrier_semaphore()
    for b in range(1, N_DEV):
        pl.semaphore_signal(barrier, inc=1, device_id={"ep": me ^ b}, device_id_type=MESH)
    for copy in small + own:
        copy.start()
    for copy in small:
        copy.wait()
    slot_all[0] = slot_ref[...].reshape(SEL, TOK).T
    gate_all[0] = gate_ref[...].reshape(SEL, TOK).T
    pl.semaphore_wait(barrier, N_DEV - 1)

    asks = [push(req_ref, (0, pl.ds(me ^ b, 1)), asked, pl.ds(b, 1), b) for b in range(1, N_DEV)]
    first = [push(x_ref, None, x_all, 4, 4), push(dy_ref, None, dy_all, 2, 2)]
    near_own = [push(x_ref, None, x_all, 1, 1), push(dy_ref, None, dy_all, 1, 1)]
    low, top = pl.ds(0, LOW), pl.ds(LOW, TOK - LOW)
    second = [push(x_ref, low, x_all, (2, low), 2), push(dy_ref, low, dy_all, (4, low), 4)]
    asked[pl.ds(0, 1), :] = req_ref[0, pl.ds(me, 1), :]
    arrive(asks)
    to_smem = pltpu.make_async_copy(asked, asked_s, smem_sem)
    to_smem.start()
    to_smem.wait()
    keep_asked = pltpu.make_async_copy(asked, asked_out, own_sem.at[5])
    keep_asked.start()

    def gather_all(table, wide, picked):
        def fetch(k):
            ref, _, col = steps[k]
            return pltpu.make_async_copy(ref.at[:, pl.ds(col, CHUNK)], table, in_sem.at[0])

        fetch(0).start()
        for sub in range(2 * len(steps)):
            if sub == SIDE_STEP:
                side = [push(gate_all, 0, gate_all, 4, 4), push(slot_all, 0, slot_all, 2, 2)]
                near_own.extend([push(gate_all, 0, gate_all, 1, 1), push(slot_all, 0, slot_all, 1, 1)])
            if sub == FAR_STEP:
                arrive(first)
                far = [push(x_all, 4, x_all, 6, 2), push(dy_all, 2, dy_all, 6, 4)]
                near_first = [push(x_all, 4, x_all, 5, 1), push(dy_all, 2, dy_all, 3, 1)]
            if sub == REST_STEP:
                arrive(side)
                far.extend([push(gate_all, 4, gate_all, 6, 2), push(slot_all, 2, slot_all, 6, 4)])
                near_first.extend([push(gate_all, 4, gate_all, 5, 1), push(slot_all, 2, slot_all, 3, 1)])
                second.extend([push(gate_all, 0, gate_all, 2, 2), push(slot_all, 0, slot_all, 4, 4)])
                second.extend([push(x_ref, top, x_all, (2, top), 2), push(dy_ref, top, dy_all, (4, top), 4)])
            k = sub // 2
            if sub % 2 == 0:
                fetch(k).wait()

                def fill(t, _):
                    r = pl.multiple_of(t * 32, 32)
                    for j in range(tiles):
                        wide[pl.ds(j * wide_step + r, 32), :] = table[pl.ds(r, 32), j * LANES:(j + 1) * LANES].astype(F32)
                    return 0

                lax.fori_loop(0, n_rows // 32, fill, 0)
                if k + 1 < len(steps):
                    fetch(k + 1).start()
            else:
                _, rows_ref, col = steps[k]

                def pick_device(b, _):
                    def pick(t, _):
                        for u in range(16):
                            row = asked_s[b, t * 16 + u]
                            picked[pl.ds(t * 16 + u, tiles, stride=pick_step), :] = wide[pl.ds(row, tiles, stride=wide_step), :]
                        return 0

                    lax.fori_loop(0, SLOTS // 16, pick, 0)

                    def drain(t, _):
                        r = pl.multiple_of(t * 32, 32)
                        into = pl.multiple_of(b * SLOTS + t * 32, 32)
                        for j in range(tiles):
                            rows_ref[pl.ds(into, 32), col + j * LANES:col + (j + 1) * LANES] = picked[pl.ds(j * pick_step + r, 32), :].astype(BF16)
                        return 0

                    return lax.fori_loop(0, SLOTS // 32, drain, 0)

                lax.fori_loop(0, N_DEV, pick_device, 0)
        return far, near_first

    kept = []
    pl.run_scoped(
        lambda *bufs: kept.append(gather_all(*bufs)),
        pltpu.VMEM((n_rows, CHUNK), BF16), pltpu.VMEM((tiles * wide_step, LANES), F32), pltpu.VMEM((tiles * pick_step, LANES), F32),
    )
    far, near_first = kept[0]
    for copy in own:
        copy.wait()
    keep_asked.wait()
    dims = (((1,), (1,)), ((), ()))
    row_iota = lax.broadcasted_iota(I32, (SLOTS, PAIR), 0)
    block_diag = (lax.broadcasted_iota(I32, (PAIR, 2 * SLOTS), 0) < TOK) == (lax.broadcasted_iota(I32, (PAIR, 2 * SLOTS), 1) < SLOTS)

    def front(r):
        toks, rows = pl.ds(2 * r, 2), pl.ds(2 * r * SLOTS, 2 * SLOTS)

        def dots(tok, table):
            full = lax.dot_general(table[rows, :], tok[toks].reshape(PAIR, width), dims, preferred_element_type=F32).T
            return jnp.concatenate([full[:TOK, :SLOTS], full[TOK:, SLOTS:]], axis=0)

        act, slope = gelu_pair(dots(x_all, up_rows))
        slope = slope * dots(dy_all, down_rows)
        local = slot_all[toks].reshape(PAIR, SEL) - me * SLOTS
        valid = (local >= 0) & (local < SLOTS)
        index = jnp.where(valid, local, 0)
        act = jnp.take_along_axis(act, index, axis=1)
        slope = jnp.take_along_axis(slope, index, axis=1)
        gate = gate_all[toks].reshape(PAIR, SEL)
        w_t[...] = jnp.where(valid, (gate * act).astype(BF16).astype(F32), 0.0).T
        c_t[...] = jnp.where(valid, (gate * slope).astype(BF16).astype(F32), 0.0).T
        slot_t[...] = jnp.where(valid, local, -1).T

        def step(s, acc):
            acc_w, acc_c = acc
            hit = row_iota == slot_t[pl.ds(s, 1), :]
            acc_w += jnp.where(hit, w_t[pl.ds(s, 1), :], 0.0)
            acc_c += jnp.where(hit, c_t[pl.ds(s, 1), :], 0.0)
            return acc_w, acc_c

        zero = jnp.zeros((SLOTS, PAIR), F32)
        acc_w, acc_c = lax.fori_loop(0, SEL, step, (zero, zero), unroll=8)
        for ref, acc in ((w_buf, acc_w), (c_buf, acc_c)):
            terms = split3(acc)
            for j in range(2):
                ref[2 * r + j] = jnp.concatenate([term[:, j * TOK:(j + 1) * TOK] for term in terms], axis=1)

        def spread(acc):
            both = jnp.concatenate([acc.T, acc.T], axis=1)
            return split3(jnp.where(block_diag, both, 0.0))

        return spread(acc_w), spread(acc_c)

    def columns(r, terms, col, mine, other):
        rows = pl.ds(2 * r * SLOTS, 2 * SLOTS)
        table, terms = (down_rows, terms[0]) if col < half else (up_rows, terms[1])
        here = pl.ds(pl.multiple_of(core * half + col % half, COLS), COLS)
        there = pl.ds(pl.multiple_of((1 - core) * half + col % half, COLS), COLS)
        mine[:, col:col + COLS] = sum(jnp.dot(term, table[rows, here], preferred_element_type=F32) for term in terms)
        part = sum(jnp.dot(term, table[rows, there], preferred_element_type=F32) for term in terms)
        other[:TOK, col:col + COLS] = part[TOK:]
        other[TOK:, col:col + COLS] = part[:TOK]

    def block(r, mine, other):
        terms = front(r)
        for col in range(0, width, COLS):
            columns(r, terms, col, mine, other)

    def add_into(dst, src, cols=slice(None), step=16):
        def add(t, _):
            r = pl.ds(pl.multiple_of(t * step, step), step)
            dst[r, cols] = dst[r, cols] + src[r, cols]
            return 0

        lax.fori_loop(0, PAIR // step, add, 0)

    def blocks(mine, other):
        save = lambda src, dst, k: pltpu.make_async_copy(src, dst, out_sem.at[k])
        saves = []

        def keep_terms(r):
            for n, (src, dst) in enumerate(((c_buf, c_out), (w_buf, w_out))):
                saves.append(save(src.at[pl.ds(2 * r, 2)], dst.at[pl.ds(2 * r, 2)], TERM_SEM + 2 * r + n))
                saves[-1].start()

        arrive(near_own)
        arrive(far)
        near_far = [push(ref, 6, ref, 7, 1) for ref in (gate_all, slot_all, x_all, dy_all)]
        arrive(near_first + near_far)
        terms = front(3)
        pair_far, hop = [], []
        chunks = [pl.ds(col, COLS) for col in range(0, width, COLS)]
        every = slice(None)
        for cols in chunks:
            columns(3, terms, cols.start, mine.at[3], other.at[0])
            pair_far.append(push(other, (0, every, cols), pair_recv, (0, every, cols), 1))
        for k, cols in enumerate(chunks):
            arrive([pair_far[k]])
            add_into(mine.at[3], pair_recv.at[0], cols, 64)
            hop.append(push(mine, (3, every, cols), hop_recv, (every, cols), 2 + 2 * core))
        keep_terms(3)
        arrive(second)
        near_second = [push(gate_all, 2, gate_all, 3, 1), push(slot_all, 4, slot_all, 5, 1), push(x_all, 2, x_all, 3, 1), push(dy_all, 4, dy_all, 5, 1)]
        arrive(near_second)
        for k, (src, dst) in enumerate(((x_all, x_out), (dy_all, dy_out))):
            saves.append(save(src, dst, 1 + k))
            saves[-1].start()
        leave(pair_far)
        block(1, mine.at[1], other.at[0])
        pair_x = push(other, 0, pair_recv, 1, 1)
        keep_terms(1)
        block(2, mine.at[2], other.at[1])
        pair_y = push(other, 1, pair_recv, 2, 1)
        keep_terms(2)
        arrive([pair_x])
        add_into(mine.at[1], pair_recv.at[1])
        arrive([pair_y])
        add_into(mine.at[2], pair_recv.at[2])
        near, cross = pl.ds(0, TOK), pl.ds(TOK, TOK)
        part = push(mine, (1 + core, pl.ds(0, PART)), first_part, None, 2 + 2 * core)
        saves.append(save(mine.at[1 + core, pl.ds(PART, TOK - PART)], first_keep, 0))
        saves.append(save(mine.at[1 + core, cross], first_cross, 3))
        for copy in saves[-2:]:
            copy.start()
        leave([pair_x])
        block(0, mine.at[0], other.at[0])
        pair_own = push(other, 0, pair_recv, 3, 1)
        keep_terms(0)
        arrive([pair_own])
        add_into(mine.at[0], pair_recv.at[3])
        mine_cross = push(mine, (0, cross), own_cross, None, 1)
        saves.append(save(mine.at[0, near], own_keep, 4))
        saves[-1].start()
        for k, cols in enumerate(chunks):
            arrive([hop[k]])
            add_into(mine.at[2 - core], hop_recv, cols, 64)
            for n, (rows, dst) in enumerate(((near, second_keep), (cross, second_cross))):
                saves.append(save(mine.at[2 - core, rows, cols], dst.at[:, cols], 5 + 2 * k + n))
                saves[-1].start()
        arrive([part, mine_cross])
        leave([spec for spec in sent if spec not in pair_far and spec is not pair_x])
        for copy in saves:
            copy.wait()

    pl.run_scoped(blocks, pltpu.VMEM((4, PAIR, width), F32), pltpu.VMEM((2, PAIR, width), F32))


def row_kernel(asked_ref, c_ref, w_ref, x_ref, dy_ref, du_ref, dv_ref, wide_u, wide_v, part_u, part_v):
    n_rows, cols = du_ref.shape
    tiles = cols // LANES
    wide_step, part_step = n_rows + PAD, SLOTS + PAD
    part_size = tiles * part_step

    def clear(t, _):
        r = pl.multiple_of(t * 32, 32)
        for j in range(tiles):
            for wide in (wide_u, wide_v):
                wide[pl.ds(j * wide_step + r, 32), :] = jnp.zeros((32, LANES), F32)
        return 0

    lax.fori_loop(0, n_rows // 32, clear, 0)

    def product(q, slot):
        for coef, tok, part in ((c_ref, x_ref, part_u), (w_ref, dy_ref, part_v)):
            rows = tok[pl.ds(pl.multiple_of(q * TOK, TOK), TOK), :]
            full = jnp.dot(coef[q], jnp.concatenate([rows] * TERMS, axis=0), preferred_element_type=F32)
            for j in range(tiles):
                part[pl.ds(slot * part_size + j * part_step, SLOTS), :] = full[:, j * LANES:(j + 1) * LANES]

    product(0, 0)

    def device(q, _):
        product(lax.rem(q + 1, N_DEV), lax.rem(q + 1, 2))
        base = lax.rem(q, 2) * part_size
        for t in range(0, SLOTS, GROUP):
            rows = [asked_ref[q, t + u] for u in range(GROUP)]
            sums = [[wide[pl.ds(row, tiles, stride=wide_step), :] + part[pl.ds(base + t + u, tiles, stride=part_step), :]
                     for wide, part in ((wide_u, part_u), (wide_v, part_v))] for u, row in enumerate(rows)]
            for row, pair in zip(rows, sums):
                for wide, value in zip((wide_u, wide_v), pair):
                    wide[pl.ds(row, tiles, stride=wide_step), :] = value
        return 0

    lax.fori_loop(0, N_DEV, device, 0)

    def drain(t, _):
        r = pl.multiple_of(t * 32, 32)
        for j in range(tiles):
            for wide, out in ((wide_u, du_ref), (wide_v, dv_ref)):
                out[pl.ds(r, 32), j * LANES:(j + 1) * LANES] = wide[pl.ds(j * wide_step + r, 32), :].astype(BF16)
        return 0

    lax.fori_loop(0, n_rows // 32, drain, 0)


def join_kernel(fp_ref, fk_ref, fc_ref, sk_ref, sc_ref, ok_ref, oc_ref, y_ref, dx_ref):
    core = lax.rem(lax.axis_index("ep"), 2)
    half = y_ref.shape[1] // 2
    late = pl.program_id(0) * y_ref.shape[0] >= PART
    keep = (ok_ref[...] + jnp.where(late, fk_ref[...], fp_ref[...]) + sk_ref[...]).astype(BF16)
    cross = (oc_ref[...] + fc_ref[...] + sc_ref[...]).astype(BF16)
    here = pl.ds(pl.multiple_of(core * half, half), half)
    there = pl.ds(pl.multiple_of((1 - core) * half, half), half)
    for ref, cols in ((y_ref, slice(0, half)), (dx_ref, slice(half, 2 * half))):
        ref[:, here] = keep[:, cols]
        ref[:, there] = cross[:, cols]


def solution(mesh):
    tok_spec = P(('dp', 'ep'))
    table_spec = P('ep')

    def per_device(tokens, slot_ids, request_rows, gate_vals, grad_out, up_local, down_local):
        width = tokens.shape[1]
        rows_owner = up_local.shape[0]
        heads, top_k = slot_ids.shape[1:]
        n_tok = N_DEV * TOK
        half = width // 2
        core = lax.axis_index('ep') % 2
        anyw = pl.BlockSpec(memory_space=pl.ANY)
        shape = jax.ShapeDtypeStruct
        sums = shape((TOK, width), F32)
        x_all, dy_all, c_terms, w_terms, asked, first_part, first_keep, first_cross, second_keep, second_cross, own_keep, own_cross = pl.pallas_call(
            layer_kernel,
            in_specs=[anyw] * 7,
            out_specs=[anyw] * 12,
            out_shape=[shape((N_DEV, TOK, width), BF16)] * 2 + [shape((N_DEV, SLOTS, TERMS * TOK), BF16)] * 2 + [shape((N_DEV, SLOTS), I32)] + [shape((PART, width), F32), shape((TOK - PART, width), F32)] + [sums] * 5,
            scratch_shapes=[
                pltpu.VMEM((N_DEV, TOK, width), BF16), pltpu.VMEM((N_DEV, TOK, width), BF16),
                pltpu.VMEM((N_DEV, TOK, SEL), I32), pltpu.VMEM((N_DEV, TOK, SEL), F32),
                pltpu.VMEM((N_DEV * SLOTS, width), BF16), pltpu.VMEM((N_DEV * SLOTS, width), BF16),
                pltpu.VMEM((4, PAIR, width), F32), pltpu.VMEM((PAIR, width), F32),
                pltpu.VMEM((heads, top_k, TOK), I32), pltpu.VMEM((heads, top_k, TOK), F32), pltpu.VMEM((1, N_DEV, SLOTS), I32),
                pltpu.VMEM((N_DEV, SLOTS, TERMS * TOK), BF16), pltpu.VMEM((N_DEV, SLOTS, TERMS * TOK), BF16),
                pltpu.VMEM((N_DEV, SLOTS), I32), pltpu.SMEM((N_DEV, SLOTS), I32),
                pltpu.VMEM((SEL, PAIR), I32), pltpu.VMEM((SEL, PAIR), F32), pltpu.VMEM((SEL, PAIR), F32),
                pltpu.SemaphoreType.DMA((N_COPIES,)), pltpu.SemaphoreType.DMA((N_COPIES,)),
                pltpu.SemaphoreType.DMA((6,)), pltpu.SemaphoreType.DMA,
                pltpu.SemaphoreType.DMA((1,)), pltpu.SemaphoreType.DMA((TERM_SEM + N_DEV,)),
            ],
            compiler_params=pltpu.CompilerParams(collective_id=0, has_side_effects=True, vmem_limit_bytes=VMEM_BYTES),
        )(tokens, grad_out, slot_ids.transpose(1, 2, 0), gate_vals.transpose(1, 2, 0), request_rows, up_local, down_local)

        first_hop = [(i, i ^ (2 if i % 2 == 0 else 4)) for i in range(N_DEV)]
        second_hop = [(i, i ^ (4 if i % 2 == 0 else 2)) for i in range(N_DEV)]
        over = lambda pairs: [(i, j ^ 1) for i, j in pairs]
        hop = lambda value, pairs: lax.ppermute(value, 'ep', pairs)

        def grad_rows():
            coef = pl.BlockSpec((N_DEV, SLOTS, TERMS * TOK), lambda i, a: (0, 0, 0))
            tok = pl.BlockSpec((n_tok, ROW_CHUNK), lambda i, a: (0, i))
            out = pl.BlockSpec((rows_owner, ROW_CHUNK), lambda i, a: (0, i))
            tiles = ROW_CHUNK // LANES
            return pl.pallas_call(
                row_kernel,
                grid_spec=pltpu.PrefetchScalarGridSpec(
                    num_scalar_prefetch=1,
                    grid=(width // ROW_CHUNK,),
                    in_specs=[coef, coef, tok, tok],
                    out_specs=[out, out],
                    scratch_shapes=[pltpu.VMEM((tiles * (rows_owner + PAD), LANES), F32)] * 2 + [pltpu.VMEM((2 * tiles * (SLOTS + PAD), LANES), F32)] * 2,
                ),
                out_shape=[shape((rows_owner, width), BF16)] * 2,
                compiler_params=pltpu.CompilerParams(vmem_limit_bytes=VMEM_BYTES),
                cost_estimate=pl.CostEstimate(flops=12 * rows_owner * width * n_tok, bytes_accessed=4 * rows_owner * width, transcendentals=0),
            )(asked, c_terms, w_terms, x_all.reshape(n_tok, width), dy_all.reshape(n_tok, width))

        got = (hop(first_keep, first_hop), hop(first_cross, over(first_hop)), hop(second_keep, second_hop), hop(second_cross, over(second_hop)))
        grad_up, grad_down = grad_rows()
        got, grad_up, grad_down = lax.optimization_barrier((got, grad_up, grad_down))
        block = 32
        rows = pl.BlockSpec((block, width), lambda i: (i, 0))
        early = pl.BlockSpec((block, width), lambda i: (0, 0))
        out_tokens, grad_tokens = pl.pallas_call(
            join_kernel,
            grid=(TOK // block,),
            in_specs=[early] * 2 + [rows] * 5,
            out_specs=[rows, rows],
            out_shape=[shape((TOK, width), BF16)] * 2,
            compiler_params=pltpu.CompilerParams(vmem_limit_bytes=VMEM_BYTES),
        )(first_part, *got, own_keep, own_cross)
        return out_tokens, grad_tokens, grad_up, grad_down

    return jax.shard_map(per_device, mesh=mesh, in_specs=(tok_spec, tok_spec, tok_spec, tok_spec, tok_spec, table_spec, table_spec), out_specs=(tok_spec, tok_spec, tok_spec, tok_spec), check_vma=False)
```

```python
import functools
import math
import jax
import jax.numpy as jnp
from jax import lax
from jax.experimental import pallas as pl
from jax.experimental.pallas import tpu as pltpu
from jax.sharding import PartitionSpec as P

F32, BF16, I32 = jnp.float32, jnp.bfloat16, jnp.int32
N_DEV, TOK, SLOTS, SEL = 8, 64, 128, 128
PAIR = 2 * TOK
TERMS = 3
CHUNK = 2048
ROW_CHUNK = 1024
GROUP = 16
LANES = 128
PAD = 4
VMEM_BYTES = 62 * 1024 * 1024
MESH = pl.DeviceIdType.MESH


def gelu_pair(pre_act):
    normal_cdf = 0.5 * (1.0 + lax.erf(pre_act * (2.0 ** -0.5)))
    normal_pdf = jnp.exp(-0.5 * pre_act * pre_act) * ((2.0 * math.pi) ** -0.5)
    return pre_act * normal_cdf, normal_cdf + pre_act * normal_pdf


def split3(wide):
    high = wide.astype(BF16)
    rest = wide - high.astype(F32)
    mid = rest.astype(BF16)
    low = (rest - mid.astype(F32)).astype(BF16)
    return high, mid, low


N_COPIES = 64
SIDE_STEP, FAR_STEP, REST_STEP = 1, 3, 5
COLS = 512
PART = 32
TERM_SEM = 5 + 16


def layer_kernel(x_ref, dy_ref, slot_in, gate_in, req_in, up_ref, down_ref,
                 x_out, dy_out, c_out, w_out, asked_out, first_part, first_keep, first_cross, second_keep, second_cross, own_keep, own_cross,
                 x_all, dy_all, slot_all, gate_all, up_rows, down_rows, pair_recv, hop_recv, slot_ref, gate_ref, req_ref, c_buf, w_buf, asked, asked_s, slot_t, w_t, c_t,
                 send_sem, recv_sem, own_sem, smem_sem, in_sem, out_sem):
    me = lax.axis_index("ep")
    core = lax.rem(me, 2)
    n_rows, width = up_ref.shape
    half = width // 2
    steps = [(ref, out, col) for ref, out in ((up_ref, up_rows), (down_ref, down_rows)) for col in range(0, width, CHUNK)]
    tiles = CHUNK // LANES
    wide_step, pick_step = n_rows + PAD, SLOTS + PAD
    sent = []

    def descriptor(k, src, dst, mask):
        view = lambda ref, index: ref if index is None else ref.at[index]
        return pltpu.make_async_remote_copy(src_ref=view(*src), dst_ref=view(*dst), send_sem=send_sem.at[k], recv_sem=recv_sem.at[k],
                                            device_id={"ep": me ^ mask}, device_id_type=MESH)

    def push(src, src_index, dst, dst_index, mask):
        spec = (len(sent), (src, src_index), (dst, dst_index), mask)
        descriptor(*spec).start()
        sent.append(spec)
        return spec

    def arrive(specs):
        for spec in specs:
            descriptor(*spec).wait_recv()

    def leave(specs):
        for spec in specs:
            descriptor(*spec).wait_send()

    own = [pltpu.make_async_copy(src, dst.at[0], own_sem.at[k]) for k, (src, dst) in enumerate(((x_ref, x_all), (dy_ref, dy_all)))]
    small = [pltpu.make_async_copy(src, dst, own_sem.at[2 + k]) for k, (src, dst) in enumerate(((slot_in, slot_ref), (gate_in, gate_ref), (req_in, req_ref)))]
    barrier = pltpu.get_barrier_semaphore()
    for b in range(1, N_DEV):
        pl.semaphore_signal(barrier, inc=1, device_id={"ep": me ^ b}, device_id_type=MESH)
    for copy in small + own:
        copy.start()
    for copy in small:
        copy.wait()
    slot_all[0] = slot_ref[...].reshape(SEL, TOK).T
    gate_all[0] = gate_ref[...].reshape(SEL, TOK).T
    pl.semaphore_wait(barrier, N_DEV - 1)

    asks = [push(req_ref, (0, pl.ds(me ^ b, 1)), asked, pl.ds(b, 1), b) for b in range(1, N_DEV)]
    first = [push(x_ref, None, x_all, 4, 4), push(dy_ref, None, dy_all, 2, 2)]
    near_own = [push(x_ref, None, x_all, 1, 1), push(dy_ref, None, dy_all, 1, 1)]
    second = []
    asked[pl.ds(0, 1), :] = req_ref[0, pl.ds(me, 1), :]
    arrive(asks)
    to_smem = pltpu.make_async_copy(asked, asked_s, smem_sem)
    to_smem.start()
    to_smem.wait()
    keep_asked = pltpu.make_async_copy(asked, asked_out, own_sem.at[5])
    keep_asked.start()

    def gather_all(table, wide, picked):
        def fetch(k):
            ref, _, col = steps[k]
            return pltpu.make_async_copy(ref.at[:, pl.ds(col, CHUNK)], table, in_sem.at[0])

        fetch(0).start()
        for sub in range(2 * len(steps)):
            if sub == SIDE_STEP:
                side = [push(gate_all, 0, gate_all, 4, 4), push(slot_all, 0, slot_all, 2, 2)]
                near_own.extend([push(gate_all, 0, gate_all, 1, 1), push(slot_all, 0, slot_all, 1, 1)])
            if sub == FAR_STEP:
                arrive(first)
                far = [push(x_all, 4, x_all, 6, 2), push(dy_all, 2, dy_all, 6, 4)]
                near_first = [push(x_all, 4, x_all, 5, 1), push(dy_all, 2, dy_all, 3, 1)]
            if sub == REST_STEP:
                arrive(side)
                far.extend([push(gate_all, 4, gate_all, 6, 2), push(slot_all, 2, slot_all, 6, 4)])
                near_first.extend([push(gate_all, 4, gate_all, 5, 1), push(slot_all, 2, slot_all, 3, 1)])
                second.extend([push(gate_all, 0, gate_all, 2, 2), push(slot_all, 0, slot_all, 4, 4)])
                second.extend([push(x_ref, None, x_all, 2, 2), push(dy_ref, None, dy_all, 4, 4)])
            k = sub // 2
            if sub % 2 == 0:
                fetch(k).wait()

                def fill(t, _):
                    r = pl.multiple_of(t * 32, 32)
                    for j in range(tiles):
                        wide[pl.ds(j * wide_step + r, 32), :] = table[pl.ds(r, 32), j * LANES:(j + 1) * LANES].astype(F32)
                    return 0

                lax.fori_loop(0, n_rows // 32, fill, 0)
                if k + 1 < len(steps):
                    fetch(k + 1).start()
            else:
                _, rows_ref, col = steps[k]

                def pick_device(b, _):
                    def pick(t, _):
                        for u in range(16):
                            row = asked_s[b, t * 16 + u]
                            picked[pl.ds(t * 16 + u, tiles, stride=pick_step), :] = wide[pl.ds(row, tiles, stride=wide_step), :]
                        return 0

                    lax.fori_loop(0, SLOTS // 16, pick, 0)

                    def drain(t, _):
                        r = pl.multiple_of(t * 32, 32)
                        into = pl.multiple_of(b * SLOTS + t * 32, 32)
                        for j in range(tiles):
                            rows_ref[pl.ds(into, 32), col + j * LANES:col + (j + 1) * LANES] = picked[pl.ds(j * pick_step + r, 32), :].astype(BF16)
                        return 0

                    return lax.fori_loop(0, SLOTS // 32, drain, 0)

                lax.fori_loop(0, N_DEV, pick_device, 0)
        return far, near_first

    kept = []
    pl.run_scoped(
        lambda *bufs: kept.append(gather_all(*bufs)),
        pltpu.VMEM((n_rows, CHUNK), BF16), pltpu.VMEM((tiles * wide_step, LANES), F32), pltpu.VMEM((tiles * pick_step, LANES), F32),
    )
    far, near_first = kept[0]
    for copy in own:
        copy.wait()
    keep_asked.wait()
    dims = (((1,), (1,)), ((), ()))
    row_iota = lax.broadcasted_iota(I32, (SLOTS, PAIR), 0)
    block_diag = (lax.broadcasted_iota(I32, (PAIR, 2 * SLOTS), 0) < TOK) == (lax.broadcasted_iota(I32, (PAIR, 2 * SLOTS), 1) < SLOTS)

    def front(r):
        toks, rows = pl.ds(2 * r, 2), pl.ds(2 * r * SLOTS, 2 * SLOTS)

        def dots(tok, table):
            full = lax.dot_general(table[rows, :], tok[toks].reshape(PAIR, width), dims, preferred_element_type=F32).T
            return jnp.concatenate([full[:TOK, :SLOTS], full[TOK:, SLOTS:]], axis=0)

        act, slope = gelu_pair(dots(x_all, up_rows))
        slope = slope * dots(dy_all, down_rows)
        local = slot_all[toks].reshape(PAIR, SEL) - me * SLOTS
        valid = (local >= 0) & (local < SLOTS)
        index = jnp.where(valid, local, 0)
        act = jnp.take_along_axis(act, index, axis=1)
        slope = jnp.take_along_axis(slope, index, axis=1)
        gate = gate_all[toks].reshape(PAIR, SEL)
        w_t[...] = jnp.where(valid, (gate * act).astype(BF16).astype(F32), 0.0).T
        c_t[...] = jnp.where(valid, (gate * slope).astype(BF16).astype(F32), 0.0).T
        slot_t[...] = jnp.where(valid, local, -1).T

        def step(s, acc):
            acc_w, acc_c = acc
            hit = row_iota == slot_t[pl.ds(s, 1), :]
            acc_w += jnp.where(hit, w_t[pl.ds(s, 1), :], 0.0)
            acc_c += jnp.where(hit, c_t[pl.ds(s, 1), :], 0.0)
            return acc_w, acc_c

        zero = jnp.zeros((SLOTS, PAIR), F32)
        acc_w, acc_c = lax.fori_loop(0, SEL, step, (zero, zero), unroll=8)
        for ref, acc in ((w_buf, acc_w), (c_buf, acc_c)):
            terms = split3(acc)
            for j in range(2):
                ref[2 * r + j] = jnp.concatenate([term[:, j * TOK:(j + 1) * TOK] for term in terms], axis=1)

        def spread(acc):
            both = jnp.concatenate([acc.T, acc.T], axis=1)
            return split3(jnp.where(block_diag, both, 0.0))

        return spread(acc_w), spread(acc_c)

    def columns(r, terms, col, mine, other):
        rows = pl.ds(2 * r * SLOTS, 2 * SLOTS)
        table, terms = (down_rows, terms[0]) if col < half else (up_rows, terms[1])
        here = pl.ds(pl.multiple_of(core * half + col % half, COLS), COLS)
        there = pl.ds(pl.multiple_of((1 - core) * half + col % half, COLS), COLS)
        mine[:, col:col + COLS] = sum(jnp.dot(term, table[rows, here], preferred_element_type=F32) for term in terms)
        part = sum(jnp.dot(term, table[rows, there], preferred_element_type=F32) for term in terms)
        other[:TOK, col:col + COLS] = part[TOK:]
        other[TOK:, col:col + COLS] = part[:TOK]

    def block(r, mine, other):
        terms = front(r)
        for col in range(0, width, COLS):
            columns(r, terms, col, mine, other)

    def add_into(dst, src, cols=slice(None), step=16):
        def add(t, _):
            r = pl.ds(pl.multiple_of(t * step, step), step)
            dst[r, cols] = dst[r, cols] + src[r, cols]
            return 0

        lax.fori_loop(0, PAIR // step, add, 0)

    def blocks(mine, other):
        save = lambda src, dst, k: pltpu.make_async_copy(src, dst, out_sem.at[k])
        saves = []

        def keep_terms(r):
            for n, (src, dst) in enumerate(((c_buf, c_out), (w_buf, w_out))):
                saves.append(save(src.at[pl.ds(2 * r, 2)], dst.at[pl.ds(2 * r, 2)], TERM_SEM + 2 * r + n))
                saves[-1].start()

        arrive(near_own)
        arrive(far)
        near_far = [push(ref, 6, ref, 7, 1) for ref in (gate_all, slot_all, x_all, dy_all)]
        arrive(near_first + near_far)
        terms = front(3)
        pair_far, hop = [], []
        chunks = [pl.ds(col, COLS) for col in range(0, width, COLS)]
        every = slice(None)
        for cols in chunks:
            columns(3, terms, cols.start, mine.at[3], other.at[0])
            pair_far.append(push(other, (0, every, cols), pair_recv, (0, every, cols), 1))
        for k, cols in enumerate(chunks):
            arrive([pair_far[k]])
            add_into(mine.at[3], pair_recv.at[0], cols, 64)
            hop.append(push(mine, (3, every, cols), hop_recv, (every, cols), 2 + 2 * core))
        keep_terms(3)
        arrive(second)
        near_second = [push(gate_all, 2, gate_all, 3, 1), push(slot_all, 4, slot_all, 5, 1), push(x_all, 2, x_all, 3, 1), push(dy_all, 4, dy_all, 5, 1)]
        arrive(near_second)
        for k, (src, dst) in enumerate(((x_all, x_out), (dy_all, dy_out))):
            saves.append(save(src, dst, 1 + k))
            saves[-1].start()
        leave(pair_far)
        block(1, mine.at[1], other.at[0])
        pair_x = push(other, 0, pair_recv, 1, 1)
        keep_terms(1)
        block(2, mine.at[2], other.at[1])
        pair_y = push(other, 1, pair_recv, 2, 1)
        keep_terms(2)
        arrive([pair_x])
        add_into(mine.at[1], pair_recv.at[1])
        arrive([pair_y])
        add_into(mine.at[2], pair_recv.at[2])
        near, cross = pl.ds(0, TOK), pl.ds(TOK, TOK)
        part = push(mine, (1 + core, pl.ds(0, PART)), first_part, None, 2 + 2 * core)
        saves.append(save(mine.at[1 + core, pl.ds(PART, TOK - PART)], first_keep, 0))
        saves.append(save(mine.at[1 + core, cross], first_cross, 3))
        for copy in saves[-2:]:
            copy.start()
        leave([pair_x])
        block(0, mine.at[0], other.at[0])
        pair_own = push(other, 0, pair_recv, 3, 1)
        keep_terms(0)
        arrive([pair_own])
        add_into(mine.at[0], pair_recv.at[3])
        mine_cross = push(mine, (0, cross), own_cross, None, 1)
        saves.append(save(mine.at[0, near], own_keep, 4))
        saves[-1].start()
        for k, cols in enumerate(chunks):
            arrive([hop[k]])
            add_into(mine.at[2 - core], hop_recv, cols, 64)
            for n, (rows, dst) in enumerate(((near, second_keep), (cross, second_cross))):
                saves.append(save(mine.at[2 - core, rows, cols], dst.at[:, cols], 5 + 2 * k + n))
                saves[-1].start()
        arrive([part, mine_cross])
        leave([spec for spec in sent if spec not in pair_far and spec is not pair_x])
        for copy in saves:
            copy.wait()

    pl.run_scoped(blocks, pltpu.VMEM((4, PAIR, width), F32), pltpu.VMEM((2, PAIR, width), F32))


def row_kernel(asked_ref, c_ref, w_ref, x_ref, dy_ref, du_ref, dv_ref, wide_u, wide_v, part_u, part_v):
    n_rows, cols = du_ref.shape
    tiles = cols // LANES
    wide_step, part_step = n_rows + PAD, SLOTS + PAD
    part_size = tiles * part_step

    def clear(t, _):
        r = pl.multiple_of(t * 32, 32)
        for j in range(tiles):
            for wide in (wide_u, wide_v):
                wide[pl.ds(j * wide_step + r, 32), :] = jnp.zeros((32, LANES), F32)
        return 0

    lax.fori_loop(0, n_rows // 32, clear, 0)

    def product(q, slot):
        for coef, tok, part in ((c_ref, x_ref, part_u), (w_ref, dy_ref, part_v)):
            rows = tok[pl.ds(pl.multiple_of(q * TOK, TOK), TOK), :]
            full = jnp.dot(coef[q], jnp.concatenate([rows] * TERMS, axis=0), preferred_element_type=F32)
            for j in range(tiles):
                part[pl.ds(slot * part_size + j * part_step, SLOTS), :] = full[:, j * LANES:(j + 1) * LANES]

    product(0, 0)

    def device(q, _):
        product(lax.rem(q + 1, N_DEV), lax.rem(q + 1, 2))
        base = lax.rem(q, 2) * part_size
        for t in range(0, SLOTS, GROUP):
            rows = [asked_ref[q, t + u] for u in range(GROUP)]
            sums = [[wide[pl.ds(row, tiles, stride=wide_step), :] + part[pl.ds(base + t + u, tiles, stride=part_step), :]
                     for wide, part in ((wide_u, part_u), (wide_v, part_v))] for u, row in enumerate(rows)]
            for row, pair in zip(rows, sums):
                for wide, value in zip((wide_u, wide_v), pair):
                    wide[pl.ds(row, tiles, stride=wide_step), :] = value
        return 0

    lax.fori_loop(0, N_DEV, device, 0)

    def drain(t, _):
        r = pl.multiple_of(t * 32, 32)
        for j in range(tiles):
            for wide, out in ((wide_u, du_ref), (wide_v, dv_ref)):
                out[pl.ds(r, 32), j * LANES:(j + 1) * LANES] = wide[pl.ds(j * wide_step + r, 32), :].astype(BF16)
        return 0

    lax.fori_loop(0, n_rows // 32, drain, 0)


def join_kernel(fp_ref, fk_ref, fc_ref, sk_ref, sc_ref, ok_ref, oc_ref, y_ref, dx_ref):
    core = lax.rem(lax.axis_index("ep"), 2)
    half = y_ref.shape[1] // 2
    late = pl.program_id(0) * y_ref.shape[0] >= PART
    keep = (ok_ref[...] + jnp.where(late, fk_ref[...], fp_ref[...]) + sk_ref[...]).astype(BF16)
    cross = (oc_ref[...] + fc_ref[...] + sc_ref[...]).astype(BF16)
    here = pl.ds(pl.multiple_of(core * half, half), half)
    there = pl.ds(pl.multiple_of((1 - core) * half, half), half)
    for ref, cols in ((y_ref, slice(0, half)), (dx_ref, slice(half, 2 * half))):
        ref[:, here] = keep[:, cols]
        ref[:, there] = cross[:, cols]


def solution(mesh):
    tok_spec = P(('dp', 'ep'))
    table_spec = P('ep')

    def per_device(tokens, slot_ids, request_rows, gate_vals, grad_out, up_local, down_local):
        width = tokens.shape[1]
        rows_owner = up_local.shape[0]
        heads, top_k = slot_ids.shape[1:]
        n_tok = N_DEV * TOK
        half = width // 2
        core = lax.axis_index('ep') % 2
        anyw = pl.BlockSpec(memory_space=pl.ANY)
        shape = jax.ShapeDtypeStruct
        sums = shape((TOK, width), F32)
        x_all, dy_all, c_terms, w_terms, asked, first_part, first_keep, first_cross, second_keep, second_cross, own_keep, own_cross = pl.pallas_call(
            layer_kernel,
            in_specs=[anyw] * 7,
            out_specs=[anyw] * 12,
            out_shape=[shape((N_DEV, TOK, width), BF16)] * 2 + [shape((N_DEV, SLOTS, TERMS * TOK), BF16)] * 2 + [shape((N_DEV, SLOTS), I32)] + [shape((PART, width), F32), shape((TOK - PART, width), F32)] + [sums] * 5,
            scratch_shapes=[
                pltpu.VMEM((N_DEV, TOK, width), BF16), pltpu.VMEM((N_DEV, TOK, width), BF16),
                pltpu.VMEM((N_DEV, TOK, SEL), I32), pltpu.VMEM((N_DEV, TOK, SEL), F32),
                pltpu.VMEM((N_DEV * SLOTS, width), BF16), pltpu.VMEM((N_DEV * SLOTS, width), BF16),
                pltpu.VMEM((4, PAIR, width), F32), pltpu.VMEM((PAIR, width), F32),
                pltpu.VMEM((heads, top_k, TOK), I32), pltpu.VMEM((heads, top_k, TOK), F32), pltpu.VMEM((1, N_DEV, SLOTS), I32),
                pltpu.VMEM((N_DEV, SLOTS, TERMS * TOK), BF16), pltpu.VMEM((N_DEV, SLOTS, TERMS * TOK), BF16),
                pltpu.VMEM((N_DEV, SLOTS), I32), pltpu.SMEM((N_DEV, SLOTS), I32),
                pltpu.VMEM((SEL, PAIR), I32), pltpu.VMEM((SEL, PAIR), F32), pltpu.VMEM((SEL, PAIR), F32),
                pltpu.SemaphoreType.DMA((N_COPIES,)), pltpu.SemaphoreType.DMA((N_COPIES,)),
                pltpu.SemaphoreType.DMA((6,)), pltpu.SemaphoreType.DMA,
                pltpu.SemaphoreType.DMA((1,)), pltpu.SemaphoreType.DMA((TERM_SEM + N_DEV,)),
            ],
            compiler_params=pltpu.CompilerParams(collective_id=0, has_side_effects=True, vmem_limit_bytes=VMEM_BYTES),
        )(tokens, grad_out, slot_ids.transpose(1, 2, 0), gate_vals.transpose(1, 2, 0), request_rows, up_local, down_local)

        first_hop = [(i, i ^ (2 if i % 2 == 0 else 4)) for i in range(N_DEV)]
        second_hop = [(i, i ^ (4 if i % 2 == 0 else 2)) for i in range(N_DEV)]
        over = lambda pairs: [(i, j ^ 1) for i, j in pairs]
        hop = lambda value, pairs: lax.ppermute(value, 'ep', pairs)

        def grad_rows():
            coef = pl.BlockSpec((N_DEV, SLOTS, TERMS * TOK), lambda i, a: (0, 0, 0))
            tok = pl.BlockSpec((n_tok, ROW_CHUNK), lambda i, a: (0, i))
            out = pl.BlockSpec((rows_owner, ROW_CHUNK), lambda i, a: (0, i))
            tiles = ROW_CHUNK // LANES
            return pl.pallas_call(
                row_kernel,
                grid_spec=pltpu.PrefetchScalarGridSpec(
                    num_scalar_prefetch=1,
                    grid=(width // ROW_CHUNK,),
                    in_specs=[coef, coef, tok, tok],
                    out_specs=[out, out],
                    scratch_shapes=[pltpu.VMEM((tiles * (rows_owner + PAD), LANES), F32)] * 2 + [pltpu.VMEM((2 * tiles * (SLOTS + PAD), LANES), F32)] * 2,
                ),
                out_shape=[shape((rows_owner, width), BF16)] * 2,
                compiler_params=pltpu.CompilerParams(vmem_limit_bytes=VMEM_BYTES),
                cost_estimate=pl.CostEstimate(flops=12 * rows_owner * width * n_tok, bytes_accessed=4 * rows_owner * width, transcendentals=0),
            )(asked, c_terms, w_terms, x_all.reshape(n_tok, width), dy_all.reshape(n_tok, width))

        got = (hop(first_keep, first_hop), hop(first_cross, over(first_hop)), hop(second_keep, second_hop), hop(second_cross, over(second_hop)))
        grad_up, grad_down = grad_rows()
        got, grad_up, grad_down = lax.optimization_barrier((got, grad_up, grad_down))
        block = 32
        rows = pl.BlockSpec((block, width), lambda i: (i, 0))
        early = pl.BlockSpec((block, width), lambda i: (0, 0))
        out_tokens, grad_tokens = pl.pallas_call(
            join_kernel,
            grid=(TOK // block,),
            in_specs=[early] * 2 + [rows] * 5,
            out_specs=[rows, rows],
            out_shape=[shape((TOK, width), BF16)] * 2,
            compiler_params=pltpu.CompilerParams(vmem_limit_bytes=VMEM_BYTES),
        )(first_part, *got, own_keep, own_cross)
        return out_tokens, grad_tokens, grad_up, grad_down

    return jax.shard_map(per_device, mesh=mesh, in_specs=(tok_spec, tok_spec, tok_spec, tok_spec, tok_spec, table_spec, table_spec), out_specs=(tok_spec, tok_spec, tok_spec, tok_spec), check_vma=False)
```

```python
import functools
import math
import jax
import jax.numpy as jnp
from jax import lax
from jax.experimental import pallas as pl
from jax.experimental.pallas import tpu as pltpu
from jax.sharding import PartitionSpec as P

F32, BF16, I32 = jnp.float32, jnp.bfloat16, jnp.int32
N_DEV, TOK, SLOTS, SEL = 8, 64, 128, 128
PAIR = 2 * TOK
TERMS = 3
CHUNK = 2048
ROW_CHUNK = 1024
GROUP = 16
LANES = 128
PAD = 4
VMEM_BYTES = 62 * 1024 * 1024
MESH = pl.DeviceIdType.MESH


def gelu_pair(pre_act):
    normal_cdf = 0.5 * (1.0 + lax.erf(pre_act * (2.0 ** -0.5)))
    normal_pdf = jnp.exp(-0.5 * pre_act * pre_act) * ((2.0 * math.pi) ** -0.5)
    return pre_act * normal_cdf, normal_cdf + pre_act * normal_pdf


def split3(wide):
    high = wide.astype(BF16)
    rest = wide - high.astype(F32)
    mid = rest.astype(BF16)
    low = (rest - mid.astype(F32)).astype(BF16)
    return high, mid, low


N_COPIES = 64
SIDE_STEP, FAR_STEP, REST_STEP = 1, 3, 5
COLS = 512
PART = 32
TERM_SEM = 5 + 16


def layer_kernel(x_ref, dy_ref, slot_in, gate_in, req_in, up_ref, down_ref,
                 x_out, dy_out, c_out, w_out, asked_out, first_part, first_keep, first_cross, second_keep, second_cross, own_keep, own_cross,
                 x_all, dy_all, slot_all, gate_all, up_rows, down_rows, pair_recv, hop_recv, slot_ref, gate_ref, req_ref, c_buf, w_buf, asked, asked_s, slot_t, w_t, c_t,
                 send_sem, recv_sem, own_sem, smem_sem, in_sem, out_sem):
    me = lax.axis_index("ep")
    core = lax.rem(me, 2)
    n_rows, width = up_ref.shape
    half = width // 2
    steps = [(ref, out, col) for ref, out in ((up_ref, up_rows), (down_ref, down_rows)) for col in range(0, width, CHUNK)]
    tiles = CHUNK // LANES
    wide_step, pick_step = n_rows + PAD, SLOTS + PAD
    sent = []

    def descriptor(k, src, dst, mask):
        view = lambda ref, index: ref if index is None else ref.at[index]
        return pltpu.make_async_remote_copy(src_ref=view(*src), dst_ref=view(*dst), send_sem=send_sem.at[k], recv_sem=recv_sem.at[k],
                                            device_id={"ep": me ^ mask}, device_id_type=MESH)

    def push(src, src_index, dst, dst_index, mask):
        spec = (len(sent), (src, src_index), (dst, dst_index), mask)
        descriptor(*spec).start()
        sent.append(spec)
        return spec

    def arrive(specs):
        for spec in specs:
            descriptor(*spec).wait_recv()

    def leave(specs):
        for spec in specs:
            descriptor(*spec).wait_send()

    own = [pltpu.make_async_copy(src, dst.at[0], own_sem.at[k]) for k, (src, dst) in enumerate(((x_ref, x_all), (dy_ref, dy_all)))]
    small = [pltpu.make_async_copy(src, dst, own_sem.at[2 + k]) for k, (src, dst) in enumerate(((slot_in, slot_ref), (gate_in, gate_ref), (req_in, req_ref)))]
    barrier = pltpu.get_barrier_semaphore()
    for b in range(1, N_DEV):
        pl.semaphore_signal(barrier, inc=1, device_id={"ep": me ^ b}, device_id_type=MESH)
    for copy in small + own:
        copy.start()
    for copy in small:
        copy.wait()
    slot_all[0] = slot_ref[...].reshape(SEL, TOK).T.astype(jnp.int16)
    gate_all[0] = gate_ref[...].reshape(SEL, TOK).T
    pl.semaphore_wait(barrier, N_DEV - 1)

    asks = [push(req_ref, (0, pl.ds(me ^ b, 1)), asked, pl.ds(b, 1), b) for b in range(1, N_DEV)]
    first = [push(x_ref, None, x_all, 4, 4), push(dy_ref, None, dy_all, 2, 2)]
    near_own = [push(x_ref, None, x_all, 1, 1), push(dy_ref, None, dy_all, 1, 1)]
    second = []
    asked[pl.ds(0, 1), :] = req_ref[0, pl.ds(me, 1), :]
    arrive(asks)
    to_smem = pltpu.make_async_copy(asked, asked_s, smem_sem)
    to_smem.start()
    to_smem.wait()
    keep_asked = pltpu.make_async_copy(asked, asked_out, own_sem.at[5])
    keep_asked.start()

    def gather_all(table, wide, picked):
        def fetch(k):
            ref, _, col = steps[k]
            return pltpu.make_async_copy(ref.at[:, pl.ds(col, CHUNK)], table, in_sem.at[0])

        fetch(0).start()
        for sub in range(2 * len(steps)):
            if sub == SIDE_STEP:
                side = [push(gate_all, 0, gate_all, 4, 4), push(slot_all, 0, slot_all, 2, 2)]
                near_own.extend([push(gate_all, 0, gate_all, 1, 1), push(slot_all, 0, slot_all, 1, 1)])
            if sub == FAR_STEP:
                arrive(first)
                far = [push(x_all, 4, x_all, 6, 2), push(dy_all, 2, dy_all, 6, 4)]
                near_first = [push(x_all, 4, x_all, 5, 1), push(dy_all, 2, dy_all, 3, 1)]
            if sub == REST_STEP:
                arrive(side)
                far.extend([push(gate_all, 4, gate_all, 6, 2), push(slot_all, 2, slot_all, 6, 4)])
                near_first.extend([push(gate_all, 4, gate_all, 5, 1), push(slot_all, 2, slot_all, 3, 1)])
                second.extend([push(gate_all, 0, gate_all, 2, 2), push(slot_all, 0, slot_all, 4, 4)])
                second.extend([push(x_ref, None, x_all, 2, 2), push(dy_ref, None, dy_all, 4, 4)])
            k = sub // 2
            if sub % 2 == 0:
                fetch(k).wait()

                def fill(t, _):
                    r = pl.multiple_of(t * 32, 32)
                    for j in range(tiles):
                        wide[pl.ds(j * wide_step + r, 32), :] = table[pl.ds(r, 32), j * LANES:(j + 1) * LANES].astype(F32)
                    return 0

                lax.fori_loop(0, n_rows // 32, fill, 0)
                if k + 1 < len(steps):
                    fetch(k + 1).start()
            else:
                _, rows_ref, col = steps[k]

                def pick_device(b, _):
                    def pick(t, _):
                        for u in range(16):
                            row = asked_s[b, t * 16 + u]
                            picked[pl.ds(t * 16 + u, tiles, stride=pick_step), :] = wide[pl.ds(row, tiles, stride=wide_step), :]
                        return 0

                    lax.fori_loop(0, SLOTS // 16, pick, 0)

                    def drain(t, _):
                        r = pl.multiple_of(t * 32, 32)
                        into = pl.multiple_of(b * SLOTS + t * 32, 32)
                        for j in range(tiles):
                            rows_ref[pl.ds(into, 32), col + j * LANES:col + (j + 1) * LANES] = picked[pl.ds(j * pick_step + r, 32), :].astype(BF16)
                        return 0

                    return lax.fori_loop(0, SLOTS // 32, drain, 0)

                lax.fori_loop(0, N_DEV, pick_device, 0)
        return far, near_first

    kept = []
    pl.run_scoped(
        lambda *bufs: kept.append(gather_all(*bufs)),
        pltpu.VMEM((n_rows, CHUNK), BF16), pltpu.VMEM((tiles * wide_step, LANES), F32), pltpu.VMEM((tiles * pick_step, LANES), F32),
    )
    far, near_first = kept[0]
    for copy in own:
        copy.wait()
    keep_asked.wait()
    dims = (((1,), (1,)), ((), ()))
    row_iota = lax.broadcasted_iota(I32, (SLOTS, PAIR), 0)
    block_diag = (lax.broadcasted_iota(I32, (PAIR, 2 * SLOTS), 0) < TOK) == (lax.broadcasted_iota(I32, (PAIR, 2 * SLOTS), 1) < SLOTS)

    def front(r):
        toks, rows = pl.ds(2 * r, 2), pl.ds(2 * r * SLOTS, 2 * SLOTS)

        def dots(tok, table):
            full = lax.dot_general(table[rows, :], tok[toks].reshape(PAIR, width), dims, preferred_element_type=F32).T
            return jnp.concatenate([full[:TOK, :SLOTS], full[TOK:, SLOTS:]], axis=0)

        act, slope = gelu_pair(dots(x_all, up_rows))
        slope = slope * dots(dy_all, down_rows)
        local = slot_all[toks].reshape(PAIR, SEL).astype(I32) - me * SLOTS
        valid = (local >= 0) & (local < SLOTS)
        index = jnp.where(valid, local, 0)
        act = jnp.take_along_axis(act, index, axis=1)
        slope = jnp.take_along_axis(slope, index, axis=1)
        gate = gate_all[toks].reshape(PAIR, SEL)
        w_t[...] = jnp.where(valid, (gate * act).astype(BF16).astype(F32), 0.0).T
        c_t[...] = jnp.where(valid, (gate * slope).astype(BF16).astype(F32), 0.0).T
        slot_t[...] = jnp.where(valid, local, -1).T

        def step(s, acc):
            acc_w, acc_c = acc
            hit = row_iota == slot_t[pl.ds(s, 1), :]
            acc_w += jnp.where(hit, w_t[pl.ds(s, 1), :], 0.0)
            acc_c += jnp.where(hit, c_t[pl.ds(s, 1), :], 0.0)
            return acc_w, acc_c

        zero = jnp.zeros((SLOTS, PAIR), F32)
        acc_w, acc_c = lax.fori_loop(0, SEL, step, (zero, zero), unroll=8)
        for ref, acc in ((w_buf, acc_w), (c_buf, acc_c)):
            terms = split3(acc)
            for j in range(2):
                ref[2 * r + j] = jnp.concatenate([term[:, j * TOK:(j + 1) * TOK] for term in terms], axis=1)

        def spread(acc):
            both = jnp.concatenate([acc.T, acc.T], axis=1)
            return split3(jnp.where(block_diag, both, 0.0))

        return spread(acc_w), spread(acc_c)

    def columns(r, terms, col, mine, other):
        rows = pl.ds(2 * r * SLOTS, 2 * SLOTS)
        table, terms = (down_rows, terms[0]) if col < half else (up_rows, terms[1])
        here = pl.ds(pl.multiple_of(core * half + col % half, COLS), COLS)
        there = pl.ds(pl.multiple_of((1 - core) * half + col % half, COLS), COLS)
        mine[:, col:col + COLS] = sum(jnp.dot(term, table[rows, here], preferred_element_type=F32) for term in terms)
        part = sum(jnp.dot(term, table[rows, there], preferred_element_type=F32) for term in terms)
        other[:TOK, col:col + COLS] = part[TOK:]
        other[TOK:, col:col + COLS] = part[:TOK]

    def block(r, mine, other):
        terms = front(r)
        for col in range(0, width, COLS):
            columns(r, terms, col, mine, other)

    def add_into(dst, src, cols=slice(None), step=16):
        def add(t, _):
            r = pl.ds(pl.multiple_of(t * step, step), step)
            dst[r, cols] = dst[r, cols] + src[r, cols]
            return 0

        lax.fori_loop(0, PAIR // step, add, 0)

    def blocks(mine, other):
        save = lambda src, dst, k: pltpu.make_async_copy(src, dst, out_sem.at[k])
        saves = []

        def keep_terms(r):
            for n, (src, dst) in enumerate(((c_buf, c_out), (w_buf, w_out))):
                saves.append(save(src.at[pl.ds(2 * r, 2)], dst.at[pl.ds(2 * r, 2)], TERM_SEM + 2 * r + n))
                saves[-1].start()

        arrive(near_own)
        arrive(far)
        near_far = [push(ref, 6, ref, 7, 1) for ref in (gate_all, slot_all, x_all, dy_all)]
        arrive(near_first + near_far)
        terms = front(3)
        pair_far, hop = [], []
        chunks = [pl.ds(col, COLS) for col in range(0, width, COLS)]
        every = slice(None)
        for cols in chunks:
            columns(3, terms, cols.start, mine.at[3], other.at[0])
            pair_far.append(push(other, (0, every, cols), pair_recv, (0, every, cols), 1))
        for k, cols in enumerate(chunks):
            arrive([pair_far[k]])
            add_into(mine.at[3], pair_recv.at[0], cols, 64)
            hop.append(push(mine, (3, every, cols), hop_recv, (every, cols), 2 + 2 * core))
        keep_terms(3)
        arrive(second)
        near_second = [push(gate_all, 2, gate_all, 3, 1), push(slot_all, 4, slot_all, 5, 1), push(x_all, 2, x_all, 3, 1), push(dy_all, 4, dy_all, 5, 1)]
        arrive(near_second)
        for k, (src, dst) in enumerate(((x_all, x_out), (dy_all, dy_out))):
            saves.append(save(src, dst, 1 + k))
            saves[-1].start()
        leave(pair_far)
        block(1, mine.at[1], other.at[0])
        pair_x = push(other, 0, pair_recv, 1, 1)
        keep_terms(1)
        block(2, mine.at[2], other.at[1])
        pair_y = push(other, 1, pair_recv, 2, 1)
        keep_terms(2)
        arrive([pair_x])
        add_into(mine.at[1], pair_recv.at[1])
        arrive([pair_y])
        add_into(mine.at[2], pair_recv.at[2])
        near, cross = pl.ds(0, TOK), pl.ds(TOK, TOK)
        part = push(mine, (1 + core, pl.ds(0, PART)), first_part, None, 2 + 2 * core)
        saves.append(save(mine.at[1 + core, pl.ds(PART, TOK - PART)], first_keep, 0))
        saves.append(save(mine.at[1 + core, cross], first_cross, 3))
        for copy in saves[-2:]:
            copy.start()
        leave([pair_x])
        block(0, mine.at[0], other.at[0])
        pair_own = push(other, 0, pair_recv, 3, 1)
        keep_terms(0)
        for k, cols in enumerate(chunks):
            arrive([hop[k]])
            add_into(mine.at[2 - core], hop_recv, cols, 64)
            for n, (rows, dst) in enumerate(((near, second_keep), (cross, second_cross))):
                saves.append(save(mine.at[2 - core, rows, cols], dst.at[:, cols], 5 + 2 * k + n))
                saves[-1].start()
        arrive([pair_own])
        add_into(mine.at[0], pair_recv.at[3])
        mine_cross = push(mine, (0, cross), own_cross, None, 1)
        saves.append(save(mine.at[0, near], own_keep, 4))
        saves[-1].start()
        arrive([part, mine_cross])
        leave([spec for spec in sent if spec not in pair_far and spec is not pair_x])
        for copy in saves:
            copy.wait()

    pl.run_scoped(blocks, pltpu.VMEM((4, PAIR, width), F32), pltpu.VMEM((2, PAIR, width), F32))


def row_kernel(asked_ref, c_ref, w_ref, x_ref, dy_ref, du_ref, dv_ref, wide_u, wide_v, part_u, part_v):
    n_rows, cols = du_ref.shape
    tiles = cols // LANES
    wide_step, part_step = n_rows + PAD, SLOTS + PAD
    part_size = tiles * part_step

    def clear(t, _):
        r = pl.multiple_of(t * 32, 32)
        for j in range(tiles):
            for wide in (wide_u, wide_v):
                wide[pl.ds(j * wide_step + r, 32), :] = jnp.zeros((32, LANES), F32)
        return 0

    lax.fori_loop(0, n_rows // 32, clear, 0)

    def product(q, slot):
        for coef, tok, part in ((c_ref, x_ref, part_u), (w_ref, dy_ref, part_v)):
            rows = tok[pl.ds(pl.multiple_of(q * TOK, TOK), TOK), :]
            full = jnp.dot(coef[q], jnp.concatenate([rows] * TERMS, axis=0), preferred_element_type=F32)
            for j in range(tiles):
                part[pl.ds(slot * part_size + j * part_step, SLOTS), :] = full[:, j * LANES:(j + 1) * LANES]

    product(0, 0)

    def device(q, _):
        product(lax.rem(q + 1, N_DEV), lax.rem(q + 1, 2))
        base = lax.rem(q, 2) * part_size
        for t in range(0, SLOTS, GROUP):
            rows = [asked_ref[q, t + u] for u in range(GROUP)]
            sums = [[wide[pl.ds(row, tiles, stride=wide_step), :] + part[pl.ds(base + t + u, tiles, stride=part_step), :]
                     for wide, part in ((wide_u, part_u), (wide_v, part_v))] for u, row in enumerate(rows)]
            for row, pair in zip(rows, sums):
                for wide, value in zip((wide_u, wide_v), pair):
                    wide[pl.ds(row, tiles, stride=wide_step), :] = value
        return 0

    lax.fori_loop(0, N_DEV, device, 0)

    def drain(t, _):
        r = pl.multiple_of(t * 32, 32)
        for j in range(tiles):
            for wide, out in ((wide_u, du_ref), (wide_v, dv_ref)):
                out[pl.ds(r, 32), j * LANES:(j + 1) * LANES] = wide[pl.ds(j * wide_step + r, 32), :].astype(BF16)
        return 0

    lax.fori_loop(0, n_rows // 32, drain, 0)


def join_kernel(fp_ref, fk_ref, fc_ref, sk_ref, sc_ref, ok_ref, oc_ref, y_ref, dx_ref):
    core = lax.rem(lax.axis_index("ep"), 2)
    half = y_ref.shape[1] // 2
    late = pl.program_id(0) * y_ref.shape[0] >= PART
    keep = (ok_ref[...] + jnp.where(late, fk_ref[...], fp_ref[...]) + sk_ref[...]).astype(BF16)
    cross = (oc_ref[...] + fc_ref[...] + sc_ref[...]).astype(BF16)
    here = pl.ds(pl.multiple_of(core * half, half), half)
    there = pl.ds(pl.multiple_of((1 - core) * half, half), half)
    for ref, cols in ((y_ref, slice(0, half)), (dx_ref, slice(half, 2 * half))):
        ref[:, here] = keep[:, cols]
        ref[:, there] = cross[:, cols]


def solution(mesh):
    tok_spec = P(('dp', 'ep'))
    table_spec = P('ep')

    def per_device(tokens, slot_ids, request_rows, gate_vals, grad_out, up_local, down_local):
        width = tokens.shape[1]
        rows_owner = up_local.shape[0]
        heads, top_k = slot_ids.shape[1:]
        n_tok = N_DEV * TOK
        half = width // 2
        core = lax.axis_index('ep') % 2
        anyw = pl.BlockSpec(memory_space=pl.ANY)
        shape = jax.ShapeDtypeStruct
        sums = shape((TOK, width), F32)
        x_all, dy_all, c_terms, w_terms, asked, first_part, first_keep, first_cross, second_keep, second_cross, own_keep, own_cross = pl.pallas_call(
            layer_kernel,
            in_specs=[anyw] * 7,
            out_specs=[anyw] * 12,
            out_shape=[shape((N_DEV, TOK, width), BF16)] * 2 + [shape((N_DEV, SLOTS, TERMS * TOK), BF16)] * 2 + [shape((N_DEV, SLOTS), I32)] + [shape((PART, width), F32), shape((TOK - PART, width), F32)] + [sums] * 5,
            scratch_shapes=[
                pltpu.VMEM((N_DEV, TOK, width), BF16), pltpu.VMEM((N_DEV, TOK, width), BF16),
                pltpu.VMEM((N_DEV, TOK, SEL), jnp.int16), pltpu.VMEM((N_DEV, TOK, SEL), F32),
                pltpu.VMEM((N_DEV * SLOTS, width), BF16), pltpu.VMEM((N_DEV * SLOTS, width), BF16),
                pltpu.VMEM((4, PAIR, width), F32), pltpu.VMEM((PAIR, width), F32),
                pltpu.VMEM((heads, top_k, TOK), I32), pltpu.VMEM((heads, top_k, TOK), F32), pltpu.VMEM((1, N_DEV, SLOTS), I32),
                pltpu.VMEM((N_DEV, SLOTS, TERMS * TOK), BF16), pltpu.VMEM((N_DEV, SLOTS, TERMS * TOK), BF16),
                pltpu.VMEM((N_DEV, SLOTS), I32), pltpu.SMEM((N_DEV, SLOTS), I32),
                pltpu.VMEM((SEL, PAIR), I32), pltpu.VMEM((SEL, PAIR), F32), pltpu.VMEM((SEL, PAIR), F32),
                pltpu.SemaphoreType.DMA((N_COPIES,)), pltpu.SemaphoreType.DMA((N_COPIES,)),
                pltpu.SemaphoreType.DMA((6,)), pltpu.SemaphoreType.DMA,
                pltpu.SemaphoreType.DMA((1,)), pltpu.SemaphoreType.DMA((TERM_SEM + N_DEV,)),
            ],
            compiler_params=pltpu.CompilerParams(collective_id=0, has_side_effects=True, vmem_limit_bytes=VMEM_BYTES),
        )(tokens, grad_out, slot_ids.transpose(1, 2, 0), gate_vals.transpose(1, 2, 0), request_rows, up_local, down_local)

        first_hop = [(i, i ^ (2 if i % 2 == 0 else 4)) for i in range(N_DEV)]
        second_hop = [(i, i ^ (4 if i % 2 == 0 else 2)) for i in range(N_DEV)]
        over = lambda pairs: [(i, j ^ 1) for i, j in pairs]
        hop = lambda value, pairs: lax.ppermute(value, 'ep', pairs)

        def grad_rows():
            coef = pl.BlockSpec((N_DEV, SLOTS, TERMS * TOK), lambda i, a: (0, 0, 0))
            tok = pl.BlockSpec((n_tok, ROW_CHUNK), lambda i, a: (0, i))
            out = pl.BlockSpec((rows_owner, ROW_CHUNK), lambda i, a: (0, i))
            tiles = ROW_CHUNK // LANES
            return pl.pallas_call(
                row_kernel,
                grid_spec=pltpu.PrefetchScalarGridSpec(
                    num_scalar_prefetch=1,
                    grid=(width // ROW_CHUNK,),
                    in_specs=[coef, coef, tok, tok],
                    out_specs=[out, out],
                    scratch_shapes=[pltpu.VMEM((tiles * (rows_owner + PAD), LANES), F32)] * 2 + [pltpu.VMEM((2 * tiles * (SLOTS + PAD), LANES), F32)] * 2,
                ),
                out_shape=[shape((rows_owner, width), BF16)] * 2,
                compiler_params=pltpu.CompilerParams(vmem_limit_bytes=VMEM_BYTES),
                cost_estimate=pl.CostEstimate(flops=12 * rows_owner * width * n_tok, bytes_accessed=4 * rows_owner * width, transcendentals=0),
            )(asked, c_terms, w_terms, x_all.reshape(n_tok, width), dy_all.reshape(n_tok, width))

        got = (hop(first_keep, first_hop), hop(first_cross, over(first_hop)), hop(second_keep, second_hop), hop(second_cross, over(second_hop)))
        grad_up, grad_down = grad_rows()
        got, grad_up, grad_down = lax.optimization_barrier((got, grad_up, grad_down))
        block = 32
        rows = pl.BlockSpec((block, width), lambda i: (i, 0))
        early = pl.BlockSpec((block, width), lambda i: (0, 0))
        out_tokens, grad_tokens = pl.pallas_call(
            join_kernel,
            grid=(TOK // block,),
            in_specs=[early] * 2 + [rows] * 5,
            out_specs=[rows, rows],
            out_shape=[shape((TOK, width), BF16)] * 2,
            compiler_params=pltpu.CompilerParams(vmem_limit_bytes=VMEM_BYTES),
        )(first_part, *got, own_keep, own_cross)
        return out_tokens, grad_tokens, grad_up, grad_down

    return jax.shard_map(per_device, mesh=mesh, in_specs=(tok_spec, tok_spec, tok_spec, tok_spec, tok_spec, table_spec, table_spec), out_specs=(tok_spec, tok_spec, tok_spec, tok_spec), check_vma=False)
```
